16 devices in a mesh: dp: 2 (over y, z), sh: 8 (over x, core).
Axes of the slice: x: 4, y: 2, z: 1, core: 2. Of those that a mesh axis runs over, the one named last changes fastest.
The devices are a block of a 4x4x8 slice.
Arguments:
- k_prefill: bfloat16 [16, 4352, 8, 128], P('dp', None, 'sh'), parts along dimension 0
- v_prefill: bfloat16 [16, 4352, 8, 128], P('dp', None, 'sh'), parts along dimension 0
- lengths: int32 [16], P('dp'), parts along dimension 0
- residual: bfloat16 [16, 4096], P(('dp', 'sh')), parts along dimension 0
- norm_gain: bfloat16 [4096], replicated
- w_query: bfloat16 [4096, 4096], replicated
- w_key: bfloat16 [4096, 1024], replicated
- w_value: bfloat16 [4096, 1024], replicated
- w_out: bfloat16 [4096, 4096], replicated
Outputs:
- output 1: bfloat16 [16, 4096], P(('dp', 'sh')), parts along dimension 0
- output 2: bfloat16 [16, 4096, 8, 128], P(('dp', 'sh')), parts along dimension 0
- output 3: bfloat16 [16, 4096, 8, 128], P(('dp', 'sh')), parts along dimension 0
There are 2 independent parts. The reference program is written for one: setup_inputs(seed, part) draws one part's arguments, and reference() takes and returns one part's arrays. A program takes and returns all parts, laid end to end along the dimension named above; an argument that names none is the same for every part.
All inputs are finite; a program needn't handle non-finite values.
Results may differ from the reference program's by a relative error of at most 0.00417.
Values are sent between devices in bfloat16 or wider.
A program may use at most 768 MiB of HBM per device.

```python
import jax
import jax.numpy as jnp
from jax import lax

MODEL_DIM = 4096
HEADS = 32
KV_HEADS = 8
HEAD_DIM = 128
WINDOW = 4096
SEQ_LEN = 4352
BATCH = 8
Q_GROUP = HEADS // KV_HEADS
Q_WIDTH = HEADS * HEAD_DIM
KV_WIDTH = KV_HEADS * HEAD_DIM
THETA = 10000.0
EPS = 1e-5


def setup_inputs(seed: int = 0, part: int = 0) -> dict:
    root_key = jax.random.key(seed)
    part_root, shared_root = jax.random.split(root_key)
    part_keys = jax.random.split(jax.random.fold_in(part_root, part), 4)
    shared_keys = jax.random.split(shared_root, 5)
    kv_shape = (BATCH, SEQ_LEN, KV_HEADS, HEAD_DIM)
    k_prefill = jax.random.normal(part_keys[0], kv_shape, jnp.float32).astype(jnp.bfloat16)
    v_prefill = jax.random.normal(part_keys[1], kv_shape, jnp.float32).astype(jnp.bfloat16)
    lengths = jax.random.randint(part_keys[2], (BATCH,), 1, SEQ_LEN + 1, dtype=jnp.int32)
    lengths = lengths.at[0].set(SEQ_LEN).at[1].set(1)
    residual = jax.random.normal(part_keys[3], (BATCH, MODEL_DIM), jnp.float32).astype(jnp.bfloat16)
    norm_gain = (1.0 + 0.3 * jax.random.normal(shared_keys[0], (MODEL_DIM,), jnp.float32)).astype(jnp.bfloat16)
    w_query = (jax.random.normal(shared_keys[1], (MODEL_DIM, Q_WIDTH), jnp.float32) * (2.0 / MODEL_DIM ** 0.5)).astype(jnp.bfloat16)
    w_key = (jax.random.normal(shared_keys[2], (MODEL_DIM, KV_WIDTH), jnp.float32) * (3.0 / MODEL_DIM ** 0.5)).astype(jnp.bfloat16)
    w_value = (jax.random.normal(shared_keys[3], (MODEL_DIM, KV_WIDTH), jnp.float32) * (3.0 / MODEL_DIM ** 0.5)).astype(jnp.bfloat16)
    w_out = (jax.random.normal(shared_keys[4], (Q_WIDTH, MODEL_DIM), jnp.float32) * (2.0 / Q_WIDTH ** 0.5)).astype(jnp.bfloat16)
    return {'k_prefill': k_prefill, 'v_prefill': v_prefill, 'lengths': lengths, 'residual': residual, 'norm_gain': norm_gain, 'w_query': w_query, 'w_key': w_key, 'w_value': w_value, 'w_out': w_out}


def rolling_cache(prefill, lengths):
    slot_ids = jnp.arange(WINDOW, dtype=jnp.int32)
    last_pos = lengths[:, None] - 1
    held_pos = last_pos - jnp.remainder(last_pos - slot_ids[None, :], WINDOW)
    held = jax.vmap(lambda row_vals, row_idx: jnp.take(row_vals, row_idx, axis=0))(prefill, jnp.maximum(held_pos, 0))
    return jnp.where((held_pos >= 0)[:, :, None, None], held, jnp.zeros((), prefill.dtype))


def rotate(heads, positions):
    half_dim = HEAD_DIM // 2
    inv_freq = THETA ** (-2.0 * jnp.arange(half_dim, dtype=jnp.float32) / HEAD_DIM)
    angles = positions.astype(jnp.float32).reshape(positions.shape + (1,) * (heads.ndim - 1)) * inv_freq
    cos_part = jnp.cos(angles)
    sin_part = jnp.sin(angles)
    first_half = heads[..., :half_dim].astype(jnp.float32)
    second_half = heads[..., half_dim:].astype(jnp.float32)
    return jnp.concatenate([first_half * cos_part - second_half * sin_part, second_half * cos_part + first_half * sin_part], axis=-1).astype(jnp.bfloat16)


def attend_row(row_args):
    q_row, k_row, v_row, live_row = row_args
    q_grouped = q_row.reshape(KV_HEADS, Q_GROUP, HEAD_DIM).astype(jnp.float32)
    scores = jnp.einsum('kgd,wkd->kgw', q_grouped, k_row.astype(jnp.float32)) / HEAD_DIM ** 0.5
    scores = jnp.where(live_row[None, None, :], scores, -jnp.inf)
    weights = jax.nn.softmax(scores, axis=-1).astype(jnp.bfloat16)
    mixed = jnp.einsum('kgw,wkd->kgd', weights.astype(jnp.float32), v_row.astype(jnp.float32))
    return mixed.astype(jnp.bfloat16).reshape(Q_WIDTH)


def reference(k_prefill, v_prefill, lengths, residual, norm_gain, w_query, w_key, w_value, w_out):
    k_cache = rolling_cache(k_prefill, lengths)
    v_cache = rolling_cache(v_prefill, lengths)
    resid_f32 = residual.astype(jnp.float32)
    inv_rms = lax.rsqrt(jnp.mean(resid_f32 * resid_f32, axis=-1, keepdims=True) + EPS)
    normed = (resid_f32 * inv_rms * norm_gain.astype(jnp.float32)).astype(jnp.bfloat16)
    q_heads = jnp.dot(normed, w_query, preferred_element_type=jnp.float32).astype(jnp.bfloat16).reshape(BATCH, HEADS, HEAD_DIM)
    k_new = jnp.dot(normed, w_key, preferred_element_type=jnp.float32).astype(jnp.bfloat16).reshape(BATCH, KV_HEADS, HEAD_DIM)
    v_new = jnp.dot(normed, w_value, preferred_element_type=jnp.float32).astype(jnp.bfloat16).reshape(BATCH, KV_HEADS, HEAD_DIM)
    q_heads = rotate(q_heads, lengths)
    k_new = rotate(k_new, lengths)
    slot_ids = jnp.arange(WINDOW, dtype=jnp.int32)
    new_slot = (slot_ids[None, :] == (lengths % WINDOW)[:, None])[:, :, None, None]
    k_cache = jnp.where(new_slot, k_new[:, None], k_cache)
    v_cache = jnp.where(new_slot, v_new[:, None], v_cache)
    live_slot = (lengths[:, None] - jnp.remainder(lengths[:, None] - slot_ids[None, :], WINDOW)) >= 0
    attn_out = lax.map(attend_row, (q_heads, k_cache, v_cache, live_slot))
    resid_out = (resid_f32 + jnp.dot(attn_out, w_out, preferred_element_type=jnp.float32)).astype(jnp.bfloat16)
    return (resid_out, k_cache, v_cache)
```

```python
import functools

import jax
import jax.numpy as jnp
from jax import lax
from jax.experimental import pallas as pl
from jax.experimental.pallas import tpu as pltpu
from jax.sharding import PartitionSpec as P

WINDOW = 4096
THETA = 10000.0
EPS = 1e-5
MESH = pl.DeviceIdType.MESH


def rotate(heads, positions):
    head_dim = heads.shape[-1]
    half_dim = head_dim // 2
    inv_freq = THETA ** (-2.0 * jnp.arange(half_dim, dtype=jnp.float32) / head_dim)
    angles = positions.astype(jnp.float32).reshape(positions.shape + (1,) * (heads.ndim - 1)) * inv_freq
    cos_part = jnp.cos(angles)
    sin_part = jnp.sin(angles)
    first_half = heads[..., :half_dim].astype(jnp.float32)
    second_half = heads[..., half_dim:].astype(jnp.float32)
    return jnp.concatenate([first_half * cos_part - second_half * sin_part, second_half * cos_part + first_half * sin_part], axis=-1).astype(jnp.bfloat16)


def decode_rows(residual, lengths, k_cache, v_cache, norm_gain, w_query, w_key, w_value, w_out):
    num_rows = residual.shape[0]
    kv_heads = k_cache.shape[2]
    head_dim = k_cache.shape[3]
    q_group = w_query.shape[1] // (kv_heads * head_dim)
    resid_f32 = residual.astype(jnp.float32)
    inv_rms = lax.rsqrt(jnp.mean(resid_f32 * resid_f32, axis=-1, keepdims=True) + EPS)
    normed = (resid_f32 * inv_rms * norm_gain.astype(jnp.float32)).astype(jnp.bfloat16)
    q_heads = jnp.dot(normed, w_query, preferred_element_type=jnp.float32).astype(jnp.bfloat16).reshape(num_rows, kv_heads, q_group, head_dim)
    k_new = jnp.dot(normed, w_key, preferred_element_type=jnp.float32).astype(jnp.bfloat16).reshape(num_rows, kv_heads, head_dim)
    v_new = jnp.dot(normed, w_value, preferred_element_type=jnp.float32).astype(jnp.bfloat16).reshape(num_rows, kv_heads, head_dim)
    q_heads = rotate(q_heads, lengths)
    k_new = rotate(k_new, lengths)
    slot_ids = jnp.arange(WINDOW, dtype=jnp.int32)
    new_slot = (slot_ids[None, :] == (lengths % WINDOW)[:, None])[:, :, None, None]
    held = (slot_ids[None, :] < lengths[:, None])[:, :, None, None]
    k_cache = jnp.where(new_slot, k_new[:, None], jnp.where(held, k_cache, 0))
    v_cache = jnp.where(new_slot, v_new[:, None], jnp.where(held, v_cache, 0))
    live_slot = slot_ids[None, :] <= lengths[:, None]
    scores = jnp.einsum('rkgd,rwkd->rkgw', q_heads, k_cache, preferred_element_type=jnp.float32) / head_dim ** 0.5
    scores = jnp.where(live_slot[:, None, None, :], scores, -jnp.inf)
    exp_scores = jnp.exp(scores - jnp.max(scores, axis=-1, keepdims=True))
    weights = (exp_scores / jnp.sum(exp_scores, axis=-1, keepdims=True)).astype(jnp.bfloat16)
    attn_out = jnp.einsum('rkgw,rwkd->rkgd', weights, v_cache, preferred_element_type=jnp.float32).astype(jnp.bfloat16).reshape(num_rows, kv_heads * q_group * head_dim)
    resid_out = (resid_f32 + jnp.dot(attn_out, w_out, preferred_element_type=jnp.float32)).astype(jnp.bfloat16)
    return resid_out, k_cache, v_cache


def exchange_kernel(n, rows, over, k_over, v_over, k_in, v_in, k_out, v_out, send_sem, recv_sem, own_sem):
    me = lax.axis_index('sh')
    window = k_out.shape[1]
    barrier = pltpu.get_barrier_semaphore()
    for d in range(1, n):
        pl.semaphore_signal(barrier, inc=1, device_id={'sh': lax.rem(me + d, n)}, device_id_type=MESH)
    pl.semaphore_wait(barrier, n - 1)
    parts = ((k_over, k_out, 0, over), (v_over, v_out, 0, over), (k_in, k_out, over, window - over), (v_in, v_out, over, window - over))
    copies = []
    for p, (src, dst, first, size) in enumerate(parts):
        for d in (2, 6, 3, 5, 4, 7, 1):
            peer = lax.rem(me + d, n)
            copy = pltpu.make_async_remote_copy(
                src_ref=src.at[peer, pl.ds(first, size)], dst_ref=dst.at[me, pl.ds(first, size)],
                send_sem=send_sem.at[d, p], recv_sem=recv_sem.at[d, p], device_id={'sh': peer}, device_id_type=MESH)
            copy.start()
            copies.append(copy)
        own = pltpu.make_async_copy(src.at[me, pl.ds(first, size)], dst.at[me, pl.ds(first, size)], own_sem.at[p])
        own.start()
        copies.append(own)
    for copy in copies:
        copy.wait()


def exchange(n, k_rows, v_rows, k_over, v_over):
    rows, _, head_dim = k_rows.shape
    out = jax.ShapeDtypeStruct((n, WINDOW, head_dim), k_rows.dtype)
    any_spec = pl.BlockSpec(memory_space=pl.ANY)
    return pl.pallas_call(
        functools.partial(exchange_kernel, n, rows, k_over.shape[1]),
        out_shape=(out, out),
        in_specs=[any_spec] * 4,
        out_specs=(any_spec, any_spec),
        scratch_shapes=[pltpu.SemaphoreType.DMA((n, 4)), pltpu.SemaphoreType.DMA((n, 4)), pltpu.SemaphoreType.DMA((4,))],
        compiler_params=pltpu.CompilerParams(collective_id=0, has_side_effects=True),
        name='exchange',
    )(k_over, v_over, k_rows, v_rows)


def solution(mesh):
    head_spec = P('dp', None, 'sh', None)
    row_spec = P(('dp', 'sh'))
    full_spec = P(None, None)
    n = mesh.shape['sh']

    def per_device(k_prefill, v_prefill, lengths, residual, norm_gain, w_query, w_key, w_value, w_out):
        num_rows = residual.shape[0]
        rows, seq, _, head_dim = k_prefill.shape
        my_lengths = lax.dynamic_slice_in_dim(lengths, lax.axis_index('sh') * num_rows, num_rows)
        k_rows = k_prefill.reshape(rows, seq, head_dim)
        v_rows = v_prefill.reshape(rows, seq, head_dim)
        over = seq - WINDOW
        wraps = (jnp.arange(over, dtype=jnp.int32)[None, :] < lengths[:, None] - WINDOW)[:, :, None]
        k_over = jnp.where(wraps, k_rows[:, WINDOW:], k_rows[:, :over])
        v_over = jnp.where(wraps, v_rows[:, WINDOW:], v_rows[:, :over])
        k_heads, v_heads = exchange(n, k_rows, v_rows, k_over, v_over)
        k_cache = k_heads.transpose(1, 0, 2)[None]
        v_cache = v_heads.transpose(1, 0, 2)[None]
        return decode_rows(residual, my_lengths, k_cache, v_cache, norm_gain, w_query, w_key, w_value, w_out)
    return jax.shard_map(per_device, mesh=mesh, in_specs=(head_spec, head_spec, P('dp'), P(('dp', 'sh'), None), P(None), full_spec, full_spec, full_spec, full_spec), out_specs=(P(('dp', 'sh'), None), row_spec, row_spec), check_vma=False)
```

```python
import functools

import jax
import jax.numpy as jnp
from jax import lax
from jax.experimental import pallas as pl
from jax.experimental.pallas import tpu as pltpu
from jax.sharding import PartitionSpec as P

WINDOW = 4096
THETA = 10000.0
EPS = 1e-5
MESH = pl.DeviceIdType.MESH


def rotate(heads, positions):
    head_dim = heads.shape[-1]
    half_dim = head_dim // 2
    inv_freq = THETA ** (-2.0 * jnp.arange(half_dim, dtype=jnp.float32) / head_dim)
    angles = positions.astype(jnp.float32).reshape(positions.shape + (1,) * (heads.ndim - 1)) * inv_freq
    cos_part = jnp.cos(angles)
    sin_part = jnp.sin(angles)
    first_half = heads[..., :half_dim].astype(jnp.float32)
    second_half = heads[..., half_dim:].astype(jnp.float32)
    return jnp.concatenate([first_half * cos_part - second_half * sin_part, second_half * cos_part + first_half * sin_part], axis=-1).astype(jnp.bfloat16)

def stage_kernel(n, group, nblk_max, len_ref, level_ref, k_in, v_in, k_over, v_over, k_stage, v_stage, over_a, over_b, over_o, sem, out_sem, blk_sem):
    over = over_a.shape[2]
    nblk = WINDOW // group
    half = level_ref[0]
    first = 2 * half - nblk
    for a, (src, _) in enumerate(((k_in, k_over), (v_in, v_over))):
        pltpu.make_async_copy(src.at[:, pl.ds(0, over)], over_a.at[a], sem.at[a, 0]).start()
        pltpu.make_async_copy(src.at[:, pl.ds(WINDOW, over)], over_b.at[a], sem.at[a, 1]).start()

    def block_copy(src, dst, r, j, a):
        blocks = lax.div(jnp.minimum(len_ref[r], WINDOW) + group - 1, group)
        mine = j < blocks
        row = jnp.where(mine, r, r + 1 - 2 * lax.rem(r, 2))
        at = jnp.where(mine, j, 2 * half - 1 - j)
        return pltpu.make_async_copy(src.at[row, pl.ds(pl.multiple_of(at * group, group), group)], dst.at[r, pl.ds(pl.multiple_of((j - first) * group, group), group)], blk_sem.at[a])

    def start(r, c):
        def one(j, c):
            block_copy(k_in, k_stage, r, j, 0).start()
            block_copy(v_in, v_stage, r, j, 1).start()
            return c
        return lax.fori_loop(first, half, one, c)
    lax.fori_loop(0, n, start, 0)
    for a, (src, dst) in enumerate(((k_in, k_over), (v_in, v_over))):
        pltpu.make_async_copy(src.at[:, pl.ds(0, over)], over_a.at[a], sem.at[a, 0]).wait()
        pltpu.make_async_copy(src.at[:, pl.ds(WINDOW, over)], over_b.at[a], sem.at[a, 1]).wait()
        for r in range(n):
            slot = lax.broadcasted_iota(jnp.int32, over_a.shape[2:], 0)
            over_o[a, r] = jnp.where(slot < len_ref[r] - WINDOW, over_b[a, r], over_a[a, r])
        pltpu.make_async_copy(over_o.at[a], dst, out_sem.at[a]).start()

    def finish(r, c):
        def one(j, c):
            block_copy(k_in, k_stage, r, j, 0).wait()
            block_copy(v_in, v_stage, r, j, 1).wait()
            return c
        return lax.fori_loop(first, half, one, c)
    lax.fori_loop(0, n, finish, 0)
    for a, dst in enumerate((k_over, v_over)):
        pltpu.make_async_copy(over_o.at[a], dst, out_sem.at[a]).wait()


def stage(n, group, lengths, half, k_rows, v_rows):
    rows, seq, head_dim = k_rows.shape
    over = seq - WINDOW
    nblk = WINDOW // group
    most = nblk - min(levels(group))
    any_spec = pl.BlockSpec(memory_space=pl.ANY)
    smem = pl.BlockSpec(memory_space=pltpu.SMEM)
    o = jax.ShapeDtypeStruct((rows, over, head_dim), k_rows.dtype)
    s = jax.ShapeDtypeStruct((rows, most * group, head_dim), k_rows.dtype)
    return pl.pallas_call(
        functools.partial(stage_kernel, n, group, most),
        out_shape=(o, o, s, s),
        in_specs=[smem, smem, any_spec, any_spec],
        out_specs=(any_spec, any_spec, pl.BlockSpec(memory_space=pltpu.VMEM), pl.BlockSpec(memory_space=pltpu.VMEM)),
        scratch_shapes=[pltpu.VMEM((2, rows, over, head_dim), k_rows.dtype)] * 3 + [pltpu.SemaphoreType.DMA((2, 2)), pltpu.SemaphoreType.DMA((2,)), pltpu.SemaphoreType.DMA((2,))],
        compiler_params=pltpu.CompilerParams(vmem_limit_bytes=40 << 20),
        name='stage',
    )(lengths, half, k_rows, v_rows)


def levels(group):
    nblk = WINDOW // group
    return tuple(range(nblk // 2 + 1, nblk + 1))


def exchange_kernel(n, group, half, k_over, v_over, k_stage, v_stage, k_in, v_in, k_out, v_out, send_sem, recv_sem, own_sem, fsend_sem, frecv_sem):
    me = lax.axis_index('sh')
    mate = me + 1 - 2 * lax.rem(me, 2)
    over = k_over.shape[1]
    nblk = WINDOW // group
    first = 2 * half - nblk
    barrier = pltpu.get_barrier_semaphore()
    for d in range(1, n):
        pl.semaphore_signal(barrier, inc=1, device_id={'sh': lax.rem(me + d, n)}, device_id_type=MESH)
    pl.semaphore_wait(barrier, n - 1)

    parts = []
    for stage_ref, over_ref, src, dst in ((k_stage, k_over, k_in, k_out), (v_stage, v_over, v_in, v_out)):
        parts.append((stage_ref, 0, dst, max(first * group, over), half * group - max(first * group, over)) if first < half else None)
        if first * group < over:
            parts[-1] = (stage_ref, over - first * group, dst, over, half * group - over)
        parts.append((over_ref, 0, dst, 0, over))
        parts.append((src, over, dst, over, first * group - over) if first * group > over else None)

    def send(p, d):
        src, at, dst, to, size = parts[p]
        peer = lax.rem(me + d, n)
        return pltpu.make_async_remote_copy(
            src_ref=src.at[peer, pl.ds(at, size)], dst_ref=dst.at[me, pl.ds(to, size)],
            send_sem=send_sem.at[d, p], recv_sem=recv_sem.at[d, p], device_id={'sh': peer}, device_id_type=MESH)

    def own(p):
        src, at, dst, to, size = parts[p]
        return pltpu.make_async_copy(src.at[me, pl.ds(at, size)], dst.at[me, pl.ds(to, size)], own_sem.at[p])

    order = (2, 6, 3, 5, 4, 7, 1)
    live = [p for p in range(len(parts)) if parts[p]]
    for p in live:
        for d in order:
            send(p, d).start()
        own(p).start()

    def forward(a, dst, head, j):
        return pltpu.make_async_remote_copy(
            src_ref=dst.at[head, pl.ds(j * group, group)], dst_ref=dst.at[head, pl.ds((2 * half - 1 - j) * group, group)],
            send_sem=fsend_sem.at[a], recv_sem=frecv_sem.at[a], device_id={'sh': mate}, device_id_type=MESH)

    waits = [(p, d) for p in live for d in order]
    owns = list(live)
    if first < half:
        for a, (p, dst) in enumerate(((0, k_out), (3, v_out))):
            own(p).wait()
            owns.remove(p)
            for d in (None, 7, 1) + order[:5]:
                if d is not None:
                    send(p, d).wait_recv()
                head = me if d is None else lax.rem(me - d + n, n)

                def go(j, c):
                    forward(a, dst, head, j).start()
                    return c
                lax.fori_loop(first, half, go, 0)
    for p, d in waits:
        copy = send(p, d)
        copy.wait_send()
        if not (first < half and p in (0, 3)):
            copy.wait_recv()
    for p in owns:
        own(p).wait()
    if first < half:
        for a, dst in enumerate((k_out, v_out)):
            all_sent = pltpu.make_async_remote_copy(
                src_ref=dst.at[:, pl.ds(first * group, (half - first) * group)], dst_ref=dst.at[:, pl.ds(half * group, (half - first) * group)],
                send_sem=fsend_sem.at[a], recv_sem=frecv_sem.at[a], device_id={'sh': mate}, device_id_type=MESH)
            all_sent.wait_send()
            all_sent.wait_recv()


def exchange(n, group, half, k_over, v_over, k_stage, v_stage, k_rows, v_rows):
    rows, _, head_dim = k_rows.shape
    out = jax.ShapeDtypeStruct((n, WINDOW, head_dim), k_rows.dtype)
    any_spec = pl.BlockSpec(memory_space=pl.ANY)
    return pl.pallas_call(
        functools.partial(exchange_kernel, n, group, half),
        out_shape=(out, out),
        in_specs=[any_spec] * 6,
        out_specs=(any_spec, any_spec),
        scratch_shapes=[pltpu.SemaphoreType.DMA((n, 6)), pltpu.SemaphoreType.DMA((n, 6)), pltpu.SemaphoreType.DMA((6,)), pltpu.SemaphoreType.DMA((2,)), pltpu.SemaphoreType.DMA((2,))],
        compiler_params=pltpu.CompilerParams(collective_id=0, has_side_effects=True, vmem_limit_bytes=4 << 20),
        name=f'exchange{half}',
    )(k_over, v_over, k_stage, v_stage, k_rows, v_rows)


def attend_kernel(blk, wblk, len_ref, k_in, v_in, q_ref, kn_ref, vn_ref, perm_ref, x_ref, w_ref, k_out, v_out, x_out, scores, probs, acc, p_new, flat, total):
    step = pl.program_id(0)
    heads, _, head_dim = k_in.shape
    q_group = q_ref.shape[1]
    steps = WINDOW // blk
    length = len_ref[0]
    fresh = lax.rem(length, WINDOW)
    part = perm_ref.shape[0] // heads

    def interleave(src, new, dst, base):
        new_rows = jnp.tile(new, (part, 1)).astype(jnp.float32)
        for g in range(0, blk // part, 2):
            pair = jnp.concatenate([src[:, pl.ds((g + e) * part, part), :].reshape(heads * part, head_dim) for e in (0, 1)], axis=1)
            mixed = jnp.dot(perm_ref[...], pair, preferred_element_type=jnp.float32)
            for e in (0, 1):
                row = lax.broadcasted_iota(jnp.int32, (heads * part, head_dim), 0) + (base + (g + e) * part) * heads
                value = mixed[:, e * head_dim:(e + 1) * head_dim]
                value = jnp.where(row < length * heads, value, 0.0)
                value = jnp.where((row >= fresh * heads) & (row < (fresh + 1) * heads), new_rows, value)
                dst[pl.ds((g + e) * part * heads, part * heads), :] = value.astype(dst.dtype)

    @pl.when(step < steps)
    def _():
        base = step * blk
        for h in range(heads):
            scores[h, :, pl.ds(pl.multiple_of(base, blk), blk)] = lax.dot_general(q_ref[h], k_in[h], (((1,), (1,)), ((), ())), preferred_element_type=jnp.float32)
        interleave(k_in, kn_ref[...], k_out, base)

    @pl.when(step == steps)
    def _():
        slot = lax.broadcasted_iota(jnp.int32, (q_group, WINDOW), 1)
        for h in range(heads):
            s_new = jnp.sum(q_ref[h].astype(jnp.float32) * kn_ref[pl.ds(h, 1), :].astype(jnp.float32), axis=-1, keepdims=True)
            s = jnp.where(slot == fresh, s_new, scores[h]) / head_dim ** 0.5
            s = jnp.where(slot <= length, s, -jnp.inf)
            e = jnp.exp(s - jnp.max(s, axis=-1, keepdims=True))
            p = e / jnp.sum(e, axis=-1, keepdims=True)
            p_new[h] = jnp.sum(jnp.where(slot == fresh, p, 0.0), axis=-1, keepdims=True)
            probs[h] = jnp.where(slot == fresh, 0.0, p).astype(probs.dtype)
            acc[h] = jnp.zeros_like(acc[h])

    @pl.when((step >= steps) & (step < 2 * steps))
    def _():
        base = (step - steps) * blk
        for h in range(heads):
            acc[h] += jnp.dot(probs[h, :, pl.ds(pl.multiple_of(base, blk), blk)], v_in[h], preferred_element_type=jnp.float32)
        interleave(v_in, vn_ref[...], v_out, base)

    @pl.when(step == 2 * steps)
    def _():
        for h in range(heads):
            o = acc[h] + p_new[h].astype(jnp.bfloat16).astype(jnp.float32) * vn_ref[pl.ds(h, 1), :].astype(jnp.float32)
            for g in range(q_group):
                flat[:, pl.ds((h * q_group + g) * head_dim, head_dim)] = o[g:g + 1].astype(flat.dtype)
        total[...] = x_ref[...].astype(jnp.float32)

    @pl.when(step >= 2 * steps)
    def _():
        at = pl.multiple_of((step - 2 * steps) * wblk, wblk)
        total[...] += jnp.dot(flat[:, pl.ds(at, wblk)], w_ref[...], preferred_element_type=jnp.float32)

    @pl.when(step == pl.num_programs(0) - 1)
    def _():
        x_out[...] = total[...].astype(x_out.dtype)


def attend(my_len, k_heads, v_heads, q, k_new, v_new, residual, w_out):
    heads, _, head_dim = k_heads.shape
    width, dim = w_out.shape
    blk, wblk, part = 512, 512, 256 // heads
    steps = WINDOW // blk
    wsteps = width // wblk
    row = jnp.arange(part * heads)
    perm = (row[None, :] == (row % heads * part + row // heads)[:, None]).astype(k_heads.dtype)
    cache = jax.ShapeDtypeStruct((WINDOW * heads, head_dim), k_heads.dtype)
    whole = lambda a: pl.BlockSpec(a.shape, lambda i, *_: (0,) * a.ndim)
    kmap = lambda i: jnp.minimum(i, steps - 1)
    vmap_ = lambda i: jnp.clip(i - steps, 0, steps - 1)
    wmap = lambda i: jnp.clip(i - 2 * steps, 0, wsteps - 1)
    return pl.pallas_call(
        functools.partial(attend_kernel, blk, wblk),
        grid_spec=pltpu.PrefetchScalarGridSpec(
            num_scalar_prefetch=1, grid=(2 * steps + wsteps,),
            in_specs=[
                pl.BlockSpec((heads, blk, head_dim), lambda i, *_: (0, kmap(i), 0)),
                pl.BlockSpec((heads, blk, head_dim), lambda i, *_: (0, vmap_(i), 0)),
                whole(q), whole(k_new), whole(v_new), whole(perm), whole(residual),
                pl.BlockSpec((wblk, dim), lambda i, *_: (wmap(i), 0)),
            ],
            out_specs=[
                pl.BlockSpec((blk * heads, head_dim), lambda i, *_: (kmap(i), 0)),
                pl.BlockSpec((blk * heads, head_dim), lambda i, *_: (vmap_(i), 0)),
                pl.BlockSpec((1, dim), lambda i, *_: (0, 0)),
            ],
            scratch_shapes=[
                pltpu.VMEM((heads, q.shape[1], WINDOW), jnp.float32),
                pltpu.VMEM((heads, q.shape[1], WINDOW), jnp.bfloat16),
                pltpu.VMEM((heads, q.shape[1], head_dim), jnp.float32),
                pltpu.VMEM((heads, q.shape[1], 1), jnp.float32),
                pltpu.VMEM((1, width), jnp.bfloat16),
                pltpu.VMEM((1, dim), jnp.float32),
            ]),
        out_shape=(cache, cache, jax.ShapeDtypeStruct(residual.shape, residual.dtype)),
        compiler_params=pltpu.CompilerParams(dimension_semantics=('arbitrary',), vmem_limit_bytes=VMEM_ATTEND),
        cost_estimate=pl.CostEstimate(flops=10 ** 9, bytes_accessed=64 << 20, transcendentals=0),
        name='attend',
    )(my_len, k_heads, v_heads, q, k_new, v_new, perm, residual, w_out)


GROUP = 256
VMEM_ATTEND = 24 << 20


def solution(mesh):
    head_spec = P('dp', None, 'sh', None)
    row_spec = P(('dp', 'sh'))
    full_spec = P(None, None)
    n = mesh.shape['sh']

    def per_device(k_prefill, v_prefill, lengths, residual, norm_gain, w_query, w_key, w_value, w_out):
        num_rows = residual.shape[0]
        rows, seq, _, head_dim = k_prefill.shape
        kv_heads = w_key.shape[1] // head_dim
        q_group = w_query.shape[1] // w_key.shape[1]
        my_len = lax.dynamic_slice_in_dim(lengths, lax.axis_index('sh') * num_rows, num_rows)
        k_rows = k_prefill.reshape(rows, seq, head_dim)
        v_rows = v_prefill.reshape(rows, seq, head_dim)
        blocks = (jnp.minimum(lengths, WINDOW) + GROUP - 1) // GROUP
        need = (jnp.max(blocks.reshape(-1, 2).sum(axis=1)) + 1) // 2
        level = jnp.maximum(need - levels(GROUP)[0], 0)
        k_over, v_over, k_stage, v_stage = stage(n, GROUP, lengths, (level + levels(GROUP)[0])[None], k_rows, v_rows)
        k_heads, v_heads = lax.switch(level, [functools.partial(exchange, n, GROUP, half) for half in levels(GROUP)], k_over, v_over, k_stage, v_stage, k_rows, v_rows)

        resid_f32 = residual.astype(jnp.float32)
        inv_rms = lax.rsqrt(jnp.mean(resid_f32 * resid_f32, axis=-1, keepdims=True) + EPS)
        normed = (resid_f32 * inv_rms * norm_gain.astype(jnp.float32)).astype(jnp.bfloat16)
        q = jnp.dot(normed, w_query, preferred_element_type=jnp.float32).astype(jnp.bfloat16).reshape(num_rows, kv_heads, q_group, head_dim)
        k_new = jnp.dot(normed, w_key, preferred_element_type=jnp.float32).astype(jnp.bfloat16).reshape(num_rows, kv_heads, head_dim)
        v_new = jnp.dot(normed, w_value, preferred_element_type=jnp.float32).astype(jnp.bfloat16).reshape(num_rows, kv_heads, head_dim)
        q = rotate(q, my_len)
        k_new = rotate(k_new, my_len)
        k_cache, v_cache, resid_out = attend(my_len, k_heads, v_heads, q[0], k_new[0], v_new[0], residual, w_out)
        cache_shape = (num_rows, WINDOW, kv_heads, head_dim)
        return resid_out, k_cache.reshape(cache_shape), v_cache.reshape(cache_shape)
    return jax.shard_map(per_device, mesh=mesh, in_specs=(head_spec, head_spec, P('dp'), P(('dp', 'sh'), None), P(None), full_spec, full_spec, full_spec, full_spec), out_specs=(P(('dp', 'sh'), None), row_spec, row_spec), check_vma=False)
```

```python
import functools

import jax
import jax.numpy as jnp
from jax import lax
from jax.experimental import pallas as pl
from jax.experimental.pallas import tpu as pltpu
from jax.sharding import PartitionSpec as P

WINDOW = 4096
THETA = 10000.0
EPS = 1e-5
MESH = pl.DeviceIdType.MESH


def levels(group):
    nblk = WINDOW // group
    return tuple(range(nblk // 2 + 1, nblk + 1))


def exchange_kernel(n, group, half, len_ref, x_ref, g_ref, cos_ref, sin_ref, k_in, v_in, wq, wk, wv,
                    k_out, v_out, flat, k_new, v_new,
                    over_a, over_b, staged, kv_buf, wbuf, normed, proj, proj2, q_heads, scores, probs, p_new, acc, k_rows32,
                    send_sem, recv_sem, own_sem, fsend_sem, frecv_sem, over_sem, stage_sem, w_sem, kv_sem):
    me = lax.axis_index('sh')
    mate = me + 1 - 2 * lax.rem(me, 2)
    heads, q_group, head_dim = q_heads.shape
    over = over_a.shape[2]
    nblk = WINDOW // group
    first = 2 * half - nblk
    nst = half - first
    barrier = pltpu.get_barrier_semaphore()
    for d in range(1, n):
        pl.semaphore_signal(barrier, inc=1, device_id={'sh': lax.rem(me + d, n)}, device_id_type=MESH)

    ins, outs = (k_in, v_in), (k_out, v_out)

    def over_load(a, e):
        return pltpu.make_async_copy(ins[a].at[:, pl.ds(e * WINDOW, over)], (over_a, over_b)[e].at[a], over_sem.at[a, e])

    def own_load(a):
        return pltpu.make_async_copy(ins[a].at[:, pl.ds(first * group, nst * group)], staged.at[a], stage_sem.at[a, 0])

    def other_load(a):
        return pltpu.make_async_copy(ins[a].at[:, pl.ds(half * group, nst * group)], kv_buf.at[:, pl.ds(a * nst * group, nst * group)], stage_sem.at[a, 1])
    for a in (0, 1):
        if nst:
            own_load(a).start()
            other_load(a).start()
        for e in (0, 1):
            over_load(a, e).start()
    depth, wide = wbuf.shape[1], wbuf.shape[2]
    wsteps = wq.shape[0] // depth
    weights = ((wq, 0), (wk, wq.shape[1]), (wv, wq.shape[1] + wk.shape[1]))

    def w_load(step, slot, i):
        src, at = weights[i]
        return pltpu.make_async_copy(src.at[pl.ds(pl.multiple_of(step * depth, depth), depth), :], wbuf.at[slot, :, pl.ds(at, src.shape[1])], w_sem.at[slot, i])
    for i in range(3):
        w_load(0, 0, i).start()
    pl.semaphore_wait(barrier, n - 1)

    tail = min(2 * group, max(first * group - over, 0))
    cut = first * group - tail
    parts = {}
    for a in (0, 1):
        parts[a, 'first'] = (over_a.at[a], 0, 0, over)
        if nst:
            parts[a, 'mixed'] = (staged.at[a], 0, first * group, nst * group)
        if cut > over:
            parts[a, 'plain'] = (ins[a], over, over, cut - over)
        if tail:
            parts[a, 'tail'] = (ins[a], cut, cut, tail)
    index = {key: i for i, key in enumerate(parts)}
    order = (2, 6, 3, 5, 4, 7, 1)

    def send(key, d):
        src, at, to, size = parts[key]
        peer = lax.rem(me + d, n)
        return pltpu.make_async_remote_copy(
            src_ref=src.at[peer, pl.ds(at, size)], dst_ref=outs[key[0]].at[me, pl.ds(to, size)],
            send_sem=send_sem.at[d, index[key]], recv_sem=recv_sem.at[d, index[key]], device_id={'sh': peer}, device_id_type=MESH)

    def own(key):
        src, at, to, size = parts[key]
        return pltpu.make_async_copy(src.at[me, pl.ds(at, size)], outs[key[0]].at[me, pl.ds(to, size)], own_sem.at[index[key]])

    def launch(key):
        if key in parts:
            for d in order:
                send(key, d).start()
            own(key).start()

    def arrived(key):
        if key in parts:
            own(key).wait()
            for d in order:
                send(key, d).wait_recv()

    launch((0, 'plain'))
    launch((0, 'tail'))
    for a in (0, 1):
        for e in (0, 1):
            over_load(a, e).wait()

        def put_first(r, c):
            slot = lax.broadcasted_iota(jnp.int32, over_a.shape[2:], 0)
            over_a[a, r] = jnp.where(slot < len_ref[r] - WINDOW, over_b[a, r], over_a[a, r])
            return c
        lax.fori_loop(0, n, put_first, 0)
        if nst:
            own_load(a).wait()
            other_load(a).wait()

            def put_mixed(i, c):
                r, j = lax.div(i, nst), lax.rem(i, nst)
                blocks = lax.div(jnp.minimum(len_ref[r], WINDOW) + group - 1, group)
                other = kv_buf[r + 1 - 2 * lax.rem(r, 2), pl.ds(pl.multiple_of((a * nst + nst - 1 - j) * group, group), group), :]
                at = pl.ds(pl.multiple_of(j * group, group), group)
                staged[a, r, at, :] = jnp.where(first + j < blocks, staged[a, r, at, :], other)
                return c
            lax.fori_loop(0, n * nst, put_mixed, 0)
    launch((0, 'mixed'))
    launch((0, 'first'))
    launch((1, 'mixed'))
    launch((1, 'first'))
    launch((1, 'plain'))
    launch((1, 'tail'))

    x = x_ref[...].astype(jnp.float32)
    inv_rms = lax.rsqrt(jnp.mean(x * x, axis=-1, keepdims=True) + EPS)
    normed[...] = (x * inv_rms * g_ref[...].astype(jnp.float32)).astype(normed.dtype)
    proj[...] = jnp.zeros_like(proj)
    strip = 1024

    def project(step, c):
        slot = lax.rem(step, 2)

        @pl.when(step + 1 < wsteps)
        def _():
            for i in range(3):
                w_load(step + 1, 1 - slot, i).start()
        for i in range(3):
            w_load(step, slot, i).wait()
        h = normed[:, pl.ds(pl.multiple_of(step * depth, depth), depth)]

        def one(s, c):
            at = pl.ds(pl.multiple_of(s * strip, strip), strip)
            proj[:, at] += jnp.dot(h, wbuf[slot, :, at], preferred_element_type=jnp.float32)
            return c
        return lax.fori_loop(0, wide // strip, one, c)
    lax.fori_loop(0, wsteps, project, 0)
    for j in range(wide // head_dim):
        proj2[pl.ds(j, 1), :] = proj[:, pl.ds(j * head_dim, head_dim)]
    cos_row, sin_row = cos_ref[pl.ds(me, 1), :], sin_ref[pl.ds(me, 1), :]

    def turn(value):
        value = value.astype(jnp.bfloat16).astype(jnp.float32)
        return (value * cos_row + pltpu.roll(value, head_dim // 2, 1) * sin_row).astype(jnp.bfloat16)
    nq = heads * q_group
    turned = turn(proj2[pl.ds(0, nq), :])
    for h in range(heads):
        q_heads[h] = turned[h * q_group:(h + 1) * q_group]
    k_turned = turn(proj2[pl.ds(nq, heads), :])
    k_new[...] = k_turned
    for h in range(heads):
        k_rows32[h] = k_turned[h:h + 1].astype(jnp.float32)
    v_new[...] = proj2[pl.ds(nq + heads, heads), :].astype(jnp.bfloat16)

    def forward(a, head, j):
        return pltpu.make_async_remote_copy(
            src_ref=outs[a].at[head, pl.ds(pl.multiple_of(j * group, group), group)],
            dst_ref=outs[a].at[head, pl.ds(pl.multiple_of((2 * half - 1 - j) * group, group), group)],
            send_sem=fsend_sem.at[a], recv_sem=frecv_sem.at[a], device_id={'sh': mate}, device_id_type=MESH)

    def pass_on(a):
        for d in (0, 7, 1, 2, 6, 3, 5, 4):
            if d == 0:
                own((a, 'mixed')).wait()
            else:
                send((a, 'mixed'), d).wait_recv()
            head = lax.rem(me - d + n, n)

            def go(j, c):
                forward(a, head, j).start()
                return c
            lax.fori_loop(first, half, go, 0)

    def passed(a):
        return pltpu.make_async_remote_copy(
            src_ref=outs[a].at[:, pl.ds(first * group, nst * group)], dst_ref=outs[a].at[:, pl.ds(half * group, nst * group)],
            send_sem=fsend_sem.at[a], recv_sem=frecv_sem.at[a], device_id={'sh': mate}, device_id_type=MESH)

    def load(a, lo, hi):
        copy = pltpu.make_async_copy(outs[a].at[:, pl.ds(lo, hi - lo)], kv_buf.at[:, pl.ds(lo, hi - lo)], kv_sem)
        copy.start()
        copy.wait()

    piece = group

    def each(lo, hi, step):
        count = (hi - lo) // piece

        def one(i, c):
            step(lax.div(i, count), pl.ds(pl.multiple_of(lo + lax.rem(i, count) * piece, piece), piece))
            return c
        lax.fori_loop(0, heads * count, one, 0)

    def score(lo, hi):
        load(0, lo, hi)

        def step(h, at):
            scores[h, :, at] = lax.dot_general(q_heads[h], kv_buf[h, at, :], (((1,), (1,)), ((), ())), preferred_element_type=jnp.float32)
        each(lo, hi, step)

    def gather(lo, hi):
        load(1, lo, hi)

        def step(h, at):
            acc[h] += jnp.dot(probs[h, :, at], kv_buf[h, at, :], preferred_element_type=jnp.float32)
        each(lo, hi, step)

    arrived((0, 'plain'))
    arrived((0, 'tail'))
    if first * group > over:
        score(over, first * group)
    if nst:
        pass_on(0)
        score(first * group, half * group)
    arrived((0, 'first'))
    score(0, over)
    if nst:
        passed(0).wait_recv()
        score(half * group, WINDOW)

    length = len_ref[me]
    fresh = lax.rem(length, WINDOW)

    def soften(h, c):
        slot = lax.broadcasted_iota(jnp.int32, (q_group, WINDOW), 1)
        s_new = jnp.sum(q_heads[h].astype(jnp.float32) * k_rows32[h], axis=-1, keepdims=True)
        s = jnp.where(slot == fresh, s_new, scores[h]) / head_dim ** 0.5
        s = jnp.where(slot <= length, s, -jnp.inf)
        e = jnp.exp(s - jnp.max(s, axis=-1, keepdims=True))
        p = e / jnp.sum(e, axis=-1, keepdims=True)
        p_new[h] = jnp.broadcast_to(jnp.sum(jnp.where(slot == fresh, p, 0.0), axis=-1, keepdims=True), (q_group, head_dim))
        probs[h] = jnp.where(slot == fresh, 0.0, p).astype(probs.dtype)
        acc[h] = jnp.zeros_like(acc[h])
        return c
    lax.fori_loop(0, heads, soften, 0)

    if nst:
        pass_on(1)
        gather(first * group, half * group)
        passed(1).wait_recv()
        gather(half * group, WINDOW)
    arrived((1, 'first'))
    gather(0, over)
    arrived((1, 'plain'))
    if cut > over:
        gather(over, cut)
    arrived((1, 'tail'))
    if tail:
        gather(cut, cut + tail)
    for h in range(heads):
        o = acc[h] + p_new[h].astype(jnp.bfloat16).astype(jnp.float32) * v_new[pl.ds(h, 1), :].astype(jnp.float32)
        for g in range(q_group):
            flat[:, pl.ds((h * q_group + g) * head_dim, head_dim)] = o[g:g + 1].astype(flat.dtype)
    for key in parts:
        for d in order:
            send(key, d).wait_send()
    if nst:
        for a in (0, 1):
            passed(a).wait_send()


def exchange(n, group, half, lengths, residual, norm_gain, cos_rows, sin_rows, k_rows, v_rows, w_query, w_key, w_value):
    rows, seq, head_dim = k_rows.shape
    over = seq - WINDOW
    kv_heads = w_key.shape[1] // head_dim
    q_group = w_query.shape[1] // w_key.shape[1]
    wide = w_query.shape[1] + w_key.shape[1] + w_value.shape[1]
    depth = 256
    nst = WINDOW // group - half
    bf16, f32 = k_rows.dtype, jnp.float32
    out = jax.ShapeDtypeStruct((n, WINDOW, head_dim), bf16)
    new = jax.ShapeDtypeStruct((kv_heads, head_dim), bf16)
    any_spec = pl.BlockSpec(memory_space=pl.ANY)
    vmem = pl.BlockSpec(memory_space=pltpu.VMEM)
    dma = pltpu.SemaphoreType.DMA
    return pl.pallas_call(
        functools.partial(exchange_kernel, n, group, half),
        out_shape=(out, out, jax.ShapeDtypeStruct((1, w_query.shape[1]), bf16), new, new),
        in_specs=[pl.BlockSpec(memory_space=pltpu.SMEM)] + [vmem] * 4 + [any_spec] * 5,
        out_specs=(any_spec, any_spec, vmem, vmem, vmem),
        scratch_shapes=[
            pltpu.VMEM((2, rows, over, head_dim), bf16), pltpu.VMEM((2, rows, over, head_dim), bf16),
            pltpu.VMEM((2, rows, max(nst, 1) * group, head_dim), bf16),
            pltpu.VMEM((n, WINDOW, head_dim), bf16),
            pltpu.VMEM((2, depth, wide), bf16),
            pltpu.VMEM((1, w_query.shape[0]), bf16), pltpu.VMEM((1, wide), f32), pltpu.VMEM((wide // head_dim, head_dim), f32),
            pltpu.VMEM((kv_heads, q_group, head_dim), bf16),
            pltpu.VMEM((kv_heads, q_group, WINDOW), f32), pltpu.VMEM((kv_heads, q_group, WINDOW), bf16),
            pltpu.VMEM((kv_heads, q_group, head_dim), f32), pltpu.VMEM((kv_heads, q_group, head_dim), f32), pltpu.VMEM((kv_heads, 1, head_dim), f32),
            dma((n, 8)), dma((n, 8)), dma((8,)), dma((2,)), dma((2,)), dma((2, 2)), dma((2, 2)), dma((2, 3)), dma,
        ],
        compiler_params=pltpu.CompilerParams(collective_id=0, has_side_effects=True, vmem_limit_bytes=VMEM_EXCHANGE),
        name=f'exchange{half}',
    )(lengths, residual, norm_gain, cos_rows, sin_rows, k_rows, v_rows, w_query, w_key, w_value)


def finish_kernel(blk, len_ref, k_in, v_in, kn_ref, vn_ref, perm_ref, x_ref, flat_ref, w_ref, k_out, v_out, x_out, total):
    step = pl.program_id(0)
    heads, _, head_dim = k_in.shape
    length = len_ref[0]
    fresh = lax.rem(length, WINDOW)
    part = perm_ref.shape[0] // heads
    base = step * blk
    wblk = w_ref.shape[0]

    @pl.when(step == 0)
    def _():
        total[...] = x_ref[...].astype(jnp.float32)
    at = pl.multiple_of(step * wblk, wblk)
    total[...] += jnp.dot(flat_ref[:, pl.ds(at, wblk)], w_ref[...], preferred_element_type=jnp.float32)

    for src, new, dst in ((k_in, kn_ref, k_out), (v_in, vn_ref, v_out)):
        new_rows = jnp.tile(new[...].astype(jnp.float32), (part, 1))
        for g in range(0, blk // part, 2):
            pair = jnp.concatenate([src[:, pl.ds((g + e) * part, part), :].reshape(heads * part, head_dim) for e in (0, 1)], axis=1)
            mixed = jnp.dot(perm_ref[...], pair, preferred_element_type=jnp.float32)
            for e in (0, 1):
                row = lax.broadcasted_iota(jnp.int32, (heads * part, head_dim), 0) + (base + (g + e) * part) * heads
                value = mixed[:, e * head_dim:(e + 1) * head_dim]
                value = jnp.where(row < length * heads, value, 0.0)
                value = jnp.where((row >= fresh * heads) & (row < (fresh + 1) * heads), new_rows, value)
                dst[pl.ds((g + e) * part * heads, part * heads), :] = value.astype(dst.dtype)

    @pl.when(step == pl.num_programs(0) - 1)
    def _():
        x_out[...] = total[...].astype(x_out.dtype)


def finish(my_len, k_heads, v_heads, k_new, v_new, residual, flat, w_out):
    heads, _, head_dim = k_heads.shape
    width, dim = w_out.shape
    blk, part = 256, 256 // heads
    steps = WINDOW // blk
    row = jnp.arange(part * heads)
    perm = (row[None, :] == (row % heads * part + row // heads)[:, None]).astype(k_heads.dtype)
    cache = jax.ShapeDtypeStruct((WINDOW * heads, head_dim), k_heads.dtype)
    whole = lambda a: pl.BlockSpec(a.shape, lambda i, *_: (0,) * a.ndim)
    return pl.pallas_call(
        functools.partial(finish_kernel, blk),
        grid_spec=pltpu.PrefetchScalarGridSpec(
            num_scalar_prefetch=1, grid=(steps,),
            in_specs=[
                pl.BlockSpec((heads, blk, head_dim), lambda i, *_: (0, i, 0)),
                pl.BlockSpec((heads, blk, head_dim), lambda i, *_: (0, i, 0)),
                whole(k_new), whole(v_new), whole(perm), whole(residual), whole(flat),
                pl.BlockSpec((width // steps, dim), lambda i, *_: (i, 0)),
            ],
            out_specs=[
                pl.BlockSpec((blk * heads, head_dim), lambda i, *_: (i, 0)),
                pl.BlockSpec((blk * heads, head_dim), lambda i, *_: (i, 0)),
                pl.BlockSpec((1, dim), lambda i, *_: (0, 0)),
            ],
            scratch_shapes=[pltpu.VMEM((1, dim), jnp.float32)]),
        out_shape=(cache, cache, jax.ShapeDtypeStruct(residual.shape, residual.dtype)),
        compiler_params=pltpu.CompilerParams(dimension_semantics=('arbitrary',), vmem_limit_bytes=VMEM_FINISH),
        cost_estimate=pl.CostEstimate(flops=10 ** 9, bytes_accessed=64 << 20, transcendentals=0),
        name='finish',
    )(my_len, k_heads, v_heads, k_new, v_new, perm, residual, flat, w_out)


GROUP = 256
VMEM_EXCHANGE = 28 << 20
VMEM_FINISH = 20 << 20


def solution(mesh):
    head_spec = P('dp', None, 'sh', None)
    row_spec = P(('dp', 'sh'))
    full_spec = P(None, None)
    n = mesh.shape['sh']

    def per_device(k_prefill, v_prefill, lengths, residual, norm_gain, w_query, w_key, w_value, w_out):
        num_rows = residual.shape[0]
        rows, seq, _, head_dim = k_prefill.shape
        kv_heads = w_key.shape[1] // head_dim
        half_dim = head_dim // 2
        my_len = lax.dynamic_slice_in_dim(lengths, lax.axis_index('sh') * num_rows, num_rows)
        k_rows = k_prefill.reshape(rows, seq, head_dim)
        v_rows = v_prefill.reshape(rows, seq, head_dim)
        blocks = (jnp.minimum(lengths, WINDOW) + GROUP - 1) // GROUP
        need = (jnp.max(blocks.reshape(-1, 2).sum(axis=1)) + 1) // 2
        level = jnp.maximum(need - levels(GROUP)[0], 0)
        inv_freq = THETA ** (-2.0 * jnp.arange(half_dim, dtype=jnp.float32) / head_dim)
        angles = lengths.astype(jnp.float32)[:, None] * inv_freq
        cos_rows = jnp.concatenate([jnp.cos(angles), jnp.cos(angles)], axis=1)
        sin_rows = jnp.concatenate([-jnp.sin(angles), jnp.sin(angles)], axis=1)
        k_heads, v_heads, flat, k_new, v_new = lax.switch(
            level, [functools.partial(exchange, n, GROUP, half) for half in levels(GROUP)],
            lengths, residual, norm_gain[None], cos_rows, sin_rows, k_rows, v_rows, w_query, w_key, w_value)
        k_cache, v_cache, resid_out = finish(my_len, k_heads, v_heads, k_new, v_new, residual, flat, w_out)
        cache_shape = (num_rows, WINDOW, kv_heads, head_dim)
        return resid_out, k_cache.reshape(cache_shape), v_cache.reshape(cache_shape)
    return jax.shard_map(per_device, mesh=mesh, in_specs=(head_spec, head_spec, P('dp'), P(('dp', 'sh'), None), P(None), full_spec, full_spec, full_spec, full_spec), out_specs=(P(('dp', 'sh'), None), row_spec, row_spec), check_vma=False)
```

```python
import functools

import jax
import jax.numpy as jnp
from jax import lax
from jax.experimental import pallas as pl
from jax.experimental.pallas import tpu as pltpu
from jax.sharding import PartitionSpec as P

WINDOW = 4096
THETA = 10000.0
EPS = 1e-5
MESH = pl.DeviceIdType.MESH


def levels(group):
    nblk = WINDOW // group
    return tuple(range(nblk // 2 + 1, nblk + 1))


def exchange_kernel(n, group, half, len_ref, x_ref, g_ref, cos_ref, sin_ref, k_in, v_in, wq, wk, wv, wo,
                    k_out, v_out, k_mid, v_mid, flat, wo_keep,
                    over_a, over_b, staged, kv_buf, wbuf, normed, proj, proj2, q_heads, scores, probs, p_new, acc, new32, perm, obuf,
                    send_sem, recv_sem, own_sem, fsend_sem, frecv_sem, over_sem, stage_sem, w_sem, kv_sem, o_sem, wo_sem):
    me = lax.axis_index('sh')
    mate = me + 1 - 2 * lax.rem(me, 2)
    heads, q_group, head_dim = q_heads.shape
    over = over_a.shape[2]
    nblk = WINDOW // group
    first = 2 * half - nblk
    nst = half - first
    barrier = pltpu.get_barrier_semaphore()
    for d in range(1, n):
        pl.semaphore_signal(barrier, inc=1, device_id={'sh': lax.rem(me + d, n)}, device_id_type=MESH)

    ins, outs, mids = (k_in, v_in), (k_out, v_out), (k_mid, v_mid)

    def over_load(a, e):
        return pltpu.make_async_copy(ins[a].at[:, pl.ds(e * WINDOW, over)], (over_a, over_b)[e].at[a], over_sem.at[a, e])

    def own_load(a):
        return pltpu.make_async_copy(ins[a].at[:, pl.ds(first * group, nst * group)], staged.at[a], stage_sem.at[a, 0])

    def other_load(a):
        return pltpu.make_async_copy(ins[a].at[:, pl.ds(half * group, nst * group)], kv_buf.at[:, pl.ds(a * nst * group, nst * group)], stage_sem.at[a, 1])
    for a in (0, 1):
        if nst:
            own_load(a).start()
            other_load(a).start()
        for e in (0, 1):
            over_load(a, e).start()
    depth, wide = wbuf.shape[1], wbuf.shape[2]
    wsteps = wq.shape[0] // depth
    weights = ((wq, 0), (wk, wq.shape[1]), (wv, wq.shape[1] + wk.shape[1]))

    def w_load(step, slot, i):
        src, at = weights[i]
        return pltpu.make_async_copy(src.at[pl.ds(pl.multiple_of(step * depth, depth), depth), :], wbuf.at[slot, :, pl.ds(at, src.shape[1])], w_sem.at[slot, i])
    for i in range(3):
        w_load(0, 0, i).start()
    pl.semaphore_wait(barrier, n - 1)

    tail = min(group, max(first * group - over, 0))
    cut = first * group - tail
    parts = {}
    for a in (0, 1):
        parts[a, 'first'] = (over_a.at[a], 0, 0, over)
        if nst:
            parts[a, 'mixed'] = (staged.at[a], 0, first * group, nst * group)
        if cut > over:
            parts[a, 'plain'] = (ins[a], over, over, cut - over)
        if tail:
            parts[a, 'tail'] = (ins[a], cut, cut, tail)
    index = {key: i for i, key in enumerate(parts)}
    order = (2, 6, 3, 5, 4, 7, 1)

    def send(key, d):
        src, at, to, size = parts[key]
        peer = lax.rem(me + d, n)
        return pltpu.make_async_remote_copy(
            src_ref=src.at[peer, pl.ds(at, size)], dst_ref=outs[key[0]].at[me, pl.ds(to, size)],
            send_sem=send_sem.at[d, index[key]], recv_sem=recv_sem.at[d, index[key]], device_id={'sh': peer}, device_id_type=MESH)

    def own(key):
        src, at, to, size = parts[key]
        return pltpu.make_async_copy(src.at[me, pl.ds(at, size)], outs[key[0]].at[me, pl.ds(to, size)], own_sem.at[index[key]])

    def launch(key):
        if key in parts:
            for d in order:
                send(key, d).start()
            own(key).start()

    def arrived(key):
        if key in parts:
            own(key).wait()
            for d in order:
                send(key, d).wait_recv()

    launch((0, 'plain'))
    launch((0, 'tail'))
    for a in (0, 1):
        for e in (0, 1):
            over_load(a, e).wait()

        def put_first(r, c):
            slot = lax.broadcasted_iota(jnp.int32, over_a.shape[2:], 0)
            over_a[a, r] = jnp.where(slot < len_ref[r] - WINDOW, over_b[a, r], over_a[a, r])
            return c
        lax.fori_loop(0, n, put_first, 0)
        if nst:
            own_load(a).wait()
            other_load(a).wait()

            def put_mixed(i, c):
                r, j = lax.div(i, nst), lax.rem(i, nst)
                blocks = lax.div(jnp.minimum(len_ref[r], WINDOW) + group - 1, group)
                other = kv_buf[r + 1 - 2 * lax.rem(r, 2), pl.ds(pl.multiple_of((a * nst + nst - 1 - j) * group, group), group), :]
                at = pl.ds(pl.multiple_of(j * group, group), group)
                staged[a, r, at, :] = jnp.where(first + j < blocks, staged[a, r, at, :], other)
                return c
            lax.fori_loop(0, n * nst, put_mixed, 0)
    launch((0, 'mixed'))
    launch((0, 'first'))
    launch((1, 'mixed'))
    launch((1, 'first'))
    launch((1, 'plain'))
    launch((1, 'tail'))

    x = x_ref[...].astype(jnp.float32)
    inv_rms = lax.rsqrt(jnp.mean(x * x, axis=-1, keepdims=True) + EPS)
    for j in range(x.shape[1] // head_dim):
        at = pl.ds(j * head_dim, head_dim)
        normed[:, at] = (x_ref[:, at].astype(jnp.float32) * inv_rms * g_ref[pl.ds(j, 1), :].astype(jnp.float32)).astype(normed.dtype)
    proj[...] = jnp.zeros_like(proj)
    strip = 1024

    def project(step, c):
        slot = lax.rem(step, 2)

        @pl.when(step + 1 < wsteps)
        def _():
            for i in range(3):
                w_load(step + 1, 1 - slot, i).start()
        for i in range(3):
            w_load(step, slot, i).wait()
        h = normed[:, pl.ds(pl.multiple_of(step * depth, depth), depth)]

        def one(s, c):
            at = pl.ds(pl.multiple_of(s * strip, strip), strip)
            proj[:, at] += jnp.dot(h, wbuf[slot, :, at], preferred_element_type=jnp.float32)
            return c
        return lax.fori_loop(0, wide // strip, one, c)
    lax.fori_loop(0, wsteps, project, 0)
    keep = pltpu.make_async_copy(wo, wo_keep, wo_sem)
    keep.start()
    for j in range(wide // head_dim):
        proj2[pl.ds(j, 1), :] = proj[:, pl.ds(j * head_dim, head_dim)]
    cos_row, sin_row = cos_ref[pl.ds(me, 1), :], sin_ref[pl.ds(me, 1), :]

    def turn(value):
        value = value.astype(jnp.bfloat16).astype(jnp.float32)
        return (value * cos_row + pltpu.roll(value, head_dim // 2, 1) * sin_row).astype(jnp.bfloat16)
    nq = heads * q_group
    turned = turn(proj2[pl.ds(0, nq), :])
    for h in range(heads):
        q_heads[h] = turned[h * q_group:(h + 1) * q_group]
    new32[0] = turn(proj2[pl.ds(nq, heads), :]).astype(jnp.float32)
    new32[1] = proj2[pl.ds(nq + heads, heads), :].astype(jnp.bfloat16).astype(jnp.float32)
    part = perm.shape[0] // heads
    row = lax.broadcasted_iota(jnp.int32, perm.shape, 0)
    col = lax.broadcasted_iota(jnp.int32, perm.shape, 1)
    perm[...] = jnp.where(col == lax.rem(row, heads) * part + lax.div(row, heads), 1.0, 0.0).astype(perm.dtype)

    def forward(a, head, j):
        return pltpu.make_async_remote_copy(
            src_ref=outs[a].at[head, pl.ds(pl.multiple_of(j * group, group), group)],
            dst_ref=outs[a].at[head, pl.ds(pl.multiple_of((2 * half - 1 - j) * group, group), group)],
            send_sem=fsend_sem.at[a], recv_sem=frecv_sem.at[a], device_id={'sh': mate}, device_id_type=MESH)

    def pass_on(a):
        for d in (0, 7, 1, 2, 6, 3, 5, 4):
            if d == 0:
                own((a, 'mixed')).wait()
            else:
                send((a, 'mixed'), d).wait_recv()
            head = lax.rem(me - d + n, n)

            def go(j, c):
                forward(a, head, j).start()
                return c
            lax.fori_loop(first, half, go, 0)

    def passed(a):
        return pltpu.make_async_remote_copy(
            src_ref=outs[a].at[:, pl.ds(first * group, nst * group)], dst_ref=outs[a].at[:, pl.ds(half * group, nst * group)],
            send_sem=fsend_sem.at[a], recv_sem=frecv_sem.at[a], device_id={'sh': mate}, device_id_type=MESH)

    length = len_ref[me]
    fresh = lax.rem(length, WINDOW)
    piece = group

    def put(a, at, parity):
        rows = piece * heads
        return pltpu.make_async_copy(obuf.at[parity], mids[a].at[pl.ds(pl.multiple_of(at * heads, rows), rows), :], o_sem.at[parity])

    def walk(a):
        def fetch(lo, hi):
            copy = pltpu.make_async_copy(outs[a].at[:, pl.ds(lo, hi - lo)], kv_buf.at[:, pl.ds(lo, hi - lo)], kv_sem)
            copy.start()
            copy.wait()

        def get(key):
            arrived(key)
            _, _, lo, size = parts[key]
            fetch(lo, lo + size)

        def get_mixed():
            pass_on(a)
            fetch(first * group, half * group)

        def get_passed():
            passed(a).wait_recv()
            fetch(half * group, WINDOW)
        due = {}
        if nst:
            due[0] = get_mixed
            due[nst] = get_passed
        due[nblk - first] = functools.partial(get, (a, 'first'))
        if (a, 'plain') in parts:
            due[nblk - first + over // group] = functools.partial(get, (a, 'plain'))
        if (a, 'tail') in parts:
            due[nblk - first + cut // group] = functools.partial(get, (a, 'tail'))

        def one(i, c):
            for at_step, action in due.items():
                pl.when(i == at_step)(action)
            base = pl.multiple_of(lax.rem(first + i, nblk) * piece, piece)
            at = pl.ds(base, piece)
            parity = lax.rem(i, 2)

            @pl.when(i >= 2)
            def _():
                put(a, base, parity).wait()
            for h in range(heads):
                if a == 0:
                    scores[h, :, at] = lax.dot_general(q_heads[h], kv_buf[h, at, :], (((1,), (1,)), ((), ())), preferred_element_type=jnp.float32)
                else:
                    acc[h] += jnp.dot(probs[h, :, at], kv_buf[h, at, :], preferred_element_type=jnp.float32)
            new_rows = jnp.tile(new32[a], (part, 1))
            for g in range(0, piece // part, 2):
                pair = jnp.concatenate([kv_buf[:, pl.ds(base + (g + e) * part, part), :].reshape(heads * part, head_dim) for e in (0, 1)], axis=1)
                mixed = jnp.dot(perm[...], pair, preferred_element_type=jnp.float32)
                for e in (0, 1):
                    row = lax.broadcasted_iota(jnp.int32, (heads * part, head_dim), 0) + (base + (g + e) * part) * heads
                    value = mixed[:, e * head_dim:(e + 1) * head_dim]
                    value = jnp.where(row < length * heads, value, 0.0)
                    value = jnp.where((row >= fresh * heads) & (row < (fresh + 1) * heads), new_rows, value)
                    obuf[parity, pl.ds((g + e) * part * heads, part * heads), :] = value.astype(obuf.dtype)
            put(a, base, parity).start()
            return c
        lax.fori_loop(0, nblk, one, 0)

        def drain():
            for i in range(nblk - 2, nblk):
                put(a, (first + i) % nblk * piece, i % 2).wait()
        return drain

    walk(0)()

    def soften(h, c):
        slot = lax.broadcasted_iota(jnp.int32, (q_group, WINDOW), 1)
        s_key = new32[0, pl.ds(h, 1), :]
        s_new = jnp.sum(q_heads[h].astype(jnp.float32) * s_key, axis=-1, keepdims=True)
        s = jnp.where(slot == fresh, s_new, scores[h]) / head_dim ** 0.5
        s = jnp.where(slot <= length, s, -jnp.inf)
        e = jnp.exp(s - jnp.max(s, axis=-1, keepdims=True))
        p = e / jnp.sum(e, axis=-1, keepdims=True)
        p_new[h] = jnp.broadcast_to(jnp.sum(jnp.where(slot == fresh, p, 0.0), axis=-1, keepdims=True), (q_group, head_dim))
        probs[h] = jnp.where(slot == fresh, 0.0, p).astype(probs.dtype)
        acc[h] = jnp.zeros_like(acc[h])
        return c
    lax.fori_loop(0, heads, soften, 0)

    last = walk(1)
    for h in range(heads):
        o = acc[h] + p_new[h].astype(jnp.bfloat16).astype(jnp.float32) * new32[1, pl.ds(h, 1), :]
        for g in range(q_group):
            flat[:, pl.ds((h * q_group + g) * head_dim, head_dim)] = o[g:g + 1].astype(flat.dtype)
    last()
    keep.wait()
    for key in parts:
        for d in order:
            send(key, d).wait_send()
    if nst:
        for a in (0, 1):
            passed(a).wait_send()


def exchange(n, group, half, lengths, residual, norm_gain, cos_rows, sin_rows, k_rows, v_rows, w_query, w_key, w_value, w_out):
    rows, seq, head_dim = k_rows.shape
    over = seq - WINDOW
    kv_heads = w_key.shape[1] // head_dim
    q_group = w_query.shape[1] // w_key.shape[1]
    wide = w_query.shape[1] + w_key.shape[1] + w_value.shape[1]
    depth = 128
    nst = WINDOW // group - half
    bf16, f32 = k_rows.dtype, jnp.float32
    out = jax.ShapeDtypeStruct((n, WINDOW, head_dim), bf16)
    mid = pltpu.HBM((WINDOW * kv_heads, head_dim), bf16)
    any_spec = pl.BlockSpec(memory_space=pl.ANY)
    vmem = pl.BlockSpec(memory_space=pltpu.VMEM)
    hbm = pl.BlockSpec(memory_space=pltpu.HBM)
    dma = pltpu.SemaphoreType.DMA
    return pl.pallas_call(
        functools.partial(exchange_kernel, n, group, half),
        out_shape=(out, out, mid, mid, pltpu.VMEM((1, w_query.shape[1]), bf16), pltpu.VMEM(w_out.shape, bf16)),
        in_specs=[pl.BlockSpec(memory_space=pltpu.SMEM)] + [vmem] * 4 + [any_spec] * 6,
        out_specs=(any_spec,) * 2 + (hbm,) * 2 + (vmem, vmem),
        scratch_shapes=[
            pltpu.VMEM((2, rows, over, head_dim), bf16), pltpu.VMEM((2, rows, over, head_dim), bf16),
            pltpu.VMEM((2, rows, max(nst, 1) * group, head_dim), bf16),
            pltpu.VMEM((n, WINDOW, head_dim), bf16),
            pltpu.VMEM((2, depth, wide), bf16),
            pltpu.VMEM((1, w_query.shape[0]), bf16), pltpu.VMEM((1, wide), f32), pltpu.VMEM((wide // head_dim, head_dim), f32),
            pltpu.VMEM((kv_heads, q_group, head_dim), bf16),
            pltpu.VMEM((kv_heads, q_group, WINDOW), f32), pltpu.VMEM((kv_heads, q_group, WINDOW), bf16),
            pltpu.VMEM((kv_heads, q_group, head_dim), f32), pltpu.VMEM((kv_heads, q_group, head_dim), f32), pltpu.VMEM((2, kv_heads, head_dim), f32),
            pltpu.VMEM((256, 256), bf16), pltpu.VMEM((2, group * kv_heads, head_dim), bf16),
            dma((n, 8)), dma((n, 8)), dma((8,)), dma((2,)), dma((2,)), dma((2, 2)), dma((2, 2)), dma((2, 3)), dma, dma((2,)), dma,
        ],
        compiler_params=pltpu.CompilerParams(collective_id=0, has_side_effects=True, vmem_limit_bytes=VMEM_EXCHANGE),
        cost_estimate=pl.CostEstimate(flops=10 ** 11, bytes_accessed=128 << 20, transcendentals=0),
        name=f'exchange{half}',
    )(lengths, residual, norm_gain, cos_rows, sin_rows, k_rows, v_rows, w_query, w_key, w_value, w_out)[2:]


def finish_kernel(k_in, v_in, x_ref, flat_ref, w_ref, k_out, v_out, x_out, bufs, total, in_sem, out_sem):
    count, size = bufs.shape[:2]
    each = count // 2
    strip = w_ref.shape[0] // count

    def read(i):
        src = (k_in, v_in)[i // each]
        return pltpu.make_async_copy(src.at[pl.ds(i % each * size, size), :], bufs.at[i], in_sem.at[i])

    def write(i):
        dst = (k_out, v_out)[i // each]
        return pltpu.make_async_copy(bufs.at[i], dst.at[pl.ds(i % each * size, size), :], out_sem.at[i])
    for i in range(count):
        read(i).start()
    total[...] = x_ref[...].astype(jnp.float32)
    for i in range(count):
        read(i).wait()
        write(i).start()

        def one(t, c):
            at = pl.ds(pl.multiple_of(t * 1024, 1024), 1024)
            total[:, at] += jnp.dot(flat_ref[:, pl.ds(i * strip, strip)], w_ref[pl.ds(i * strip, strip), at], preferred_element_type=jnp.float32)
            return c
        lax.fori_loop(0, w_ref.shape[1] // 1024, one, 0)
    x_out[...] = total[...].astype(x_out.dtype)
    for i in range(count):
        write(i).wait()


def finish(k_mid, v_mid, flat, residual, w_out):
    size, head_dim = k_mid.shape
    width, dim = w_out.shape
    count = 16
    cache = jax.ShapeDtypeStruct(k_mid.shape, k_mid.dtype)
    hbm = pl.BlockSpec(memory_space=pltpu.HBM)
    vmem = pl.BlockSpec(memory_space=pltpu.VMEM)
    return pl.pallas_call(
        finish_kernel,
        in_specs=[hbm, hbm, vmem, vmem, vmem],
        out_specs=[hbm, hbm, vmem],
        scratch_shapes=[pltpu.VMEM((count, 2 * size // count, head_dim), k_mid.dtype), pltpu.VMEM((1, dim), jnp.float32), pltpu.SemaphoreType.DMA((count,)), pltpu.SemaphoreType.DMA((count,))],
        out_shape=(cache, cache, jax.ShapeDtypeStruct(residual.shape, residual.dtype)),
        compiler_params=pltpu.CompilerParams(vmem_limit_bytes=VMEM_FINISH),
        cost_estimate=pl.CostEstimate(flops=10 ** 9, bytes_accessed=64 << 20, transcendentals=0),
        name='finish',
    )(pltpu.with_memory_space_constraint(k_mid, pltpu.HBM), pltpu.with_memory_space_constraint(v_mid, pltpu.HBM), residual, pltpu.with_memory_space_constraint(flat, pltpu.VMEM), pltpu.with_memory_space_constraint(w_out, pltpu.VMEM))


GROUP = 256
VMEM_EXCHANGE = 27 << 20
VMEM_FINISH = 20 << 20


def solution(mesh):
    head_spec = P('dp', None, 'sh', None)
    row_spec = P(('dp', 'sh'))
    full_spec = P(None, None)
    n = mesh.shape['sh']

    def per_device(k_prefill, v_prefill, lengths, residual, norm_gain, w_query, w_key, w_value, w_out):
        num_rows = residual.shape[0]
        rows, seq, _, head_dim = k_prefill.shape
        kv_heads = w_key.shape[1] // head_dim
        half_dim = head_dim // 2
        k_rows = k_prefill.reshape(rows, seq, head_dim)
        v_rows = v_prefill.reshape(rows, seq, head_dim)
        blocks = (jnp.minimum(lengths, WINDOW) + GROUP - 1) // GROUP
        need = (jnp.max(blocks.reshape(-1, 2).sum(axis=1)) + 1) // 2
        level = jnp.maximum(need - levels(GROUP)[0], 0)
        inv_freq = THETA ** (-2.0 * jnp.arange(half_dim, dtype=jnp.float32) / head_dim)
        angles = lengths.astype(jnp.float32)[:, None] * inv_freq
        cos_rows = jnp.concatenate([jnp.cos(angles), jnp.cos(angles)], axis=1)
        sin_rows = jnp.concatenate([-jnp.sin(angles), jnp.sin(angles)], axis=1)
        k_mid, v_mid, flat, w_keep = lax.switch(
            level, [functools.partial(exchange, n, GROUP, half) for half in levels(GROUP)],
            lengths, residual, norm_gain.reshape(-1, head_dim), cos_rows, sin_rows, k_rows, v_rows, w_query, w_key, w_value, w_out)
        k_cache, v_cache, resid_out = finish(k_mid, v_mid, flat, residual, w_keep)
        cache_shape = (num_rows, WINDOW, kv_heads, head_dim)
        return resid_out, k_cache.reshape(cache_shape), v_cache.reshape(cache_shape)
    return jax.shard_map(per_device, mesh=mesh, in_specs=(head_spec, head_spec, P('dp'), P(('dp', 'sh'), None), P(None), full_spec, full_spec, full_spec, full_spec), out_specs=(P(('dp', 'sh'), None), row_spec, row_spec), check_vma=False)
```

```python
import functools

import jax
import jax.numpy as jnp
from jax import lax
from jax.experimental import pallas as pl
from jax.experimental.pallas import tpu as pltpu
from jax.sharding import PartitionSpec as P

WINDOW = 4096
THETA = 10000.0
EPS = 1e-5
MESH = pl.DeviceIdType.MESH


def levels(group):
    nblk = WINDOW // group
    return tuple(range(nblk // 2 + 1, nblk + 1))


def exchange_kernel(n, group, half, len_ref, x_ref, g_ref, cos_ref, sin_ref, k_in, v_in, wq, wk, wv, wo,
                    k_out, v_out, k_mid, v_mid, flat, wo_keep,
                    over_a, over_b, staged, kv_buf, wbuf, normed, proj, proj2, q_heads, scores, probs, p_new, acc, new32, perm, obuf,
                    send_sem, recv_sem, own_sem, fsend_sem, frecv_sem, over_sem, stage_sem, w_sem, kv_sem, o_sem, wo_sem):
    me = lax.axis_index('sh')
    mate = me + 1 - 2 * lax.rem(me, 2)
    heads, q_group, head_dim = q_heads.shape
    over = over_a.shape[2]
    nblk = WINDOW // group
    first = 2 * half - nblk
    nst = half - first
    barrier = pltpu.get_barrier_semaphore()
    for d in range(1, n):
        pl.semaphore_signal(barrier, inc=1, device_id={'sh': lax.rem(me + d, n)}, device_id_type=MESH)

    ins, outs, mids = (k_in, v_in), (k_out, v_out), (k_mid, v_mid)

    def over_load(a, e):
        return pltpu.make_async_copy(ins[a].at[:, pl.ds(e * WINDOW, over)], (over_a, over_b)[e].at[a], over_sem.at[a, e])

    def own_load(a):
        return pltpu.make_async_copy(ins[a].at[:, pl.ds(first * group, nst * group)], staged.at[a], stage_sem.at[a, 0])

    def other_load(a):
        return pltpu.make_async_copy(ins[a].at[:, pl.ds(half * group, nst * group)], kv_buf.at[:, pl.ds(a * nst * group, nst * group)], stage_sem.at[a, 1])
    for a in (0, 1):
        if nst:
            own_load(a).start()
            other_load(a).start()
        for e in (0, 1):
            over_load(a, e).start()
    depth, wide = wbuf.shape[1], wbuf.shape[2]
    wsteps = wq.shape[0] // depth
    weights = ((wq, 0), (wk, wq.shape[1]), (wv, wq.shape[1] + wk.shape[1]))

    def w_load(step, slot, i):
        src, at = weights[i]
        return pltpu.make_async_copy(src.at[pl.ds(pl.multiple_of(step * depth, depth), depth), :], wbuf.at[slot, :, pl.ds(at, src.shape[1])], w_sem.at[slot, i])
    for i in range(3):
        w_load(0, 0, i).start()
    pl.semaphore_wait(barrier, n - 1)

    tail = min(group, max(first * group - over, 0))
    cut = first * group - tail
    parts = {}
    for a in (0, 1):
        parts[a, 'first'] = (over_a.at[a], 0, 0, over)
        if nst:
            parts[a, 'mixed'] = (staged.at[a], 0, first * group, nst * group)
        chunk = 2 * group if a else WINDOW
        for lo in range(over, cut, chunk):
            parts[a, 'plain', lo] = (ins[a], lo, lo, min(chunk, cut - lo))
        if tail:
            parts[a, 'tail'] = (ins[a], cut, cut, tail)
    index = {key: i for i, key in enumerate(parts)}

    def send(key, d):
        src, at, to, size = parts[key]
        peer = lax.rem(me + d, n)
        return pltpu.make_async_remote_copy(
            src_ref=src.at[peer, pl.ds(at, size)], dst_ref=outs[key[0]].at[me, pl.ds(to, size)],
            send_sem=send_sem.at[d, index[key]], recv_sem=recv_sem.at[d, index[key]], device_id={'sh': peer}, device_id_type=MESH)

    def own(key):
        src, at, to, size = parts[key]
        return pltpu.make_async_copy(src.at[me, pl.ds(at, size)], outs[key[0]].at[me, pl.ds(to, size)], own_sem.at[index[key]])

    def launch(key):
        if key in parts:
            def go(d, c):
                send(key, d).start()
                return c
            lax.fori_loop(1, n, go, 0)
            own(key).start()

    def launch_plain(a):
        for key in parts:
            if key[0] == a and key[1] in ('plain', 'tail'):
                launch(key)

    def arrived(key):
        if key in parts:
            own(key).wait()

            def go(d, c):
                send(key, d).wait_recv()
                return c
            lax.fori_loop(1, n, go, 0)

    launch_plain(0)
    for a in (0, 1):
        for e in (0, 1):
            over_load(a, e).wait()

        def put_first(r, c):
            slot = lax.broadcasted_iota(jnp.int32, over_a.shape[2:], 0)
            over_a[a, r] = jnp.where(slot < len_ref[r] - WINDOW, over_b[a, r], over_a[a, r])
            return c
        lax.fori_loop(0, n, put_first, 0)
        if nst:
            own_load(a).wait()
            other_load(a).wait()

            def put_mixed(i, c):
                r, j = lax.div(i, nst), lax.rem(i, nst)
                blocks = lax.div(jnp.minimum(len_ref[r], WINDOW) + group - 1, group)
                other = kv_buf[r + 1 - 2 * lax.rem(r, 2), pl.ds(pl.multiple_of((a * nst + nst - 1 - j) * group, group), group), :]
                at = pl.ds(pl.multiple_of(j * group, group), group)
                staged[a, r, at, :] = jnp.where(first + j < blocks, staged[a, r, at, :], other)
                return c
            lax.fori_loop(0, n * nst, put_mixed, 0)
    launch((0, 'mixed'))
    launch((0, 'first'))
    launch((1, 'mixed'))
    launch((1, 'first'))
    launch_plain(1)

    x = x_ref[...].astype(jnp.float32)
    inv_rms = lax.rsqrt(jnp.mean(x * x, axis=-1, keepdims=True) + EPS)
    for j in range(x.shape[1] // head_dim):
        at = pl.ds(j * head_dim, head_dim)
        normed[:, at] = (x_ref[:, at].astype(jnp.float32) * inv_rms * g_ref[pl.ds(j, 1), :].astype(jnp.float32)).astype(normed.dtype)
    proj[...] = jnp.zeros_like(proj)
    strip = 1024

    def project(step, c):
        slot = lax.rem(step, 2)

        @pl.when(step + 1 < wsteps)
        def _():
            for i in range(3):
                w_load(step + 1, 1 - slot, i).start()
        for i in range(3):
            w_load(step, slot, i).wait()
        h = normed[:, pl.ds(pl.multiple_of(step * depth, depth), depth)]

        for lo in range(0, wide, strip):
            proj[:, pl.ds(lo, strip)] += jnp.dot(h, wbuf[slot, :, pl.ds(lo, strip)], preferred_element_type=jnp.float32)
        return c
    lax.fori_loop(0, wsteps, project, 0)
    keep = pltpu.make_async_copy(wo, wo_keep, wo_sem)
    keep.start()
    for j in range(wide // head_dim):
        proj2[pl.ds(j, 1), :] = proj[:, pl.ds(j * head_dim, head_dim)]
    cos_row, sin_row = cos_ref[pl.ds(me, 1), :], sin_ref[pl.ds(me, 1), :]

    def turn(value):
        value = value.astype(jnp.bfloat16).astype(jnp.float32)
        return (value * cos_row + pltpu.roll(value, head_dim // 2, 1) * sin_row).astype(jnp.bfloat16)
    nq = heads * q_group
    turned = turn(proj2[pl.ds(0, nq), :])
    for h in range(heads):
        q_heads[h] = turned[h * q_group:(h + 1) * q_group]
    new32[0] = turn(proj2[pl.ds(nq, heads), :]).astype(jnp.float32)
    new32[1] = proj2[pl.ds(nq + heads, heads), :].astype(jnp.bfloat16).astype(jnp.float32)
    part = perm.shape[0] // heads
    row = lax.broadcasted_iota(jnp.int32, perm.shape, 0)
    col = lax.broadcasted_iota(jnp.int32, perm.shape, 1)
    perm[...] = jnp.where(col == lax.rem(row, heads) * part + lax.div(row, heads), 1.0, 0.0).astype(perm.dtype)

    def forward(a, head, j):
        return pltpu.make_async_remote_copy(
            src_ref=outs[a].at[head, pl.ds(pl.multiple_of(j * group, group), group)],
            dst_ref=outs[a].at[head, pl.ds(pl.multiple_of((2 * half - 1 - j) * group, group), group)],
            send_sem=fsend_sem.at[a], recv_sem=frecv_sem.at[a], device_id={'sh': mate}, device_id_type=MESH)

    def pass_on(a):
        def go_block(d):
            def go(j, c):
                forward(a, lax.rem(me + n - d, n), j).start()
                return c
            lax.fori_loop(first, half, go, 0)

        def go_from(d, c):
            send((a, 'mixed'), d).wait_recv()
            go_block(d)
            return c
        own((a, 'mixed')).wait()
        go_block(0)
        lax.fori_loop(1, n, go_from, 0)

    def passed(a):
        return pltpu.make_async_remote_copy(
            src_ref=outs[a].at[:, pl.ds(first * group, nst * group)], dst_ref=outs[a].at[:, pl.ds(half * group, nst * group)],
            send_sem=fsend_sem.at[a], recv_sem=frecv_sem.at[a], device_id={'sh': mate}, device_id_type=MESH)

    length = len_ref[me]
    fresh = lax.rem(length, WINDOW)
    piece = group

    def put(a, at, parity):
        rows = piece * heads
        return pltpu.make_async_copy(obuf.at[parity], mids[a].at[pl.ds(pl.multiple_of(at * heads, rows), rows), :], o_sem.at[parity])

    def walk(a):
        def fetch(lo, hi):
            copy = pltpu.make_async_copy(outs[a].at[:, pl.ds(lo, hi - lo)], kv_buf.at[:, pl.ds(lo, hi - lo)], kv_sem)
            copy.start()
            copy.wait()

        def get(key):
            arrived(key)
            _, _, lo, size = parts[key]
            fetch(lo, lo + size)

        def get_mixed():
            pass_on(a)
            fetch(first * group, half * group)

        def get_passed():
            passed(a).wait_recv()
            fetch(half * group, WINDOW)
        due = {}
        if nst:
            due[0] = get_mixed
            due[nst] = get_passed
        due[nblk - first] = functools.partial(get, (a, 'first'))
        for key in parts:
            if key[0] == a and key[1] in ('plain', 'tail'):
                due[nblk - first + parts[key][2] // group] = functools.partial(get, key)

        def one(i, c):
            for at_step, action in due.items():
                pl.when(i == at_step)(action)
            base = pl.multiple_of(lax.rem(first + i, nblk) * piece, piece)
            at = pl.ds(base, piece)
            parity = lax.rem(i, 2)

            @pl.when(i >= 2)
            def _():
                put(a, base, parity).wait()
            for h in range(heads):
                if a == 0:
                    scores[h, :, at] = lax.dot_general(q_heads[h], kv_buf[h, at, :], (((1,), (1,)), ((), ())), preferred_element_type=jnp.float32)
                else:
                    acc[h] += jnp.dot(probs[h, :, at], kv_buf[h, at, :], preferred_element_type=jnp.float32)
            new_rows = jnp.tile(new32[a], (part, 1))
            for g in range(0, piece // part, 2):
                pair = jnp.concatenate([kv_buf[:, pl.ds(base + (g + e) * part, part), :].reshape(heads * part, head_dim) for e in (0, 1)], axis=1)
                mixed = jnp.dot(perm[...], pair, preferred_element_type=jnp.float32)
                for e in (0, 1):
                    row = lax.broadcasted_iota(jnp.int32, (heads * part, head_dim), 0) + (base + (g + e) * part) * heads
                    value = mixed[:, e * head_dim:(e + 1) * head_dim]
                    value = jnp.where(row < length * heads, value, 0.0)
                    value = jnp.where((row >= fresh * heads) & (row < (fresh + 1) * heads), new_rows, value)
                    obuf[parity, pl.ds((g + e) * part * heads, part * heads), :] = value.astype(obuf.dtype)
            put(a, base, parity).start()
            return c
        lax.fori_loop(0, nblk, one, 0)

        def drain():
            for i in range(nblk - 2, nblk):
                put(a, (first + i) % nblk * piece, i % 2).wait()
        return drain

    walk(0)()

    def soften(h, c):
        slot = lax.broadcasted_iota(jnp.int32, (q_group, WINDOW), 1)
        s_key = new32[0, pl.ds(h, 1), :]
        s_new = jnp.sum(q_heads[h].astype(jnp.float32) * s_key, axis=-1, keepdims=True)
        s = jnp.where(slot == fresh, s_new, scores[h]) / head_dim ** 0.5
        s = jnp.where(slot <= length, s, -jnp.inf)
        e = jnp.exp(s - jnp.max(s, axis=-1, keepdims=True))
        p = e / jnp.sum(e, axis=-1, keepdims=True)
        p_new[h] = jnp.broadcast_to(jnp.sum(jnp.where(slot == fresh, p, 0.0), axis=-1, keepdims=True), (q_group, head_dim))
        probs[h] = jnp.where(slot == fresh, 0.0, p).astype(probs.dtype)
        acc[h] = jnp.zeros_like(acc[h])
        return c
    lax.fori_loop(0, heads, soften, 0)

    last = walk(1)
    for h in range(heads):
        o = acc[h] + p_new[h].astype(jnp.bfloat16).astype(jnp.float32) * new32[1, pl.ds(h, 1), :]
        for g in range(q_group):
            flat[:, pl.ds((h * q_group + g) * head_dim, head_dim)] = o[g:g + 1].astype(flat.dtype)
    last()
    keep.wait()
    def sent(d, c):
        for key in parts:
            send(key, d).wait_send()
        return c
    lax.fori_loop(1, n, sent, 0)
    if nst:
        for a in (0, 1):
            passed(a).wait_send()


def exchange(n, group, half, lengths, residual, norm_gain, cos_rows, sin_rows, k_rows, v_rows, w_query, w_key, w_value, w_out):
    rows, seq, head_dim = k_rows.shape
    over = seq - WINDOW
    kv_heads = w_key.shape[1] // head_dim
    q_group = w_query.shape[1] // w_key.shape[1]
    wide = w_query.shape[1] + w_key.shape[1] + w_value.shape[1]
    depth = 128
    nst = WINDOW // group - half
    bf16, f32 = k_rows.dtype, jnp.float32
    out = jax.ShapeDtypeStruct((n, WINDOW, head_dim), bf16)
    mid = pltpu.HBM((WINDOW * kv_heads, head_dim), bf16)
    any_spec = pl.BlockSpec(memory_space=pl.ANY)
    vmem = pl.BlockSpec(memory_space=pltpu.VMEM)
    hbm = pl.BlockSpec(memory_space=pltpu.HBM)
    dma = pltpu.SemaphoreType.DMA
    return pl.pallas_call(
        functools.partial(exchange_kernel, n, group, half),
        out_shape=(out, out, mid, mid, pltpu.VMEM((1, w_query.shape[1]), bf16), pltpu.VMEM(w_out.shape, bf16)),
        in_specs=[pl.BlockSpec(memory_space=pltpu.SMEM)] + [vmem] * 4 + [any_spec] * 6,
        out_specs=(any_spec,) * 2 + (hbm,) * 2 + (vmem, vmem),
        scratch_shapes=[
            pltpu.VMEM((2, rows, over, head_dim), bf16), pltpu.VMEM((2, rows, over, head_dim), bf16),
            pltpu.VMEM((2, rows, max(nst, 1) * group, head_dim), bf16),
            pltpu.VMEM((n, WINDOW, head_dim), bf16),
            pltpu.VMEM((2, depth, wide), bf16),
            pltpu.VMEM((1, w_query.shape[0]), bf16), pltpu.VMEM((1, wide), f32), pltpu.VMEM((wide // head_dim, head_dim), f32),
            pltpu.VMEM((kv_heads, q_group, head_dim), bf16),
            pltpu.VMEM((kv_heads, q_group, WINDOW), f32), pltpu.VMEM((kv_heads, q_group, WINDOW), bf16),
            pltpu.VMEM((kv_heads, q_group, head_dim), f32), pltpu.VMEM((kv_heads, q_group, head_dim), f32), pltpu.VMEM((2, kv_heads, head_dim), f32),
            pltpu.VMEM((256, 256), bf16), pltpu.VMEM((2, group * kv_heads, head_dim), bf16),
            dma((n, 16)), dma((n, 16)), dma((16,)), dma((2,)), dma((2,)), dma((2, 2)), dma((2, 2)), dma((2, 3)), dma, dma((2,)), dma,
        ],
        compiler_params=pltpu.CompilerParams(collective_id=0, has_side_effects=True, vmem_limit_bytes=VMEM_EXCHANGE),
        cost_estimate=pl.CostEstimate(flops=10 ** 11, bytes_accessed=128 << 20, transcendentals=0),
        name=f'exchange{half}',
    )(lengths, residual, norm_gain, cos_rows, sin_rows, k_rows, v_rows, w_query, w_key, w_value, w_out)[2:]


def finish_kernel(k_in, v_in, x_ref, flat_ref, w_ref, k_out, v_out, x_out, bufs, in_sem, out_sem):
    count, size = bufs.shape[:2]
    each = count // 2

    def rows(i):
        return pl.ds(pl.multiple_of(i * size, size), size)

    def read(a, i):
        return pltpu.make_async_copy((k_in, v_in)[a].at[rows(i), :], bufs.at[a * each + i], in_sem.at[a * each + i])

    def write(a, i):
        return pltpu.make_async_copy(bufs.at[a * each + i], (k_out, v_out)[a].at[rows(i), :], out_sem.at[a * each + i])
    for i in range(each):
        for a in (0, 1):
            read(a, i).start()
    wide = w_ref.shape[1] // each

    def one(i, c):
        at = pl.ds(pl.multiple_of(i * wide, wide), wide)
        o = jnp.dot(flat_ref[...], w_ref[:, at], preferred_element_type=jnp.float32)
        x_out[:, at] = (x_ref[:, at].astype(jnp.float32) + o).astype(x_out.dtype)
        for a in (0, 1):
            read(a, i).wait()
            write(a, i).start()
        return c
    lax.fori_loop(0, each, one, 0)
    for i in range(each):
        for a in (0, 1):
            write(a, i).wait()


def finish(k_mid, v_mid, flat, residual, w_out):
    size, head_dim = k_mid.shape
    width, dim = w_out.shape
    count = 16
    cache = jax.ShapeDtypeStruct(k_mid.shape, k_mid.dtype)
    hbm = pl.BlockSpec(memory_space=pltpu.HBM)
    vmem = pl.BlockSpec(memory_space=pltpu.VMEM)
    return pl.pallas_call(
        finish_kernel,
        in_specs=[hbm, hbm, vmem, vmem, vmem],
        out_specs=[hbm, hbm, vmem],
        scratch_shapes=[pltpu.VMEM((count, 2 * size // count, head_dim), k_mid.dtype), pltpu.SemaphoreType.DMA((count,)), pltpu.SemaphoreType.DMA((count,))],
        out_shape=(cache, cache, jax.ShapeDtypeStruct(residual.shape, residual.dtype)),
        compiler_params=pltpu.CompilerParams(vmem_limit_bytes=VMEM_FINISH),
        cost_estimate=pl.CostEstimate(flops=10 ** 9, bytes_accessed=64 << 20, transcendentals=0),
        name='finish',
    )(pltpu.with_memory_space_constraint(k_mid, pltpu.HBM), pltpu.with_memory_space_constraint(v_mid, pltpu.HBM), residual, pltpu.with_memory_space_constraint(flat, pltpu.VMEM), pltpu.with_memory_space_constraint(w_out, pltpu.VMEM))


GROUP = 256
VMEM_EXCHANGE = 27 << 20
VMEM_FINISH = 20 << 20


def solution(mesh):
    head_spec = P('dp', None, 'sh', None)
    row_spec = P(('dp', 'sh'))
    full_spec = P(None, None)
    n = mesh.shape['sh']

    def per_device(k_prefill, v_prefill, lengths, residual, norm_gain, w_query, w_key, w_value, w_out):
        num_rows = residual.shape[0]
        rows, seq, _, head_dim = k_prefill.shape
        kv_heads = w_key.shape[1] // head_dim
        half_dim = head_dim // 2
        k_rows = k_prefill.reshape(rows, seq, head_dim)
        v_rows = v_prefill.reshape(rows, seq, head_dim)
        blocks = (jnp.minimum(lengths, WINDOW) + GROUP - 1) // GROUP
        need = (jnp.max(blocks.reshape(-1, 2).sum(axis=1)) + 1) // 2
        level = jnp.maximum(need - levels(GROUP)[0], 0)
        inv_freq = THETA ** (-2.0 * jnp.arange(half_dim, dtype=jnp.float32) / head_dim)
        angles = lengths.astype(jnp.float32)[:, None] * inv_freq
        cos_rows = jnp.concatenate([jnp.cos(angles), jnp.cos(angles)], axis=1)
        sin_rows = jnp.concatenate([-jnp.sin(angles), jnp.sin(angles)], axis=1)
        k_mid, v_mid, flat, w_keep = lax.switch(
            level, [functools.partial(exchange, n, GROUP, half) for half in levels(GROUP)],
            lengths, residual, norm_gain.reshape(-1, head_dim), cos_rows, sin_rows, k_rows, v_rows, w_query, w_key, w_value, w_out)
        k_cache, v_cache, resid_out = finish(k_mid, v_mid, flat, residual, w_keep)
        cache_shape = (num_rows, WINDOW, kv_heads, head_dim)
        return resid_out, k_cache.reshape(cache_shape), v_cache.reshape(cache_shape)
    return jax.shard_map(per_device, mesh=mesh, in_specs=(head_spec, head_spec, P('dp'), P(('dp', 'sh'), None), P(None), full_spec, full_spec, full_spec, full_spec), out_specs=(P(('dp', 'sh'), None), row_spec, row_spec), check_vma=False)
```

```python
import functools

import jax
import jax.numpy as jnp
from jax import lax
from jax.experimental import pallas as pl
from jax.experimental.pallas import tpu as pltpu
from jax.sharding import PartitionSpec as P

WINDOW = 4096
THETA = 10000.0
EPS = 1e-5
MESH = pl.DeviceIdType.MESH


SIZES = ((17, 17), (17, 23), (17, 27), (18, 25), (18, 30), (19, 19), (20, 28), (20, 31), (21, 21), (22, 22), (22, 32), (24, 24), (25, 19), (26, 26), (27, 27), (29, 29), (30, 21), (30, 30), (32, 23), (32, 32))


def variants():
    return sorted(SIZES, key=lambda p: (3 * max(p) + min(p), p))


def exchange_kernel(n, group, pair, len_ref, x_ref, g_ref, cos_ref, sin_ref, k_in, v_in, wq, wk, wv, wo,
                    k_out, v_out, k_mid, v_mid, flat, wo_keep,
                    over_a, over_b, staged, kv_buf, wbuf, normed, proj, proj2, q_heads, scores, probs, p_new, acc, new32, perm, obuf,
                    send_sem, recv_sem, own_sem, fsend_sem, frecv_sem, over_sem, stage_sem, w_sem, kv_sem, o_sem, wo_sem):
    me = lax.axis_index('sh')
    mate = me + 1 - 2 * lax.rem(me, 2)
    heads, q_group, head_dim = q_heads.shape
    over = over_a.shape[2]
    nblk = WINDOW // group
    spare = staged.shape[2] // group

    def plan(dev):
        odd = lax.rem(lax.div(dev, 2), 2)
        both = pair[0] + odd * (pair[1] - pair[0])
        mine = lax.div(both + 1 - lax.rem(dev, 2), 2)
        return both, mine, both - nblk
    both, mine, first = plan(me)
    barrier = pltpu.get_barrier_semaphore()

    def hello(d, c):
        pl.semaphore_signal(barrier, inc=1, device_id={'sh': lax.rem(me + d, n)}, device_id_type=MESH)
        return c
    lax.fori_loop(1, n, hello, 0)

    ins, outs, mids = (k_in, v_in), (k_out, v_out), (k_mid, v_mid)

    def span(block, count=1):
        return pl.ds(pl.multiple_of(block * group, group), count * group)

    def over_load(a, e):
        return pltpu.make_async_copy(ins[a].at[:, pl.ds(e * WINDOW, over)], (over_a, over_b)[e].at[a], over_sem.at[a, e])

    def shown(dev):
        return jnp.minimum(plan(dev)[2], nblk - spare)

    def own_load(a, r):
        return pltpu.make_async_copy(ins[a].at[r, span(shown(r), spare)], staged.at[a, r], stage_sem.at[a, r])

    def other_load(a):
        return pltpu.make_async_copy(ins[a].at[:, pl.ds((nblk - spare) * group, spare * group)], kv_buf.at[:, pl.ds(a * spare * group, spare * group)], stage_sem.at[a, n])
    for a in (0, 1):
        for e in (0, 1):
            over_load(a, e).start()
    for a in (0, 1):
        other_load(a).start()

        def go(r, c):
            own_load(a, r).start()
            return c
        lax.fori_loop(0, n, go, 0)
    depth, wide = wbuf.shape[1], wbuf.shape[2]
    wsteps = wq.shape[0] // depth
    weights = ((wq, 0), (wk, wq.shape[1]), (wv, wq.shape[1] + wk.shape[1]))

    def w_load(step, slot, i):
        src, at = weights[i]
        return pltpu.make_async_copy(src.at[pl.ds(pl.multiple_of(step * depth, depth), depth), :], wbuf.at[slot, :, pl.ds(at, src.shape[1])], w_sem.at[slot, i])
    for i in range(3):
        w_load(0, 0, i).start()

    def source(kind, a, dev, j):
        if kind == 'first':
            return over_a.at[a, dev]
        if kind == 'plain':
            return ins[a].at[dev, span(j)]
        return staged.at[a, dev, span(j - shown(dev))]

    def send(kind, a, d, j):
        peer = lax.rem(me + d, n)
        return pltpu.make_async_remote_copy(
            src_ref=source(kind, a, peer, j), dst_ref=outs[a].at[me, span(j)],
            send_sem=send_sem.at[a, d], recv_sem=recv_sem.at[a, j], device_id={'sh': peer}, device_id_type=MESH)

    def own(kind, a, j):
        return pltpu.make_async_copy(source(kind, a, me, j), outs[a].at[me, span(j)], own_sem.at[a, j])

    bounds = {'first': lambda p: (0, 1), 'plain': lambda p: (1, p[2]), 'mixed': lambda p: (p[2], p[1])}
    reach = {'first': (0, 1), 'plain': (1, max(pair) - nblk), 'mixed': (min(pair) - nblk, (max(pair) + 1) // 2)}

    def launch(kind, a):
        def at_block(j, c):
            def to(d, c):
                lo, hi = bounds[kind](plan(lax.rem(me + d, n)))

                @pl.when((j >= lo) & (j < hi))
                def _():
                    send(kind, a, d, j).start()
                return c
            lax.fori_loop(1, n, to, 0)
            lo, hi = bounds[kind]((both, mine, first))

            @pl.when((j >= lo) & (j < hi))
            def _():
                own(kind, a, j).start()
            return c
        lax.fori_loop(*reach[kind], at_block, 0)

    for a in (0, 1):
        for e in (0, 1):
            over_load(a, e).wait()

        def put_first(r, c):
            slot = lax.broadcasted_iota(jnp.int32, over_a.shape[2:], 0)
            over_a[a, r] = jnp.where(slot < len_ref[r] - WINDOW, over_b[a, r], over_a[a, r])
            return c
        lax.fori_loop(0, n, put_first, 0)
    pl.semaphore_wait(barrier, n - 1)
    launch('plain', 0)
    launch('first', 0)
    launch('first', 1)
    for a in (0, 1):
        other_load(a).wait()

        def put_mixed(r, c):
            own_load(a, r).wait()
            both_r, mine_r, first_r = plan(r)
            blocks = lax.div(jnp.minimum(len_ref[r], WINDOW) + group - 1, group)

            def one(j, c):
                other = kv_buf[r + 1 - 2 * lax.rem(r, 2), span(a * spare + both_r - 1 - j - (nblk - spare)), :]
                at = span(j - shown(r))
                staged[a, r, at, :] = jnp.where(j < blocks, staged[a, r, at, :], other)
                return c
            return lax.fori_loop(first_r, mine_r, one, c)
        lax.fori_loop(0, n, put_mixed, 0)
    launch('mixed', 0)
    launch('mixed', 1)
    launch('plain', 1)

    x = x_ref[...].astype(jnp.float32)
    inv_rms = lax.rsqrt(jnp.mean(x * x, axis=-1, keepdims=True) + EPS)
    for j in range(x.shape[1] // head_dim):
        at = pl.ds(j * head_dim, head_dim)
        normed[:, at] = (x_ref[:, at].astype(jnp.float32) * inv_rms * g_ref[pl.ds(j, 1), :].astype(jnp.float32)).astype(normed.dtype)
    proj[...] = jnp.zeros_like(proj)
    strip = 2048

    def project(step, c):
        slot = lax.rem(step, 2)

        @pl.when(step + 1 < wsteps)
        def _():
            for i in range(3):
                w_load(step + 1, 1 - slot, i).start()
        for i in range(3):
            w_load(step, slot, i).wait()
        h = normed[:, pl.ds(pl.multiple_of(step * depth, depth), depth)]

        def one(t, c):
            at = pl.ds(pl.multiple_of(t * strip, strip), strip)
            proj[:, at] += jnp.dot(h, wbuf[slot, :, at], preferred_element_type=jnp.float32)
            return c
        return lax.fori_loop(0, wide // strip, one, c)
    lax.fori_loop(0, wsteps, project, 0)
    keep = pltpu.make_async_copy(wo, wo_keep, wo_sem)
    keep.start()
    for j in range(wide // head_dim):
        proj2[pl.ds(j, 1), :] = proj[:, pl.ds(j * head_dim, head_dim)]
    cos_row, sin_row = cos_ref[pl.ds(me, 1), :], sin_ref[pl.ds(me, 1), :]

    def turn(value):
        value = value.astype(jnp.bfloat16).astype(jnp.float32)
        return (value * cos_row + pltpu.roll(value, head_dim // 2, 1) * sin_row).astype(jnp.bfloat16)
    nq = heads * q_group
    turned = turn(proj2[pl.ds(0, nq), :])
    for h in range(heads):
        q_heads[h] = turned[h * q_group:(h + 1) * q_group]
    new32[0] = turn(proj2[pl.ds(nq, heads), :]).astype(jnp.float32)
    new32[1] = proj2[pl.ds(nq + heads, heads), :].astype(jnp.bfloat16).astype(jnp.float32)
    part = perm.shape[0] // heads
    row = lax.broadcasted_iota(jnp.int32, perm.shape, 0)
    col = lax.broadcasted_iota(jnp.int32, perm.shape, 1)
    perm[...] = jnp.where(col == lax.rem(row, heads) * part + lax.div(row, heads), 1.0, 0.0).astype(perm.dtype)

    def forward(a, head, j):
        return pltpu.make_async_remote_copy(
            src_ref=outs[a].at[head, span(j)], dst_ref=outs[a].at[head, span(both - 1 - j)],
            send_sem=fsend_sem.at[a], recv_sem=frecv_sem.at[a, both - 1 - j], device_id={'sh': mate}, device_id_type=MESH)

    length = len_ref[me]
    fresh = lax.rem(length, WINDOW)
    piece = group
    mixed_count, passed_count = mine - first, nblk - mine

    def put(a, at, parity):
        rows = piece * heads
        return pltpu.make_async_copy(obuf.at[parity], mids[a].at[pl.ds(pl.multiple_of(at * heads, rows), rows), :], o_sem.at[parity])

    def arrive(a, block):
        @pl.when(block < mine)
        def _():
            own('first', a, block).wait()

            from_all = outs[a].at[pl.ds(0, n - 1), span(block)]
            pltpu.make_async_copy(from_all, from_all, recv_sem.at[a, block]).wait()

        @pl.when((block >= first) & (block < mine))
        def _():
            def go(h, c):
                forward(a, h, block).start()
                return c
            lax.fori_loop(0, heads, go, 0)

        @pl.when(block >= mine)
        def _():
            from_mate = outs[a].at[:, span(block)]
            pltpu.make_async_copy(from_mate, from_mate, frecv_sem.at[a, block]).wait()
        fetch = pltpu.make_async_copy(outs[a].at[:, span(block)], kv_buf.at[:, span(block)], kv_sem)
        fetch.start()
        fetch.wait()

    def soften(h, c):
        slot = lax.broadcasted_iota(jnp.int32, (q_group, WINDOW), 1)
        s_key = new32[0, pl.ds(h, 1), :]
        s_new = jnp.sum(q_heads[h].astype(jnp.float32) * s_key, axis=-1, keepdims=True)
        s = jnp.where(slot == fresh, s_new, scores[h]) / head_dim ** 0.5
        s = jnp.where(slot <= length, s, -jnp.inf)
        e = jnp.exp(s - jnp.max(s, axis=-1, keepdims=True))
        p = e / jnp.sum(e, axis=-1, keepdims=True)
        p_new[h] = jnp.broadcast_to(jnp.sum(jnp.where(slot == fresh, p, 0.0), axis=-1, keepdims=True), (q_group, head_dim))
        probs[h] = jnp.where(slot == fresh, 0.0, p).astype(probs.dtype)
        acc[h] = jnp.zeros_like(acc[h])
        return c
    def walk(t, c):
        a, i = lax.div(t, nblk), lax.rem(t, nblk)
        second = lax.div(i, 2)
        is_mixed = (lax.rem(i, 2) == 0) & (second < mixed_count)
        block = jnp.where(i >= mixed_count + passed_count, i - mixed_count - passed_count, jnp.where(is_mixed, first + second, nblk - 1 - second))
        base = pl.multiple_of(block * piece, piece)
        at = pl.ds(base, piece)
        parity = lax.rem(t, 2)

        @pl.when(t >= 2)
        def _():
            put(0, base, parity).wait()

        @pl.when(a == 0)
        def _():
            arrive(0, block)
            for h in range(heads):
                scores[h, :, at] = lax.dot_general(q_heads[h], kv_buf[h, at, :], (((1,), (1,)), ((), ())), preferred_element_type=jnp.float32)

        @pl.when(t == nblk)
        def _():
            lax.fori_loop(0, heads, soften, 0)

        @pl.when(a == 1)
        def _():
            arrive(1, block)
            for h in range(heads):
                acc[h] += jnp.dot(probs[h, :, at], kv_buf[h, at, :], preferred_element_type=jnp.float32)

        def mingle(g, c):
            def heads_of(e):
                return kv_buf[:, pl.ds(pl.multiple_of(base + (2 * g + e) * part, part), part), :].reshape(heads * part, head_dim)
            mixed = jnp.dot(perm[...], jnp.concatenate([heads_of(0), heads_of(1)], axis=1), preferred_element_type=jnp.float32)
            new_rows = jnp.tile(new32[a], (part, 1))
            for e in (0, 1):
                lo = (2 * g + e) * part * heads
                row = lax.broadcasted_iota(jnp.int32, (heads * part, head_dim), 0) + (base * heads + lo)
                value = mixed[:, e * head_dim:(e + 1) * head_dim]
                value = jnp.where(row < length * heads, value, 0.0)
                value = jnp.where((row >= fresh * heads) & (row < (fresh + 1) * heads), new_rows, value)
                obuf[parity, pl.ds(pl.multiple_of(lo, part * heads), part * heads), :] = value.astype(obuf.dtype)
            return c
        lax.fori_loop(0, piece // part // 2, mingle, 0)
        for b in (0, 1):
            pl.when(a == b)(put(b, base, parity).start)
        return c
    lax.fori_loop(0, 2 * nblk, walk, 0)
    for h in range(heads):
        o = acc[h] + p_new[h].astype(jnp.bfloat16).astype(jnp.float32) * new32[1, pl.ds(h, 1), :]
        for g in range(q_group):
            flat[:, pl.ds((h * q_group + g) * head_dim, head_dim)] = o[g:g + 1].astype(flat.dtype)
    for parity in (0, 1):
        put(0, 0, parity).wait()
    keep.wait()

    for odd in (0, 1):
        for core in (0, 1):
            count = (pair[odd] + 1 - core) // 2

            def is_place(dev):
                return (lax.rem(lax.div(dev, 2), 2) == odd) & (lax.rem(dev, 2) == core)

            def sent(d, c):
                @pl.when(is_place(lax.rem(me + d, n)))
                def _():
                    for a in (0, 1):
                        gone = outs[a].at[0, pl.ds(0, count * group)]
                        pltpu.make_async_copy(gone, gone, send_sem.at[a, d]).wait()
                return c
            lax.fori_loop(1, n, sent, 0)
            passing = count - (pair[odd] - nblk)
            if passing:
                @pl.when(is_place(me))
                def _():
                    for a in (0, 1):
                        gone = outs[a].at[:, pl.ds(0, passing * group)]
                        pltpu.make_async_copy(gone, gone, fsend_sem.at[a]).wait()


def exchange(n, group, pair, lengths, residual, norm_gain, cos_rows, sin_rows, k_rows, v_rows, w_query, w_key, w_value, w_out):
    rows, seq, head_dim = k_rows.shape
    over = seq - WINDOW
    kv_heads = w_key.shape[1] // head_dim
    q_group = w_query.shape[1] // w_key.shape[1]
    wide = w_query.shape[1] + w_key.shape[1] + w_value.shape[1]
    depth = 128
    nblk = WINDOW // group
    spare = nblk // 2
    bf16, f32 = k_rows.dtype, jnp.float32
    out = jax.ShapeDtypeStruct((n, WINDOW, head_dim), bf16)
    mid = pltpu.HBM((WINDOW * kv_heads, head_dim), bf16)
    any_spec = pl.BlockSpec(memory_space=pl.ANY)
    vmem = pl.BlockSpec(memory_space=pltpu.VMEM)
    hbm = pl.BlockSpec(memory_space=pltpu.HBM)
    dma = pltpu.SemaphoreType.DMA
    return pl.pallas_call(
        functools.partial(exchange_kernel, n, group, pair),
        out_shape=(out, out, mid, mid, pltpu.VMEM((1, w_query.shape[1]), bf16), pltpu.VMEM(w_out.shape, bf16)),
        in_specs=[pl.BlockSpec(memory_space=pltpu.SMEM)] + [vmem] * 4 + [any_spec] * 6,
        out_specs=(any_spec,) * 2 + (hbm,) * 2 + (vmem, vmem),
        scratch_shapes=[
            pltpu.VMEM((2, rows, over, head_dim), bf16), pltpu.VMEM((2, rows, over, head_dim), bf16),
            pltpu.VMEM((2, rows, spare * group, head_dim), bf16),
            pltpu.VMEM((n, WINDOW, head_dim), bf16),
            pltpu.VMEM((2, depth, wide), bf16),
            pltpu.VMEM((1, w_query.shape[0]), bf16), pltpu.VMEM((1, wide), f32), pltpu.VMEM((wide // head_dim, head_dim), f32),
            pltpu.VMEM((kv_heads, q_group, head_dim), bf16),
            pltpu.VMEM((kv_heads, q_group, WINDOW), f32), pltpu.VMEM((kv_heads, q_group, WINDOW), bf16),
            pltpu.VMEM((kv_heads, q_group, head_dim), f32), pltpu.VMEM((kv_heads, q_group, head_dim), f32), pltpu.VMEM((2, kv_heads, head_dim), f32),
            pltpu.VMEM((256, 256), bf16), pltpu.VMEM((2, group * kv_heads, head_dim), bf16),
            dma((2, n)), dma((2, nblk)), dma((2, nblk)), dma((2,)), dma((2, nblk)), dma((2, 2)), dma((2, n + 1)), dma((2, 3)), dma, dma((2,)), dma,
        ],
        compiler_params=pltpu.CompilerParams(collective_id=0, has_side_effects=True, vmem_limit_bytes=VMEM_EXCHANGE),
        cost_estimate=pl.CostEstimate(flops=10 ** 11, bytes_accessed=128 << 20, transcendentals=0),
        name=f'exchange{pair[0]}_{pair[1]}',
    )(lengths, residual, norm_gain, cos_rows, sin_rows, k_rows, v_rows, w_query, w_key, w_value, w_out)[2:]


def finish_kernel(k_in, v_in, x_ref, flat_ref, w_ref, k_out, v_out, x_out, bufs, in_sem, out_sem):
    count, size = bufs.shape[:2]
    each = count // 2

    def rows(i):
        return pl.ds(pl.multiple_of(i * size, size), size)

    def read(a, i):
        return pltpu.make_async_copy((k_in, v_in)[a].at[rows(i), :], bufs.at[a * each + i], in_sem.at[a * each + i])

    def write(a, i):
        return pltpu.make_async_copy(bufs.at[a * each + i], (k_out, v_out)[a].at[rows(i), :], out_sem.at[a * each + i])
    for i in range(each):
        for a in (0, 1):
            read(a, i).start()
    wide = w_ref.shape[1] // each

    def one(i, c):
        at = pl.ds(pl.multiple_of(i * wide, wide), wide)
        o = jnp.dot(flat_ref[...], w_ref[:, at], preferred_element_type=jnp.float32)
        x_out[:, at] = (x_ref[:, at].astype(jnp.float32) + o).astype(x_out.dtype)
        for a in (0, 1):
            read(a, i).wait()
            write(a, i).start()
        return c
    lax.fori_loop(0, each, one, 0)
    for i in range(each):
        for a in (0, 1):
            write(a, i).wait()


def finish(k_mid, v_mid, flat, residual, w_out):
    size, head_dim = k_mid.shape
    width, dim = w_out.shape
    count = 16
    cache = jax.ShapeDtypeStruct(k_mid.shape, k_mid.dtype)
    hbm = pl.BlockSpec(memory_space=pltpu.HBM)
    vmem = pl.BlockSpec(memory_space=pltpu.VMEM)
    return pl.pallas_call(
        finish_kernel,
        in_specs=[hbm, hbm, vmem, vmem, vmem],
        out_specs=[hbm, hbm, vmem],
        scratch_shapes=[pltpu.VMEM((count, 2 * size // count, head_dim), k_mid.dtype), pltpu.SemaphoreType.DMA((count,)), pltpu.SemaphoreType.DMA((count,))],
        out_shape=(cache, cache, jax.ShapeDtypeStruct(residual.shape, residual.dtype)),
        compiler_params=pltpu.CompilerParams(vmem_limit_bytes=VMEM_FINISH),
        cost_estimate=pl.CostEstimate(flops=10 ** 9, bytes_accessed=64 << 20, transcendentals=0),
        name='finish',
    )(pltpu.with_memory_space_constraint(k_mid, pltpu.HBM), pltpu.with_memory_space_constraint(v_mid, pltpu.HBM), residual, pltpu.with_memory_space_constraint(flat, pltpu.VMEM), pltpu.with_memory_space_constraint(w_out, pltpu.VMEM))


GROUP = 256
VMEM_EXCHANGE = 27 << 20
VMEM_FINISH = 20 << 20


def solution(mesh):
    head_spec = P('dp', None, 'sh', None)
    row_spec = P(('dp', 'sh'))
    full_spec = P(None, None)
    n = mesh.shape['sh']

    def per_device(k_prefill, v_prefill, lengths, residual, norm_gain, w_query, w_key, w_value, w_out):
        num_rows = residual.shape[0]
        rows, seq, _, head_dim = k_prefill.shape
        kv_heads = w_key.shape[1] // head_dim
        half_dim = head_dim // 2
        k_rows = k_prefill.reshape(rows, seq, head_dim)
        v_rows = v_prefill.reshape(rows, seq, head_dim)
        blocks = (jnp.minimum(lengths, WINDOW) + GROUP - 1) // GROUP
        chips = [blocks[2 * c] + blocks[2 * c + 1] for c in range(rows // 2)]
        even, odd = functools.reduce(jnp.maximum, chips[0::2]), functools.reduce(jnp.maximum, chips[1::2])
        choices = variants()
        fits = (even <= jnp.array([p[0] for p in choices])) & (odd <= jnp.array([p[1] for p in choices]))
        level = jnp.min(jnp.where(fits, jnp.arange(len(choices), dtype=jnp.int32), len(choices) - 1))
        inv_freq = THETA ** (-2.0 * jnp.arange(half_dim, dtype=jnp.float32) / head_dim)
        angles = lengths.astype(jnp.float32)[:, None] * inv_freq
        cos_rows = jnp.concatenate([jnp.cos(angles), jnp.cos(angles)], axis=1)
        sin_rows = jnp.concatenate([-jnp.sin(angles), jnp.sin(angles)], axis=1)
        k_mid, v_mid, flat, w_keep = lax.switch(
            level, [functools.partial(exchange, n, GROUP, pair) for pair in choices],
            lengths, residual, norm_gain.reshape(-1, head_dim), cos_rows, sin_rows, k_rows, v_rows, w_query, w_key, w_value, w_out)
        k_cache, v_cache, resid_out = finish(k_mid, v_mid, flat, residual, w_keep)
        cache_shape = (num_rows, WINDOW, kv_heads, head_dim)
        return resid_out, k_cache.reshape(cache_shape), v_cache.reshape(cache_shape)
    return jax.shard_map(per_device, mesh=mesh, in_specs=(head_spec, head_spec, P('dp'), P(('dp', 'sh'), None), P(None), full_spec, full_spec, full_spec, full_spec), out_specs=(P(('dp', 'sh'), None), row_spec, row_spec), check_vma=False)
```

```python
import functools

import jax
import jax.numpy as jnp
from jax import lax
from jax.experimental import pallas as pl
from jax.experimental.pallas import tpu as pltpu
from jax.sharding import PartitionSpec as P

WINDOW = 4096
THETA = 10000.0
EPS = 1e-5
MESH = pl.DeviceIdType.MESH


def levels(group):
    nblk = WINDOW // group
    return tuple(range(nblk // 2 + 1, nblk + 1))


def exchange_kernel(n, group, half, len_ref, x_ref, g_ref, cos_ref, sin_ref, k_in, v_in, wq, wk, wv, wo,
                    k_out, v_out, k_mid, v_mid, flat, wo_keep,
                    over_a, over_b, staged, kv_buf, wbuf, normed, proj, proj2, q_heads, scores, probs, p_new, acc, new32, perm, obuf,
                    send_sem, recv_sem, own_sem, fsend_sem, frecv_sem, over_sem, stage_sem, w_sem, kv_sem, o_sem, wo_sem):
    me = lax.axis_index('sh')
    mate = me + 1 - 2 * lax.rem(me, 2)
    heads, q_group, head_dim = q_heads.shape
    over = over_a.shape[2]
    nblk = WINDOW // group
    first = 2 * half - nblk
    nst = half - first
    barrier = pltpu.get_barrier_semaphore()
    for d in range(1, n):
        pl.semaphore_signal(barrier, inc=1, device_id={'sh': lax.rem(me + d, n)}, device_id_type=MESH)

    ins, outs, mids = (k_in, v_in), (k_out, v_out), (k_mid, v_mid)

    def over_load(a, e):
        return pltpu.make_async_copy(ins[a].at[:, pl.ds(e * WINDOW, over)], (over_a, over_b)[e].at[a], over_sem.at[a, e])

    def own_load(a):
        return pltpu.make_async_copy(ins[a].at[:, pl.ds(first * group, nst * group)], staged.at[a], stage_sem.at[a, 0])

    def other_load(a):
        return pltpu.make_async_copy(ins[a].at[:, pl.ds(half * group, nst * group)], kv_buf.at[:, pl.ds(a * nst * group, nst * group)], stage_sem.at[a, 1])
    for a in (0, 1):
        if nst:
            own_load(a).start()
            other_load(a).start()
        for e in (0, 1):
            over_load(a, e).start()
    depth, wide = wbuf.shape[1], wbuf.shape[2]
    wsteps = wq.shape[0] // depth
    weights = ((wq, 0), (wk, wq.shape[1]), (wv, wq.shape[1] + wk.shape[1]))

    def w_load(step, slot, i):
        src, at = weights[i]
        return pltpu.make_async_copy(src.at[pl.ds(pl.multiple_of(step * depth, depth), depth), :], wbuf.at[slot, :, pl.ds(at, src.shape[1])], w_sem.at[slot, i])
    for i in range(3):
        w_load(0, 0, i).start()
    pl.semaphore_wait(barrier, n - 1)

    piece = 2 * group
    tail = min(piece, max(first * group - over, 0))
    cut = first * group - tail
    parts = {}
    for a in (0, 1):
        parts[a, 'first'] = (over_a.at[a], 0, 0, over)
        if nst:
            parts[a, 'mixed'] = (staged.at[a], 0, first * group, nst * group)
        chunk = 2 * piece if a else WINDOW
        for lo in range(over, cut, chunk):
            parts[a, 'plain', lo] = (ins[a], lo, lo, min(chunk, cut - lo))
        if tail:
            parts[a, 'tail'] = (ins[a], cut, cut, tail)
    index = {key: i for i, key in enumerate(parts)}

    def send(key, d):
        src, at, to, size = parts[key]
        peer = lax.rem(me + d, n)
        return pltpu.make_async_remote_copy(
            src_ref=src.at[peer, pl.ds(at, size)], dst_ref=outs[key[0]].at[me, pl.ds(to, size)],
            send_sem=send_sem.at[d], recv_sem=recv_sem.at[index[key]], device_id={'sh': peer}, device_id_type=MESH)

    def own(key):
        src, at, to, size = parts[key]
        return pltpu.make_async_copy(src.at[me, pl.ds(at, size)], outs[key[0]].at[me, pl.ds(to, size)], own_sem.at[index[key]])

    def launch(key):
        if key in parts:
            def go(d, c):
                send(key, d).start()
                return c
            lax.fori_loop(1, n, go, 0)
            own(key).start()

    def launch_plain(a):
        for key in parts:
            if key[0] == a and key[1] in ('plain', 'tail'):
                launch(key)

    def arrived(key):
        if key in parts:
            own(key).wait()
            _, _, to, size = parts[key]
            from_all = outs[key[0]].at[pl.ds(0, n - 1), pl.ds(to, size)]
            pltpu.make_async_copy(from_all, from_all, recv_sem.at[index[key]]).wait()

    launch_plain(0)
    for a in (0, 1):
        for e in (0, 1):
            over_load(a, e).wait()

        def put_first(r, c):
            slot = lax.broadcasted_iota(jnp.int32, over_a.shape[2:], 0)
            over_a[a, r] = jnp.where(slot < len_ref[r] - WINDOW, over_b[a, r], over_a[a, r])
            return c
        lax.fori_loop(0, n, put_first, 0)
        if nst:
            own_load(a).wait()
            other_load(a).wait()

            def put_mixed(i, c):
                r, j = lax.div(i, nst), lax.rem(i, nst)
                blocks = lax.div(jnp.minimum(len_ref[r], WINDOW) + group - 1, group)
                other = kv_buf[r + 1 - 2 * lax.rem(r, 2), pl.ds(pl.multiple_of((a * nst + nst - 1 - j) * group, group), group), :]
                at = pl.ds(pl.multiple_of(j * group, group), group)
                staged[a, r, at, :] = jnp.where(first + j < blocks, staged[a, r, at, :], other)
                return c
            lax.fori_loop(0, n * nst, put_mixed, 0)
    launch((0, 'mixed'))
    launch((0, 'first'))
    launch((1, 'mixed'))
    launch((1, 'first'))
    launch_plain(1)

    x = x_ref[...].astype(jnp.float32)
    inv_rms = lax.rsqrt(jnp.mean(x * x, axis=-1, keepdims=True) + EPS)
    for j in range(x.shape[1] // head_dim):
        at = pl.ds(j * head_dim, head_dim)
        normed[:, at] = (x_ref[:, at].astype(jnp.float32) * inv_rms * g_ref[pl.ds(j, 1), :].astype(jnp.float32)).astype(normed.dtype)
    proj[...] = jnp.zeros_like(proj)
    strip = 1024

    def project(step, c):
        slot = lax.rem(step, 2)

        @pl.when(step + 1 < wsteps)
        def _():
            for i in range(3):
                w_load(step + 1, 1 - slot, i).start()
        for i in range(3):
            w_load(step, slot, i).wait()
        h = normed[:, pl.ds(pl.multiple_of(step * depth, depth), depth)]

        for lo in range(0, wide, strip):
            proj[:, pl.ds(lo, strip)] += jnp.dot(h, wbuf[slot, :, pl.ds(lo, strip)], preferred_element_type=jnp.float32)
        return c
    lax.fori_loop(0, wsteps, project, 0)
    keep = pltpu.make_async_copy(wo, wo_keep, wo_sem)
    keep.start()
    for j in range(wide // head_dim):
        proj2[pl.ds(j, 1), :] = proj[:, pl.ds(j * head_dim, head_dim)]
    cos_row, sin_row = cos_ref[pl.ds(me, 1), :], sin_ref[pl.ds(me, 1), :]

    def turn(value):
        value = value.astype(jnp.bfloat16).astype(jnp.float32)
        return (value * cos_row + pltpu.roll(value, head_dim // 2, 1) * sin_row).astype(jnp.bfloat16)
    nq = heads * q_group
    turned = turn(proj2[pl.ds(0, nq), :])
    for h in range(heads):
        q_heads[h] = turned[h * q_group:(h + 1) * q_group]
    new32[0] = turn(proj2[pl.ds(nq, heads), :]).astype(jnp.float32)
    new32[1] = proj2[pl.ds(nq + heads, heads), :].astype(jnp.bfloat16).astype(jnp.float32)
    part = perm.shape[0] // heads
    row = lax.broadcasted_iota(jnp.int32, perm.shape, 0)
    col = lax.broadcasted_iota(jnp.int32, perm.shape, 1)
    perm[...] = jnp.where(col == lax.rem(row, heads) * part + lax.div(row, heads), 1.0, 0.0).astype(perm.dtype)

    def forward(a, head, j):
        return pltpu.make_async_remote_copy(
            src_ref=outs[a].at[head, pl.ds(pl.multiple_of(j * group, group), group)],
            dst_ref=outs[a].at[head, pl.ds(pl.multiple_of((2 * half - 1 - j) * group, group), group)],
            send_sem=fsend_sem.at[a], recv_sem=frecv_sem.at[a], device_id={'sh': mate}, device_id_type=MESH)

    def pass_on(a):
        arrived((a, 'mixed'))

        def go(i, c):
            forward(a, lax.div(i, nst), first + lax.rem(i, nst)).start()
            return c
        lax.fori_loop(0, n * nst, go, 0)

    def passed(a):
        return pltpu.make_async_remote_copy(
            src_ref=outs[a].at[:, pl.ds(first * group, nst * group)], dst_ref=outs[a].at[:, pl.ds(half * group, nst * group)],
            send_sem=fsend_sem.at[a], recv_sem=frecv_sem.at[a], device_id={'sh': mate}, device_id_type=MESH)

    length = len_ref[me]
    fresh = lax.rem(length, WINDOW)

    def put(a, at, parity):
        rows = piece * heads
        return pltpu.make_async_copy(obuf.at[parity], mids[a].at[pl.ds(pl.multiple_of(at * heads, rows), rows), :], o_sem.at[parity])

    npiece, start_piece = WINDOW // piece, first * group // piece
    due = {}

    def fetch(a, lo, hi):
        copy = pltpu.make_async_copy(outs[a].at[:, pl.ds(lo, hi - lo)], kv_buf.at[:, pl.ds(lo, hi - lo)], kv_sem)
        copy.start()
        copy.wait()

    def get(key):
        arrived(key)
        _, _, lo, size = parts[key]
        fetch(key[0], lo, lo + size)

    def get_mixed(a):
        pass_on(a)
        fetch(a, first * group, half * group)

    def get_passed(a):
        passed(a).wait_recv()
        fetch(a, half * group, WINDOW)
    for a in (0, 1):
        if nst:
            due.setdefault(a * npiece, []).append(functools.partial(get_mixed, a))
            due.setdefault(a * npiece + half * group // piece - start_piece, []).append(functools.partial(get_passed, a))
        for key in parts:
            if key[0] == a and key[1] != 'mixed':
                due.setdefault(a * npiece + npiece - start_piece + parts[key][2] // piece, []).append(functools.partial(get, key))

    def soften(h, c):
        slot = lax.broadcasted_iota(jnp.int32, (q_group, WINDOW), 1)
        s_key = new32[0, pl.ds(h, 1), :]
        s_new = jnp.sum(q_heads[h].astype(jnp.float32) * s_key, axis=-1, keepdims=True)
        s = jnp.where(slot == fresh, s_new, scores[h]) / head_dim ** 0.5
        s = jnp.where(slot <= length, s, -jnp.inf)
        e = jnp.exp(s - jnp.max(s, axis=-1, keepdims=True))
        p = e / jnp.sum(e, axis=-1, keepdims=True)
        p_new[h] = jnp.broadcast_to(jnp.sum(jnp.where(slot == fresh, p, 0.0), axis=-1, keepdims=True), (q_group, head_dim))
        probs[h] = jnp.where(slot == fresh, 0.0, p).astype(probs.dtype)
        acc[h] = jnp.zeros_like(acc[h])
        return c
    def soften_all():
        lax.fori_loop(0, heads, soften, 0)
    due.setdefault(npiece, []).insert(0, soften_all)

    def walk(t, c):
        def act(actions):
            for action in actions:
                action()
        for at_step, actions in due.items():
            pl.when(t == at_step)(functools.partial(act, actions))
        a = lax.div(t, npiece)
        base = pl.multiple_of(lax.rem(start_piece + t, npiece) * piece, piece)
        at = pl.ds(base, piece)
        parity = lax.rem(t, 2)

        @pl.when(t >= 2)
        def _():
            put(0, base, parity).wait()

        @pl.when(a == 0)
        def _():
            for h in range(heads):
                scores[h, :, at] = lax.dot_general(q_heads[h], kv_buf[h, at, :], (((1,), (1,)), ((), ())), preferred_element_type=jnp.float32)

        @pl.when(a == 1)
        def _():
            for h in range(heads):
                acc[h] += jnp.dot(probs[h, :, at], kv_buf[h, at, :], preferred_element_type=jnp.float32)
        new_rows = jnp.tile(new32[a], (part, 1))
        for g in range(0, piece // part, 2):
            pair = jnp.concatenate([kv_buf[:, pl.ds(base + (g + e) * part, part), :].reshape(heads * part, head_dim) for e in (0, 1)], axis=1)
            mixed = jnp.dot(perm[...], pair, preferred_element_type=jnp.float32)
            for e in (0, 1):
                row = lax.broadcasted_iota(jnp.int32, (heads * part, head_dim), 0) + (base + (g + e) * part) * heads
                value = mixed[:, e * head_dim:(e + 1) * head_dim]
                value = jnp.where(row < length * heads, value, 0.0)
                value = jnp.where((row >= fresh * heads) & (row < (fresh + 1) * heads), new_rows, value)
                obuf[parity, pl.ds((g + e) * part * heads, part * heads), :] = value.astype(obuf.dtype)
        for b in (0, 1):
            pl.when(a == b)(put(b, base, parity).start)
        return c
    lax.fori_loop(0, 2 * npiece, walk, 0)
    for h in range(heads):
        o = acc[h] + p_new[h].astype(jnp.bfloat16).astype(jnp.float32) * new32[1, pl.ds(h, 1), :]
        for g in range(q_group):
            flat[:, pl.ds((h * q_group + g) * head_dim, head_dim)] = o[g:g + 1].astype(flat.dtype)
    for parity in (0, 1):
        put(0, 0, parity).wait()
    keep.wait()
    def sent(d, c):
        gone = outs[0].at[pl.ds(0, 2), pl.ds(0, half * group)]
        pltpu.make_async_copy(gone, gone, send_sem.at[d]).wait()
        return c
    lax.fori_loop(1, n, sent, 0)
    if nst:
        for a in (0, 1):
            passed(a).wait_send()


def exchange(n, group, half, lengths, residual, norm_gain, cos_rows, sin_rows, k_rows, v_rows, w_query, w_key, w_value, w_out):
    rows, seq, head_dim = k_rows.shape
    over = seq - WINDOW
    kv_heads = w_key.shape[1] // head_dim
    q_group = w_query.shape[1] // w_key.shape[1]
    wide = w_query.shape[1] + w_key.shape[1] + w_value.shape[1]
    depth = 128
    nst = WINDOW // group - half
    bf16, f32 = k_rows.dtype, jnp.float32
    out = jax.ShapeDtypeStruct((n, WINDOW, head_dim), bf16)
    mid = pltpu.HBM((WINDOW * kv_heads, head_dim), bf16)
    any_spec = pl.BlockSpec(memory_space=pl.ANY)
    vmem = pl.BlockSpec(memory_space=pltpu.VMEM)
    hbm = pl.BlockSpec(memory_space=pltpu.HBM)
    dma = pltpu.SemaphoreType.DMA
    return pl.pallas_call(
        functools.partial(exchange_kernel, n, group, half),
        out_shape=(out, out, mid, mid, pltpu.VMEM((1, w_query.shape[1]), bf16), pltpu.VMEM(w_out.shape, bf16)),
        in_specs=[pl.BlockSpec(memory_space=pltpu.SMEM)] + [vmem] * 4 + [any_spec] * 6,
        out_specs=(any_spec,) * 2 + (hbm,) * 2 + (vmem, vmem),
        scratch_shapes=[
            pltpu.VMEM((2, rows, over, head_dim), bf16), pltpu.VMEM((2, rows, over, head_dim), bf16),
            pltpu.VMEM((2, rows, max(nst, 1) * group, head_dim), bf16),
            pltpu.VMEM((n, WINDOW, head_dim), bf16),
            pltpu.VMEM((2, depth, wide), bf16),
            pltpu.VMEM((1, w_query.shape[0]), bf16), pltpu.VMEM((1, wide), f32), pltpu.VMEM((wide // head_dim, head_dim), f32),
            pltpu.VMEM((kv_heads, q_group, head_dim), bf16),
            pltpu.VMEM((kv_heads, q_group, WINDOW), f32), pltpu.VMEM((kv_heads, q_group, WINDOW), bf16),
            pltpu.VMEM((kv_heads, q_group, head_dim), f32), pltpu.VMEM((kv_heads, q_group, head_dim), f32), pltpu.VMEM((2, kv_heads, head_dim), f32),
            pltpu.VMEM((256, 256), bf16), pltpu.VMEM((2, 2 * group * kv_heads, head_dim), bf16),
            dma((n,)), dma((16,)), dma((16,)), dma((2,)), dma((2,)), dma((2, 2)), dma((2, 2)), dma((2, 3)), dma, dma((2,)), dma,
        ],
        compiler_params=pltpu.CompilerParams(collective_id=0, has_side_effects=True, vmem_limit_bytes=VMEM_EXCHANGE),
        cost_estimate=pl.CostEstimate(flops=10 ** 11, bytes_accessed=128 << 20, transcendentals=0),
        name=f'exchange{half}',
    )(lengths, residual, norm_gain, cos_rows, sin_rows, k_rows, v_rows, w_query, w_key, w_value, w_out)[2:]


def finish_kernel(k_in, v_in, x_ref, flat_ref, w_ref, k_out, v_out, x_out, bufs, in_sem, out_sem):
    count, size = bufs.shape[:2]
    each = count // 2

    def rows(i):
        return pl.ds(pl.multiple_of(i * size, size), size)

    def read(a, i):
        return pltpu.make_async_copy((k_in, v_in)[a].at[rows(i), :], bufs.at[a * each + i], in_sem.at[a * each + i])

    def write(a, i):
        return pltpu.make_async_copy(bufs.at[a * each + i], (k_out, v_out)[a].at[rows(i), :], out_sem.at[a * each + i])
    for i in range(each):
        for a in (0, 1):
            read(a, i).start()
    wide = w_ref.shape[1] // each

    def one(i, c):
        at = pl.ds(pl.multiple_of(i * wide, wide), wide)
        o = jnp.dot(flat_ref[...], w_ref[:, at], preferred_element_type=jnp.float32)
        x_out[:, at] = (x_ref[:, at].astype(jnp.float32) + o).astype(x_out.dtype)
        for a in (0, 1):
            read(a, i).wait()
            write(a, i).start()
        return c
    lax.fori_loop(0, each, one, 0)
    for i in range(each):
        for a in (0, 1):
            write(a, i).wait()


def finish(k_mid, v_mid, flat, residual, w_out):
    size, head_dim = k_mid.shape
    width, dim = w_out.shape
    count = 16
    cache = jax.ShapeDtypeStruct(k_mid.shape, k_mid.dtype)
    hbm = pl.BlockSpec(memory_space=pltpu.HBM)
    vmem = pl.BlockSpec(memory_space=pltpu.VMEM)
    return pl.pallas_call(
        finish_kernel,
        in_specs=[hbm, hbm, vmem, vmem, vmem],
        out_specs=[hbm, hbm, vmem],
        scratch_shapes=[pltpu.VMEM((count, 2 * size // count, head_dim), k_mid.dtype), pltpu.SemaphoreType.DMA((count,)), pltpu.SemaphoreType.DMA((count,))],
        out_shape=(cache, cache, jax.ShapeDtypeStruct(residual.shape, residual.dtype)),
        compiler_params=pltpu.CompilerParams(vmem_limit_bytes=VMEM_FINISH),
        cost_estimate=pl.CostEstimate(flops=10 ** 9, bytes_accessed=64 << 20, transcendentals=0),
        name='finish',
    )(pltpu.with_memory_space_constraint(k_mid, pltpu.HBM), pltpu.with_memory_space_constraint(v_mid, pltpu.HBM), residual, pltpu.with_memory_space_constraint(flat, pltpu.VMEM), pltpu.with_memory_space_constraint(w_out, pltpu.VMEM))


GROUP = 128
VMEM_EXCHANGE = 27 << 20
VMEM_FINISH = 20 << 20


def solution(mesh):
    head_spec = P('dp', None, 'sh', None)
    row_spec = P(('dp', 'sh'))
    full_spec = P(None, None)
    n = mesh.shape['sh']

    def per_device(k_prefill, v_prefill, lengths, residual, norm_gain, w_query, w_key, w_value, w_out):
        num_rows = residual.shape[0]
        rows, seq, _, head_dim = k_prefill.shape
        kv_heads = w_key.shape[1] // head_dim
        half_dim = head_dim // 2
        k_rows = k_prefill.reshape(rows, seq, head_dim)
        v_rows = v_prefill.reshape(rows, seq, head_dim)
        blocks = (jnp.minimum(lengths, WINDOW) + GROUP - 1) // GROUP
        need = (jnp.max(blocks.reshape(-1, 2).sum(axis=1)) + 1) // 2
        level = jnp.maximum(need - levels(GROUP)[0], 0)
        inv_freq = THETA ** (-2.0 * jnp.arange(half_dim, dtype=jnp.float32) / head_dim)
        angles = lengths.astype(jnp.float32)[:, None] * inv_freq
        cos_rows = jnp.concatenate([jnp.cos(angles), jnp.cos(angles)], axis=1)
        sin_rows = jnp.concatenate([-jnp.sin(angles), jnp.sin(angles)], axis=1)
        k_mid, v_mid, flat, w_keep = lax.switch(
            level, [functools.partial(exchange, n, GROUP, half) for half in levels(GROUP)],
            lengths, residual, norm_gain.reshape(-1, head_dim), cos_rows, sin_rows, k_rows, v_rows, w_query, w_key, w_value, w_out)
        k_cache, v_cache, resid_out = finish(k_mid, v_mid, flat, residual, w_keep)
        cache_shape = (num_rows, WINDOW, kv_heads, head_dim)
        return resid_out, k_cache.reshape(cache_shape), v_cache.reshape(cache_shape)
    return jax.shard_map(per_device, mesh=mesh, in_specs=(head_spec, head_spec, P('dp'), P(('dp', 'sh'), None), P(None), full_spec, full_spec, full_spec, full_spec), out_specs=(P(('dp', 'sh'), None), row_spec, row_spec), check_vma=False)
```

```python
import functools

import jax
import jax.numpy as jnp
from jax import lax
from jax.experimental import pallas as pl
from jax.experimental.pallas import tpu as pltpu
from jax.sharding import PartitionSpec as P

WINDOW = 4096
THETA = 10000.0
EPS = 1e-5
MESH = pl.DeviceIdType.MESH


def levels(group):
    nblk = WINDOW // group
    return tuple(range(nblk // 2 + 1, nblk + 1))


def exchange_kernel(n, group, half, len_ref, x_ref, g_ref, cos_ref, sin_ref, k_in, v_in, wq, wk, wv, wo,
                    k_out, v_out, k_mid, v_mid, flat, wo_keep,
                    over_a, over_b, staged, kv_buf, wbuf, normed, proj, proj2, q_heads, scores, probs, p_new, acc, new32, perm, obuf, tail_buf,
                    send_sem, recv_sem, own_sem, fsend_sem, frecv_sem, over_sem, stage_sem, w_sem, kv_sem, o_sem, wo_sem):
    me = lax.axis_index('sh')
    mate = me + 1 - 2 * lax.rem(me, 2)
    heads, q_group, head_dim = q_heads.shape
    over = over_a.shape[2]
    nblk = WINDOW // group
    first = 2 * half - nblk
    nst = half - first
    barrier = pltpu.get_barrier_semaphore()
    for d in range(1, n):
        pl.semaphore_signal(barrier, inc=1, device_id={'sh': lax.rem(me + d, n)}, device_id_type=MESH)

    ins, outs, mids = (k_in, v_in), (k_out, v_out), (k_mid, v_mid)

    def over_load(a, e):
        return pltpu.make_async_copy(ins[a].at[:, pl.ds(e * WINDOW, over)], (over_a, over_b)[e].at[a], over_sem.at[a, e])

    def own_load(a):
        return pltpu.make_async_copy(ins[a].at[:, pl.ds(first * group, nst * group)], staged.at[a], stage_sem.at[a, 0])

    def other_load(a):
        return pltpu.make_async_copy(ins[a].at[:, pl.ds(half * group, nst * group)], kv_buf.at[:, pl.ds(a * nst * group, nst * group)], stage_sem.at[a, 1])
    for a in (0, 1):
        if nst:
            own_load(a).start()
            other_load(a).start()
        for e in (0, 1):
            over_load(a, e).start()
    depth, wide = wbuf.shape[1], wbuf.shape[2]
    wsteps = wq.shape[0] // depth
    weights = ((wq, 0), (wk, wq.shape[1]), (wv, wq.shape[1] + wk.shape[1]))

    def w_load(step, slot, i):
        src, at = weights[i]
        return pltpu.make_async_copy(src.at[pl.ds(pl.multiple_of(step * depth, depth), depth), :], wbuf.at[slot, :, pl.ds(at, src.shape[1])], w_sem.at[slot, i])
    for i in range(3):
        w_load(0, 0, i).start()
    pl.semaphore_wait(barrier, n - 1)

    piece = 2 * group
    tail = min(piece, max(first * group - over, 0))
    cut = first * group - tail
    parts = {}
    for a in (0, 1):
        parts[a, 'first'] = (over_a.at[a], 0, 0, over)
        if nst:
            parts[a, 'mixed'] = (staged.at[a], 0, first * group, nst * group)
        chunk = 2 * piece if a else WINDOW
        for lo in range(over, cut, chunk):
            parts[a, 'plain', lo] = (ins[a], lo, lo, min(chunk, cut - lo))
        if tail:
            parts[a, 'tail'] = (ins[a], cut, cut, tail)
    index = {key: i for i, key in enumerate(parts)}

    def landing(key, head):
        _, _, to, size = parts[key]
        if key == (1, 'tail'):
            return tail_buf.at[head]
        return outs[key[0]].at[head, pl.ds(to, size)]

    def send(key, d):
        src, at, to, size = parts[key]
        peer = lax.rem(me + d, n)
        return pltpu.make_async_remote_copy(
            src_ref=src.at[peer, pl.ds(at, size)], dst_ref=landing(key, me),
            send_sem=send_sem.at[d], recv_sem=recv_sem.at[index[key]], device_id={'sh': peer}, device_id_type=MESH)

    def own(key):
        src, at, to, size = parts[key]
        return pltpu.make_async_copy(src.at[me, pl.ds(at, size)], landing(key, me), own_sem.at[index[key]])

    def launch(key):
        if key in parts:
            def go(d, c):
                send(key, d).start()
                return c
            lax.fori_loop(1, n, go, 0)
            own(key).start()

    def launch_plain(a):
        for key in parts:
            if key[0] == a and key[1] in ('plain', 'tail'):
                launch(key)

    def arrived(key):
        if key in parts:
            own(key).wait()
            _, _, to, size = parts[key]
            from_all = tail_buf.at[pl.ds(0, n - 1)] if key == (1, 'tail') else outs[key[0]].at[pl.ds(0, n - 1), pl.ds(to, size)]
            pltpu.make_async_copy(from_all, from_all, recv_sem.at[index[key]]).wait()

    launch_plain(0)
    for a in (0, 1):
        for e in (0, 1):
            over_load(a, e).wait()

        def put_first(r, c):
            slot = lax.broadcasted_iota(jnp.int32, over_a.shape[2:], 0)
            over_a[a, r] = jnp.where(slot < len_ref[r] - WINDOW, over_b[a, r], over_a[a, r])
            return c
        lax.fori_loop(0, n, put_first, 0)
        if nst:
            own_load(a).wait()
            other_load(a).wait()

            def put_mixed(i, c):
                r, j = lax.div(i, nst), lax.rem(i, nst)
                blocks = lax.div(jnp.minimum(len_ref[r], WINDOW) + group - 1, group)
                other = kv_buf[r + 1 - 2 * lax.rem(r, 2), pl.ds(pl.multiple_of((a * nst + nst - 1 - j) * group, group), group), :]
                at = pl.ds(pl.multiple_of(j * group, group), group)
                staged[a, r, at, :] = jnp.where(first + j < blocks, staged[a, r, at, :], other)
                return c
            lax.fori_loop(0, n * nst, put_mixed, 0)
    launch((0, 'mixed'))
    launch((0, 'first'))
    launch((1, 'mixed'))
    launch((1, 'first'))
    launch_plain(1)

    x = x_ref[...].astype(jnp.float32)
    inv_rms = lax.rsqrt(jnp.mean(x * x, axis=-1, keepdims=True) + EPS)
    for j in range(x.shape[1] // head_dim):
        at = pl.ds(j * head_dim, head_dim)
        normed[:, at] = (x_ref[:, at].astype(jnp.float32) * inv_rms * g_ref[pl.ds(j, 1), :].astype(jnp.float32)).astype(normed.dtype)
    proj[...] = jnp.zeros_like(proj)
    strip = 1024

    def project(step, c):
        slot = lax.rem(step, 2)

        @pl.when(step + 1 < wsteps)
        def _():
            for i in range(3):
                w_load(step + 1, 1 - slot, i).start()
        for i in range(3):
            w_load(step, slot, i).wait()
        h = normed[:, pl.ds(pl.multiple_of(step * depth, depth), depth)]

        for lo in range(0, wide, strip):
            proj[:, pl.ds(lo, strip)] += jnp.dot(h, wbuf[slot, :, pl.ds(lo, strip)], preferred_element_type=jnp.float32)
        return c
    lax.fori_loop(0, wsteps, project, 0)
    keep = pltpu.make_async_copy(wo, wo_keep, wo_sem)
    keep.start()
    for j in range(wide // head_dim):
        proj2[pl.ds(j, 1), :] = proj[:, pl.ds(j * head_dim, head_dim)]
    cos_row, sin_row = cos_ref[pl.ds(me, 1), :], sin_ref[pl.ds(me, 1), :]

    def turn(value):
        value = value.astype(jnp.bfloat16).astype(jnp.float32)
        return (value * cos_row + pltpu.roll(value, head_dim // 2, 1) * sin_row).astype(jnp.bfloat16)
    nq = heads * q_group
    turned = turn(proj2[pl.ds(0, nq), :])
    for h in range(heads):
        q_heads[h] = turned[h * q_group:(h + 1) * q_group]
    new32[0] = turn(proj2[pl.ds(nq, heads), :]).astype(jnp.float32)
    new32[1] = proj2[pl.ds(nq + heads, heads), :].astype(jnp.bfloat16).astype(jnp.float32)
    part = perm.shape[0] // heads
    row = lax.broadcasted_iota(jnp.int32, perm.shape, 0)
    col = lax.broadcasted_iota(jnp.int32, perm.shape, 1)
    perm[...] = jnp.where(col == lax.rem(row, heads) * part + lax.div(row, heads), 1.0, 0.0).astype(perm.dtype)

    def forward(a, head, j):
        return pltpu.make_async_remote_copy(
            src_ref=outs[a].at[head, pl.ds(pl.multiple_of(j * group, group), group)],
            dst_ref=outs[a].at[head, pl.ds(pl.multiple_of((2 * half - 1 - j) * group, group), group)],
            send_sem=fsend_sem.at[a], recv_sem=frecv_sem.at[a], device_id={'sh': mate}, device_id_type=MESH)

    def pass_on(a):
        arrived((a, 'mixed'))

        def go(i, c):
            forward(a, lax.div(i, nst), first + lax.rem(i, nst)).start()
            return c
        lax.fori_loop(0, n * nst, go, 0)

    def passed(a):
        return pltpu.make_async_remote_copy(
            src_ref=outs[a].at[:, pl.ds(first * group, nst * group)], dst_ref=outs[a].at[:, pl.ds(half * group, nst * group)],
            send_sem=fsend_sem.at[a], recv_sem=frecv_sem.at[a], device_id={'sh': mate}, device_id_type=MESH)

    length = len_ref[me]
    fresh = lax.rem(length, WINDOW)

    def put(a, at, parity):
        rows = piece * heads
        return pltpu.make_async_copy(obuf.at[parity], mids[a].at[pl.ds(pl.multiple_of(at * heads, rows), rows), :], o_sem.at[parity])

    npiece, start_piece = WINDOW // piece, first * group // piece
    due = {}

    def fetch(a, lo, hi):
        copy = pltpu.make_async_copy(outs[a].at[:, pl.ds(lo, hi - lo)], kv_buf.at[:, pl.ds(lo, hi - lo)], kv_sem)
        copy.start()
        copy.wait()

    def get(key):
        arrived(key)
        _, _, lo, size = parts[key]
        if key == (1, 'tail'):
            kv_buf[:, pl.ds(lo, size), :] = tail_buf[...]
        else:
            fetch(key[0], lo, lo + size)

    def get_mixed(a):
        pass_on(a)
        fetch(a, first * group, half * group)

    def get_passed(a):
        passed(a).wait_recv()
        fetch(a, half * group, WINDOW)
    for a in (0, 1):
        if nst:
            due.setdefault(a * npiece, []).append(functools.partial(get_mixed, a))
            due.setdefault(a * npiece + half * group // piece - start_piece, []).append(functools.partial(get_passed, a))
        for key in parts:
            if key[0] == a and key[1] != 'mixed':
                due.setdefault(a * npiece + npiece - start_piece + parts[key][2] // piece, []).append(functools.partial(get, key))

    def soften(h, c):
        slot = lax.broadcasted_iota(jnp.int32, (q_group, WINDOW), 1)
        s_key = new32[0, pl.ds(h, 1), :]
        s_new = jnp.sum(q_heads[h].astype(jnp.float32) * s_key, axis=-1, keepdims=True)
        s = jnp.where(slot == fresh, s_new, scores[h]) / head_dim ** 0.5
        s = jnp.where(slot <= length, s, -jnp.inf)
        e = jnp.exp(s - jnp.max(s, axis=-1, keepdims=True))
        p = e / jnp.sum(e, axis=-1, keepdims=True)
        p_new[h] = jnp.broadcast_to(jnp.sum(jnp.where(slot == fresh, p, 0.0), axis=-1, keepdims=True), (q_group, head_dim))
        probs[h] = jnp.where(slot == fresh, 0.0, p).astype(probs.dtype)
        acc[h] = jnp.zeros_like(acc[h])
        return c
    def soften_all():
        lax.fori_loop(0, heads, soften, 0)
    due.setdefault(npiece, []).insert(0, soften_all)

    def walk(t, c):
        def act(actions):
            for action in actions:
                action()
        for at_step, actions in due.items():
            pl.when(t == at_step)(functools.partial(act, actions))
        a = lax.div(t, npiece)
        base = pl.multiple_of(lax.rem(start_piece + t, npiece) * piece, piece)
        at = pl.ds(base, piece)
        parity = lax.rem(t, 2)

        @pl.when(t >= 2)
        def _():
            put(0, base, parity).wait()

        @pl.when(a == 0)
        def _():
            for h in range(heads):
                scores[h, :, at] = lax.dot_general(q_heads[h], kv_buf[h, at, :], (((1,), (1,)), ((), ())), preferred_element_type=jnp.float32)

        @pl.when(a == 1)
        def _():
            for h in range(heads):
                acc[h] += jnp.dot(probs[h, :, at], kv_buf[h, at, :], preferred_element_type=jnp.float32)
        new_rows = jnp.tile(new32[a], (part, 1))
        for g in range(0, piece // part, 2):
            pair = jnp.concatenate([kv_buf[:, pl.ds(base + (g + e) * part, part), :].reshape(heads * part, head_dim) for e in (0, 1)], axis=1)
            mixed = jnp.dot(perm[...], pair, preferred_element_type=jnp.float32)
            for e in (0, 1):
                row = lax.broadcasted_iota(jnp.int32, (heads * part, head_dim), 0) + (base + (g + e) * part) * heads
                value = mixed[:, e * head_dim:(e + 1) * head_dim]
                value = jnp.where(row < length * heads, value, 0.0)
                value = jnp.where((row >= fresh * heads) & (row < (fresh + 1) * heads), new_rows, value)
                obuf[parity, pl.ds((g + e) * part * heads, part * heads), :] = value.astype(obuf.dtype)
        for b in (0, 1):
            pl.when(a == b)(put(b, base, parity).start)
        return c
    lax.fori_loop(0, 2 * npiece, walk, 0)
    for h in range(heads):
        o = acc[h] + p_new[h].astype(jnp.bfloat16).astype(jnp.float32) * new32[1, pl.ds(h, 1), :]
        for g in range(q_group):
            flat[:, pl.ds((h * q_group + g) * head_dim, head_dim)] = o[g:g + 1].astype(flat.dtype)
    for parity in (0, 1):
        put(0, 0, parity).wait()
    keep.wait()
    def sent(d, c):
        gone = outs[0].at[pl.ds(0, 2), pl.ds(0, half * group)]
        pltpu.make_async_copy(gone, gone, send_sem.at[d]).wait()
        return c
    lax.fori_loop(1, n, sent, 0)
    if nst:
        for a in (0, 1):
            passed(a).wait_send()


def exchange(n, group, half, lengths, residual, norm_gain, cos_rows, sin_rows, k_rows, v_rows, w_query, w_key, w_value, w_out):
    rows, seq, head_dim = k_rows.shape
    over = seq - WINDOW
    kv_heads = w_key.shape[1] // head_dim
    q_group = w_query.shape[1] // w_key.shape[1]
    wide = w_query.shape[1] + w_key.shape[1] + w_value.shape[1]
    depth = 128
    nst = WINDOW // group - half
    bf16, f32 = k_rows.dtype, jnp.float32
    out = jax.ShapeDtypeStruct((n, WINDOW, head_dim), bf16)
    mid = pltpu.HBM((WINDOW * kv_heads, head_dim), bf16)
    any_spec = pl.BlockSpec(memory_space=pl.ANY)
    vmem = pl.BlockSpec(memory_space=pltpu.VMEM)
    hbm = pl.BlockSpec(memory_space=pltpu.HBM)
    dma = pltpu.SemaphoreType.DMA
    return pl.pallas_call(
        functools.partial(exchange_kernel, n, group, half),
        out_shape=(out, out, mid, mid, pltpu.VMEM((1, w_query.shape[1]), bf16), pltpu.VMEM(w_out.shape, bf16)),
        in_specs=[pl.BlockSpec(memory_space=pltpu.SMEM)] + [vmem] * 4 + [any_spec] * 6,
        out_specs=(any_spec,) * 2 + (hbm,) * 2 + (vmem, vmem),
        scratch_shapes=[
            pltpu.VMEM((2, rows, over, head_dim), bf16), pltpu.VMEM((2, rows, over, head_dim), bf16),
            pltpu.VMEM((2, rows, max(nst, 1) * group, head_dim), bf16),
            pltpu.VMEM((n, WINDOW, head_dim), bf16),
            pltpu.VMEM((2, depth, wide), bf16),
            pltpu.VMEM((1, w_query.shape[0]), bf16), pltpu.VMEM((1, wide), f32), pltpu.VMEM((wide // head_dim, head_dim), f32),
            pltpu.VMEM((kv_heads, q_group, head_dim), bf16),
            pltpu.VMEM((kv_heads, q_group, WINDOW), f32), pltpu.VMEM((kv_heads, q_group, WINDOW), bf16),
            pltpu.VMEM((kv_heads, q_group, head_dim), f32), pltpu.VMEM((kv_heads, q_group, head_dim), f32), pltpu.VMEM((2, kv_heads, head_dim), f32),
            pltpu.VMEM((256, 256), bf16), pltpu.VMEM((2, 2 * group * kv_heads, head_dim), bf16), pltpu.VMEM((n, 2 * group, head_dim), bf16),
            dma((n,)), dma((16,)), dma((16,)), dma((2,)), dma((2,)), dma((2, 2)), dma((2, 2)), dma((2, 3)), dma, dma((2,)), dma,
        ],
        compiler_params=pltpu.CompilerParams(collective_id=0, has_side_effects=True, vmem_limit_bytes=VMEM_EXCHANGE),
        cost_estimate=pl.CostEstimate(flops=10 ** 11, bytes_accessed=128 << 20, transcendentals=0),
        name=f'exchange{half}',
    )(lengths, residual, norm_gain, cos_rows, sin_rows, k_rows, v_rows, w_query, w_key, w_value, w_out)[2:]


def finish_kernel(k_in, v_in, x_ref, flat_ref, w_ref, k_out, v_out, x_out, bufs, in_sem, out_sem):
    count, size = bufs.shape[:2]
    each = count // 2

    def rows(i):
        return pl.ds(pl.multiple_of(i * size, size), size)

    def read(a, i):
        return pltpu.make_async_copy((k_in, v_in)[a].at[rows(i), :], bufs.at[a * each + i], in_sem.at[a * each + i])

    def write(a, i):
        return pltpu.make_async_copy(bufs.at[a * each + i], (k_out, v_out)[a].at[rows(i), :], out_sem.at[a * each + i])
    for i in range(each):
        for a in (0, 1):
            read(a, i).start()
    wide = w_ref.shape[1] // each

    def one(i, c):
        at = pl.ds(pl.multiple_of(i * wide, wide), wide)
        o = jnp.dot(flat_ref[...], w_ref[:, at], preferred_element_type=jnp.float32)
        x_out[:, at] = (x_ref[:, at].astype(jnp.float32) + o).astype(x_out.dtype)

        @pl.when(i < each // 2)
        def _():
            for a in (0, 1):
                for b in (0, 1):
                    read(a, 2 * i + b).wait()
                    write(a, 2 * i + b).start()
        return c
    lax.fori_loop(0, each, one, 0)
    for i in range(each):
        for a in (0, 1):
            write(a, i).wait()


def finish(k_mid, v_mid, flat, residual, w_out):
    size, head_dim = k_mid.shape
    width, dim = w_out.shape
    count = 16
    cache = jax.ShapeDtypeStruct(k_mid.shape, k_mid.dtype)
    hbm = pl.BlockSpec(memory_space=pltpu.HBM)
    vmem = pl.BlockSpec(memory_space=pltpu.VMEM)
    return pl.pallas_call(
        finish_kernel,
        in_specs=[hbm, hbm, vmem, vmem, vmem],
        out_specs=[hbm, hbm, vmem],
        scratch_shapes=[pltpu.VMEM((count, 2 * size // count, head_dim), k_mid.dtype), pltpu.SemaphoreType.DMA((count,)), pltpu.SemaphoreType.DMA((count,))],
        out_shape=(cache, cache, jax.ShapeDtypeStruct(residual.shape, residual.dtype)),
        compiler_params=pltpu.CompilerParams(vmem_limit_bytes=VMEM_FINISH),
        cost_estimate=pl.CostEstimate(flops=10 ** 9, bytes_accessed=64 << 20, transcendentals=0),
        name='finish',
    )(pltpu.with_memory_space_constraint(k_mid, pltpu.HBM), pltpu.with_memory_space_constraint(v_mid, pltpu.HBM), residual, pltpu.with_memory_space_constraint(flat, pltpu.VMEM), pltpu.with_memory_space_constraint(w_out, pltpu.VMEM))


GROUP = 128
VMEM_EXCHANGE = 27 << 20
VMEM_FINISH = 20 << 20


def solution(mesh):
    head_spec = P('dp', None, 'sh', None)
    row_spec = P(('dp', 'sh'))
    full_spec = P(None, None)
    n = mesh.shape['sh']

    def per_device(k_prefill, v_prefill, lengths, residual, norm_gain, w_query, w_key, w_value, w_out):
        num_rows = residual.shape[0]
        rows, seq, _, head_dim = k_prefill.shape
        kv_heads = w_key.shape[1] // head_dim
        half_dim = head_dim // 2
        k_rows = k_prefill.reshape(rows, seq, head_dim)
        v_rows = v_prefill.reshape(rows, seq, head_dim)
        blocks = (jnp.minimum(lengths, WINDOW) + GROUP - 1) // GROUP
        need = (jnp.max(blocks.reshape(-1, 2).sum(axis=1)) + 1) // 2
        level = jnp.maximum(need - levels(GROUP)[0], 0)
        inv_freq = THETA ** (-2.0 * jnp.arange(half_dim, dtype=jnp.float32) / head_dim)
        angles = lengths.astype(jnp.float32)[:, None] * inv_freq
        cos_rows = jnp.concatenate([jnp.cos(angles), jnp.cos(angles)], axis=1)
        sin_rows = jnp.concatenate([-jnp.sin(angles), jnp.sin(angles)], axis=1)
        k_mid, v_mid, flat, w_keep = lax.switch(
            level, [functools.partial(exchange, n, GROUP, half) for half in levels(GROUP)],
            lengths, residual, norm_gain.reshape(-1, head_dim), cos_rows, sin_rows, k_rows, v_rows, w_query, w_key, w_value, w_out)
        k_cache, v_cache, resid_out = finish(k_mid, v_mid, flat, residual, w_keep)
        cache_shape = (num_rows, WINDOW, kv_heads, head_dim)
        return resid_out, k_cache.reshape(cache_shape), v_cache.reshape(cache_shape)
    return jax.shard_map(per_device, mesh=mesh, in_specs=(head_spec, head_spec, P('dp'), P(('dp', 'sh'), None), P(None), full_spec, full_spec, full_spec, full_spec), out_specs=(P(('dp', 'sh'), None), row_spec, row_spec), check_vma=False)
```

```python
import functools

import jax
import jax.numpy as jnp
from jax import lax
from jax.experimental import pallas as pl
from jax.experimental.pallas import tpu as pltpu
from jax.sharding import PartitionSpec as P

WINDOW = 4096
THETA = 10000.0
EPS = 1e-5
MESH = pl.DeviceIdType.MESH


def levels(group):
    nblk = WINDOW // group
    return tuple(range(nblk // 2 + 1, nblk + 1))


def exchange_kernel(n, group, half, len_ref, x_ref, g_ref, cos_ref, sin_ref, k_in, v_in, wq, wk, wv, wo,
                    k_out, v_out, k_mid, v_mid, flat, wo_keep,
                    over_a, over_b, staged, kv_buf, wbuf, normed, proj, proj2, q_heads, scores, probs, p_new, acc, new32, perm, obuf, tail_buf,
                    send_sem, recv_sem, own_sem, fsend_sem, frecv_sem, over_sem, stage_sem, w_sem, kv_sem, o_sem, wo_sem):
    me = lax.axis_index('sh')
    mate = me + 1 - 2 * lax.rem(me, 2)
    heads, q_group, head_dim = q_heads.shape
    over = over_a.shape[2]
    nblk = WINDOW // group
    first = 2 * half - nblk
    nst = half - first
    barrier = pltpu.get_barrier_semaphore()
    for d in range(1, n):
        pl.semaphore_signal(barrier, inc=1, device_id={'sh': lax.rem(me + d, n)}, device_id_type=MESH)

    ins, outs, mids = (k_in, v_in), (k_out, v_out), (k_mid, v_mid)

    def over_load(a, e):
        return pltpu.make_async_copy(ins[a].at[:, pl.ds(e * WINDOW, over)], (over_a, over_b)[e].at[a], over_sem.at[a, e])

    def own_load(a):
        return pltpu.make_async_copy(ins[a].at[:, pl.ds(first * group, nst * group)], staged.at[a], stage_sem.at[a, 0])

    def other_load(a):
        return pltpu.make_async_copy(ins[a].at[:, pl.ds(half * group, nst * group)], kv_buf.at[:, pl.ds(a * nst * group, nst * group)], stage_sem.at[a, 1])
    for a in (0, 1):
        if nst:
            own_load(a).start()
            other_load(a).start()
        for e in (0, 1):
            over_load(a, e).start()
    depth, wide = wbuf.shape[1], wbuf.shape[2]
    wsteps = wq.shape[0] // depth
    weights = ((wq, 0), (wk, wq.shape[1]), (wv, wq.shape[1] + wk.shape[1]))

    def w_load(step, slot, i):
        src, at = weights[i]
        return pltpu.make_async_copy(src.at[pl.ds(pl.multiple_of(step * depth, depth), depth), :], wbuf.at[slot, :, pl.ds(at, src.shape[1])], w_sem.at[slot, i])
    for i in range(3):
        w_load(0, 0, i).start()
    pl.semaphore_wait(barrier, n - 1)

    piece = 2 * group
    tail = min(piece, max(first * group - over, 0))
    cut = first * group - tail
    parts = {}
    for a in (0, 1):
        parts[a, 'first'] = (over_a.at[a], 0, 0, over)
        if nst:
            parts[a, 'mixed'] = (staged.at[a], 0, first * group, nst * group)
        chunk = 2 * piece if a else WINDOW
        for lo in range(over, cut, chunk):
            parts[a, 'plain', lo] = (ins[a], lo, lo, min(chunk, cut - lo))
        if tail:
            parts[a, 'tail'] = (ins[a], cut, cut, tail)
    index = {key: i for i, key in enumerate(parts)}

    def landing(key, head):
        _, _, to, size = parts[key]
        if key == (1, 'tail'):
            return tail_buf.at[head]
        return outs[key[0]].at[head, pl.ds(to, size)]

    def send(key, d):
        src, at, to, size = parts[key]
        peer = lax.rem(me + d, n)
        return pltpu.make_async_remote_copy(
            src_ref=src.at[peer, pl.ds(at, size)], dst_ref=landing(key, me),
            send_sem=send_sem.at[d], recv_sem=recv_sem.at[index[key]], device_id={'sh': peer}, device_id_type=MESH)

    def own(key):
        src, at, to, size = parts[key]
        return pltpu.make_async_copy(src.at[me, pl.ds(at, size)], landing(key, me), own_sem.at[index[key]])

    def launch(key):
        if key in parts:
            def go(d, c):
                send(key, d).start()
                return c
            lax.fori_loop(1, n, go, 0)
            own(key).start()

    def launch_plain(a):
        for key in parts:
            if key[0] == a and key[1] in ('plain', 'tail'):
                launch(key)

    def arrived(key):
        if key in parts:
            own(key).wait()
            _, _, to, size = parts[key]
            from_all = tail_buf.at[pl.ds(0, n - 1)] if key == (1, 'tail') else outs[key[0]].at[pl.ds(0, n - 1), pl.ds(to, size)]
            pltpu.make_async_copy(from_all, from_all, recv_sem.at[index[key]]).wait()

    launch_plain(0)
    for a in (0, 1):
        for e in (0, 1):
            over_load(a, e).wait()

        def put_first(r, c):
            slot = lax.broadcasted_iota(jnp.int32, over_a.shape[2:], 0)
            over_a[a, r] = jnp.where(slot < len_ref[r] - WINDOW, over_b[a, r], over_a[a, r])
            return c
        lax.fori_loop(0, n, put_first, 0)
        if nst:
            own_load(a).wait()
            other_load(a).wait()

            def put_mixed(i, c):
                r, j = lax.div(i, nst), lax.rem(i, nst)
                blocks = lax.div(jnp.minimum(len_ref[r], WINDOW) + group - 1, group)
                other = kv_buf[r + 1 - 2 * lax.rem(r, 2), pl.ds(pl.multiple_of((a * nst + nst - 1 - j) * group, group), group), :]
                at = pl.ds(pl.multiple_of(j * group, group), group)
                staged[a, r, at, :] = jnp.where(first + j < blocks, staged[a, r, at, :], other)
                return c
            lax.fori_loop(0, n * nst, put_mixed, 0)
    launch((0, 'mixed'))
    launch((0, 'first'))
    launch((1, 'mixed'))
    launch((1, 'first'))
    launch_plain(1)

    x = x_ref[...].astype(jnp.float32)
    inv_rms = lax.rsqrt(jnp.mean(x * x, axis=-1, keepdims=True) + EPS)
    for j in range(x.shape[1] // head_dim):
        at = pl.ds(j * head_dim, head_dim)
        normed[:, at] = (x_ref[:, at].astype(jnp.float32) * inv_rms * g_ref[pl.ds(j, 1), :].astype(jnp.float32)).astype(normed.dtype)
    proj[...] = jnp.zeros_like(proj)
    strip = 1024

    def project(step, c):
        slot = lax.rem(step, 2)

        @pl.when(step + 1 < wsteps)
        def _():
            for i in range(3):
                w_load(step + 1, 1 - slot, i).start()
        for i in range(3):
            w_load(step, slot, i).wait()
        h = normed[:, pl.ds(pl.multiple_of(step * depth, depth), depth)]

        for lo in range(0, wide, strip):
            proj[:, pl.ds(lo, strip)] += jnp.dot(h, wbuf[slot, :, pl.ds(lo, strip)], preferred_element_type=jnp.float32)
        return c
    lax.fori_loop(0, wsteps, project, 0)
    keep = pltpu.make_async_copy(wo, wo_keep, wo_sem)
    keep.start()
    for j in range(wide // head_dim):
        proj2[pl.ds(j, 1), :] = proj[:, pl.ds(j * head_dim, head_dim)]
    cos_row, sin_row = cos_ref[pl.ds(me, 1), :], sin_ref[pl.ds(me, 1), :]

    def turn(value):
        value = value.astype(jnp.bfloat16).astype(jnp.float32)
        return (value * cos_row + pltpu.roll(value, head_dim // 2, 1) * sin_row).astype(jnp.bfloat16)
    nq = heads * q_group
    turned = turn(proj2[pl.ds(0, nq), :])
    for h in range(heads):
        q_heads[h] = turned[h * q_group:(h + 1) * q_group]
    new32[0] = turn(proj2[pl.ds(nq, heads), :]).astype(jnp.float32)
    new32[1] = proj2[pl.ds(nq + heads, heads), :].astype(jnp.bfloat16).astype(jnp.float32)
    part = perm.shape[0] // heads
    row = lax.broadcasted_iota(jnp.int32, perm.shape, 0)
    col = lax.broadcasted_iota(jnp.int32, perm.shape, 1)
    perm[...] = jnp.where(col == lax.rem(row, heads) * part + lax.div(row, heads), 1.0, 0.0).astype(perm.dtype)

    def forward(a, head, j):
        return pltpu.make_async_remote_copy(
            src_ref=outs[a].at[head, pl.ds(pl.multiple_of(j * group, group), group)],
            dst_ref=outs[a].at[head, pl.ds(pl.multiple_of((2 * half - 1 - j) * group, group), group)],
            send_sem=fsend_sem.at[a], recv_sem=frecv_sem.at[a], device_id={'sh': mate}, device_id_type=MESH)

    def pass_on(a):
        arrived((a, 'mixed'))

        def go(i, c):
            forward(a, lax.div(i, nst), first + lax.rem(i, nst)).start()
            return c
        lax.fori_loop(0, n * nst, go, 0)

    def passed(a):
        return pltpu.make_async_remote_copy(
            src_ref=outs[a].at[:, pl.ds(first * group, nst * group)], dst_ref=outs[a].at[:, pl.ds(half * group, nst * group)],
            send_sem=fsend_sem.at[a], recv_sem=frecv_sem.at[a], device_id={'sh': mate}, device_id_type=MESH)

    length = len_ref[me]
    fresh = lax.rem(length, WINDOW)

    def put(a, at, parity):
        rows = piece * heads
        return pltpu.make_async_copy(obuf.at[parity], mids[a].at[pl.ds(pl.multiple_of(at * heads, rows), rows), :], o_sem.at[parity])

    npiece, start_piece = WINDOW // piece, first * group // piece
    due = {}

    def fetch(a, lo, hi):
        copy = pltpu.make_async_copy(outs[a].at[:, pl.ds(lo, hi - lo)], kv_buf.at[:, pl.ds(lo, hi - lo)], kv_sem)
        copy.start()
        copy.wait()

    def get(key):
        arrived(key)
        _, _, lo, size = parts[key]
        if key == (1, 'tail'):
            kv_buf[:, pl.ds(lo, size), :] = tail_buf[...]
        else:
            fetch(key[0], lo, lo + size)

    def get_mixed(a):
        pass_on(a)
        fetch(a, first * group, half * group)

    def get_passed(a):
        passed(a).wait_recv()
        fetch(a, half * group, WINDOW)
    for a in (0, 1):
        if nst:
            due.setdefault(a * npiece, []).append(functools.partial(get_mixed, a))
            due.setdefault(a * npiece + half * group // piece - start_piece, []).append(functools.partial(get_passed, a))
        for key in parts:
            if key[0] == a and key[1] != 'mixed':
                due.setdefault(a * npiece + npiece - start_piece + parts[key][2] // piece, []).append(functools.partial(get, key))

    def soften(h, c):
        slot = lax.broadcasted_iota(jnp.int32, (q_group, WINDOW), 1)
        s_key = new32[0, pl.ds(h, 1), :]
        s_new = jnp.sum(q_heads[h].astype(jnp.float32) * s_key, axis=-1, keepdims=True)
        s = jnp.where(slot == fresh, s_new, scores[h]) / head_dim ** 0.5
        s = jnp.where(slot <= length, s, -jnp.inf)
        e = jnp.exp(s - jnp.max(s, axis=-1, keepdims=True))
        p = e / jnp.sum(e, axis=-1, keepdims=True)
        p_new[h] = jnp.broadcast_to(jnp.sum(jnp.where(slot == fresh, p, 0.0), axis=-1, keepdims=True), (q_group, head_dim))
        probs[h] = jnp.where(slot == fresh, 0.0, p).astype(probs.dtype)
        acc[h] = jnp.zeros_like(acc[h])
        return c
    def soften_all():
        lax.fori_loop(0, heads, soften, 0)
    due.setdefault(npiece, []).insert(0, soften_all)

    def walk(t, c):
        def act(actions):
            for action in actions:
                action()
        for at_step, actions in due.items():
            pl.when(t == at_step)(functools.partial(act, actions))
        a = lax.div(t, npiece)
        base = pl.multiple_of(lax.rem(start_piece + t, npiece) * piece, piece)
        at = pl.ds(base, piece)
        parity = lax.rem(t, 2)

        @pl.when(t >= 2)
        def _():
            put(0, base, parity).wait()

        @pl.when(a == 0)
        def _():
            for h in range(heads):
                scores[h, :, at] = lax.dot_general(q_heads[h], kv_buf[h, at, :], (((1,), (1,)), ((), ())), preferred_element_type=jnp.float32)

        @pl.when(a == 1)
        def _():
            for h in range(heads):
                acc[h] += jnp.dot(probs[h, :, at], kv_buf[h, at, :], preferred_element_type=jnp.float32)
        new_rows = jnp.tile(new32[a], (part, 1))
        for g in range(0, piece // part, 2):
            pair = jnp.concatenate([kv_buf[:, pl.ds(base + (g + e) * part, part), :].reshape(heads * part, head_dim) for e in (0, 1)], axis=1)
            mixed = jnp.dot(perm[...], pair, preferred_element_type=jnp.float32)
            for e in (0, 1):
                row = lax.broadcasted_iota(jnp.int32, (heads * part, head_dim), 0) + (base + (g + e) * part) * heads
                value = mixed[:, e * head_dim:(e + 1) * head_dim]
                value = jnp.where(row < length * heads, value, 0.0)
                value = jnp.where((row >= fresh * heads) & (row < (fresh + 1) * heads), new_rows, value)
                obuf[parity, pl.ds((g + e) * part * heads, part * heads), :] = value.astype(obuf.dtype)
        for b in (0, 1):
            pl.when(a == b)(put(b, base, parity).start)
        return c
    lax.fori_loop(0, 2 * npiece, walk, 0)
    for h in range(heads):
        o = acc[h] + p_new[h].astype(jnp.bfloat16).astype(jnp.float32) * new32[1, pl.ds(h, 1), :]
        for g in range(q_group):
            flat[:, pl.ds((h * q_group + g) * head_dim, head_dim)] = o[g:g + 1].astype(flat.dtype)
    for parity in (0, 1):
        put(0, 0, parity).wait()
    keep.wait()
    def sent(d, c):
        gone = outs[0].at[pl.ds(0, 2), pl.ds(0, half * group)]
        pltpu.make_async_copy(gone, gone, send_sem.at[d]).wait()
        return c
    lax.fori_loop(1, n, sent, 0)
    if nst:
        for a in (0, 1):
            passed(a).wait_send()


def exchange(n, group, half, lengths, residual, norm_gain, cos_rows, sin_rows, k_rows, v_rows, w_query, w_key, w_value, w_out):
    rows, seq, head_dim = k_rows.shape
    over = seq - WINDOW
    kv_heads = w_key.shape[1] // head_dim
    q_group = w_query.shape[1] // w_key.shape[1]
    wide = w_query.shape[1] + w_key.shape[1] + w_value.shape[1]
    depth = 128
    nst = WINDOW // group - half
    bf16, f32 = k_rows.dtype, jnp.float32
    out = jax.ShapeDtypeStruct((n, WINDOW, head_dim), bf16)
    mid = pltpu.HBM((WINDOW * kv_heads, head_dim), bf16)
    any_spec = pl.BlockSpec(memory_space=pl.ANY)
    vmem = pl.BlockSpec(memory_space=pltpu.VMEM)
    hbm = pl.BlockSpec(memory_space=pltpu.HBM)
    dma = pltpu.SemaphoreType.DMA
    return pl.pallas_call(
        functools.partial(exchange_kernel, n, group, half),
        out_shape=(out, out, mid, mid, pltpu.VMEM((1, w_query.shape[1]), bf16), pltpu.VMEM(w_out.shape, bf16)),
        in_specs=[pl.BlockSpec(memory_space=pltpu.SMEM)] + [vmem] * 4 + [any_spec] * 6,
        out_specs=(any_spec,) * 2 + (hbm,) * 2 + (vmem, vmem),
        scratch_shapes=[
            pltpu.VMEM((2, rows, over, head_dim), bf16), pltpu.VMEM((2, rows, over, head_dim), bf16),
            pltpu.VMEM((2, rows, max(nst, 1) * group, head_dim), bf16),
            pltpu.VMEM((n, WINDOW, head_dim), bf16),
            pltpu.VMEM((2, depth, wide), bf16),
            pltpu.VMEM((1, w_query.shape[0]), bf16), pltpu.VMEM((1, wide), f32), pltpu.VMEM((wide // head_dim, head_dim), f32),
            pltpu.VMEM((kv_heads, q_group, head_dim), bf16),
            pltpu.VMEM((kv_heads, q_group, WINDOW), f32), pltpu.VMEM((kv_heads, q_group, WINDOW), bf16),
            pltpu.VMEM((kv_heads, q_group, head_dim), f32), pltpu.VMEM((kv_heads, q_group, head_dim), f32), pltpu.VMEM((2, kv_heads, head_dim), f32),
            pltpu.VMEM((256, 256), bf16), pltpu.VMEM((2, 2 * group * kv_heads, head_dim), bf16), pltpu.VMEM((n, 2 * group, head_dim), bf16),
            dma((n,)), dma((16,)), dma((16,)), dma((2,)), dma((2,)), dma((2, 2)), dma((2, 2)), dma((2, 3)), dma, dma((2,)), dma,
        ],
        compiler_params=pltpu.CompilerParams(collective_id=0, has_side_effects=True, vmem_limit_bytes=VMEM_EXCHANGE),
        cost_estimate=pl.CostEstimate(flops=10 ** 11, bytes_accessed=128 << 20, transcendentals=0),
        name=f'exchange{half}',
    )(lengths, residual, norm_gain, cos_rows, sin_rows, k_rows, v_rows, w_query, w_key, w_value, w_out)[2:]


def finish_kernel(k_in, v_in, x_ref, flat_ref, w_ref, k_out, v_out, x_out, bufs, in_sem, out_sem):
    count, size = bufs.shape[:2]
    each = count // 2

    def rows(i):
        return pl.ds(pl.multiple_of(i * size, size), size)

    def read(a, i):
        return pltpu.make_async_copy((k_in, v_in)[a].at[rows(i), :], bufs.at[a * each + i], in_sem.at[a * each + i])

    def write(a, i):
        return pltpu.make_async_copy(bufs.at[a * each + i], (k_out, v_out)[a].at[rows(i), :], out_sem.at[a * each + i])
    for i in range(each):
        for a in (0, 1):
            read(a, i).start()
    wide = w_ref.shape[1] // each

    def one(i, c):
        at = pl.ds(pl.multiple_of(i * wide, wide), wide)
        o = jnp.dot(flat_ref[...], w_ref[:, at], preferred_element_type=jnp.float32)
        x_out[:, at] = (x_ref[:, at].astype(jnp.float32) + o).astype(x_out.dtype)

        @pl.when(i == each // 2 - 1)
        def _():
            def go(b, c):
                for a in (0, 1):
                    read(a, b).wait()
                    write(a, b).start()
                return c
            lax.fori_loop(0, each, go, 0)
        return c
    lax.fori_loop(0, each, one, 0)
    for i in range(each):
        for a in (0, 1):
            write(a, i).wait()


def finish(k_mid, v_mid, flat, residual, w_out):
    size, head_dim = k_mid.shape
    width, dim = w_out.shape
    count = 16
    cache = jax.ShapeDtypeStruct(k_mid.shape, k_mid.dtype)
    hbm = pl.BlockSpec(memory_space=pltpu.HBM)
    vmem = pl.BlockSpec(memory_space=pltpu.VMEM)
    return pl.pallas_call(
        finish_kernel,
        in_specs=[hbm, hbm, vmem, vmem, vmem],
        out_specs=[hbm, hbm, vmem],
        scratch_shapes=[pltpu.VMEM((count, 2 * size // count, head_dim), k_mid.dtype), pltpu.SemaphoreType.DMA((count,)), pltpu.SemaphoreType.DMA((count,))],
        out_shape=(cache, cache, jax.ShapeDtypeStruct(residual.shape, residual.dtype)),
        compiler_params=pltpu.CompilerParams(vmem_limit_bytes=VMEM_FINISH),
        cost_estimate=pl.CostEstimate(flops=10 ** 9, bytes_accessed=64 << 20, transcendentals=0),
        name='finish',
    )(pltpu.with_memory_space_constraint(k_mid, pltpu.HBM), pltpu.with_memory_space_constraint(v_mid, pltpu.HBM), residual, pltpu.with_memory_space_constraint(flat, pltpu.VMEM), pltpu.with_memory_space_constraint(w_out, pltpu.VMEM))


GROUP = 128
VMEM_EXCHANGE = 27 << 20
VMEM_FINISH = 20 << 20


def solution(mesh):
    head_spec = P('dp', None, 'sh', None)
    row_spec = P(('dp', 'sh'))
    full_spec = P(None, None)
    n = mesh.shape['sh']

    def per_device(k_prefill, v_prefill, lengths, residual, norm_gain, w_query, w_key, w_value, w_out):
        num_rows = residual.shape[0]
        rows, seq, _, head_dim = k_prefill.shape
        kv_heads = w_key.shape[1] // head_dim
        half_dim = head_dim // 2
        k_rows = k_prefill.reshape(rows, seq, head_dim)
        v_rows = v_prefill.reshape(rows, seq, head_dim)
        blocks = (jnp.minimum(lengths, WINDOW) + GROUP - 1) // GROUP
        need = (jnp.max(blocks.reshape(-1, 2).sum(axis=1)) + 1) // 2
        level = jnp.maximum(need - levels(GROUP)[0], 0)
        inv_freq = THETA ** (-2.0 * jnp.arange(half_dim, dtype=jnp.float32) / head_dim)
        angles = lengths.astype(jnp.float32)[:, None] * inv_freq
        cos_rows = jnp.concatenate([jnp.cos(angles), jnp.cos(angles)], axis=1)
        sin_rows = jnp.concatenate([-jnp.sin(angles), jnp.sin(angles)], axis=1)
        k_mid, v_mid, flat, w_keep = lax.switch(
            level, [functools.partial(exchange, n, GROUP, half) for half in levels(GROUP)],
            lengths, residual, norm_gain.reshape(-1, head_dim), cos_rows, sin_rows, k_rows, v_rows, w_query, w_key, w_value, w_out)
        k_cache, v_cache, resid_out = finish(k_mid, v_mid, flat, residual, w_keep)
        cache_shape = (num_rows, WINDOW, kv_heads, head_dim)
        return resid_out, k_cache.reshape(cache_shape), v_cache.reshape(cache_shape)
    return jax.shard_map(per_device, mesh=mesh, in_specs=(head_spec, head_spec, P('dp'), P(('dp', 'sh'), None), P(None), full_spec, full_spec, full_spec, full_spec), out_specs=(P(('dp', 'sh'), None), row_spec, row_spec), check_vma=False)
```

```python
import functools

import jax
import jax.numpy as jnp
from jax import lax
from jax.experimental import pallas as pl
from jax.experimental.pallas import tpu as pltpu
from jax.sharding import PartitionSpec as P

WINDOW = 4096
THETA = 10000.0
EPS = 1e-5
MESH = pl.DeviceIdType.MESH


def levels(group):
    nblk = WINDOW // group
    return tuple(range(nblk // 2 + 1, nblk + 1))


def exchange_kernel(n, group, half, len_ref, x_ref, g_ref, cos_ref, sin_ref, k_in, v_in, wq, wk, wv, wo,
                    k_out, v_out, k_mid, v_mid, flat, wo_keep,
                    over_a, over_b, staged, kv_buf, wbuf, normed, proj, proj2, q_heads, scores, probs, p_new, acc, new32, perm, obuf, tail_buf,
                    send_sem, recv_sem, own_sem, fsend_sem, frecv_sem, over_sem, stage_sem, w_sem, kv_sem, o_sem, wo_sem):
    me = lax.axis_index('sh')
    mate = me + 1 - 2 * lax.rem(me, 2)
    heads, q_group, head_dim = q_heads.shape
    over = over_a.shape[2]
    nblk = WINDOW // group
    first = 2 * half - nblk
    nst = half - first
    barrier = pltpu.get_barrier_semaphore()
    for d in range(1, n):
        pl.semaphore_signal(barrier, inc=1, device_id={'sh': lax.rem(me + d, n)}, device_id_type=MESH)

    ins, outs, mids = (k_in, v_in), (k_out, v_out), (k_mid, v_mid)

    def over_load(a, e):
        return pltpu.make_async_copy(ins[a].at[:, pl.ds(e * WINDOW, over)], (over_a, over_b)[e].at[a], over_sem.at[a, e])

    def own_load(a):
        return pltpu.make_async_copy(ins[a].at[:, pl.ds(first * group, nst * group)], staged.at[a], stage_sem.at[a, 0])

    def other_load(a):
        return pltpu.make_async_copy(ins[a].at[:, pl.ds(half * group, nst * group)], kv_buf.at[:, pl.ds(a * nst * group, nst * group)], stage_sem.at[a, 1])
    for a in (0, 1):
        if nst:
            own_load(a).start()
            other_load(a).start()
        for e in (0, 1):
            over_load(a, e).start()
    depth, wide = wbuf.shape[1], wbuf.shape[2]
    wsteps = wq.shape[0] // depth
    weights = ((wq, 0), (wk, wq.shape[1]), (wv, wq.shape[1] + wk.shape[1]))

    def w_load(step, slot, i):
        src, at = weights[i]
        return pltpu.make_async_copy(src.at[pl.ds(pl.multiple_of(step * depth, depth), depth), :], wbuf.at[slot, :, pl.ds(at, src.shape[1])], w_sem.at[slot, i])
    for i in range(3):
        w_load(0, 0, i).start()
    pl.semaphore_wait(barrier, n - 1)

    piece = 2 * group
    tail = min(piece, max(first * group - over, 0))
    cut = first * group - tail
    parts = {}
    for a in (0, 1):
        parts[a, 'first'] = (over_a.at[a], 0, 0, over)
        if nst:
            parts[a, 'mixed'] = (staged.at[a], 0, first * group, nst * group)
        chunk = 2 * piece if a else WINDOW
        for lo in range(over, cut, chunk):
            parts[a, 'plain', lo] = (ins[a], lo, lo, min(chunk, cut - lo))
        if tail:
            parts[a, 'tail'] = (ins[a], cut, cut, tail)
    index = {key: i for i, key in enumerate(parts)}

    def landing(key, head):
        _, _, to, size = parts[key]
        if key == (1, 'tail'):
            return tail_buf.at[head]
        return outs[key[0]].at[head, pl.ds(to, size)]

    def send(key, d):
        src, at, to, size = parts[key]
        peer = lax.rem(me + d, n)
        return pltpu.make_async_remote_copy(
            src_ref=src.at[peer, pl.ds(at, size)], dst_ref=landing(key, me),
            send_sem=send_sem.at[d], recv_sem=recv_sem.at[index[key]], device_id={'sh': peer}, device_id_type=MESH)

    def own(key):
        src, at, to, size = parts[key]
        return pltpu.make_async_copy(src.at[me, pl.ds(at, size)], landing(key, me), own_sem.at[index[key]])

    def launch(key):
        if key in parts:
            def go(d, c):
                send(key, d).start()
                return c
            lax.fori_loop(1, n, go, 0)
            own(key).start()

    def launch_plain(a):
        for key in parts:
            if key[0] == a and key[1] in ('plain', 'tail'):
                launch(key)

    def arrived(key):
        if key in parts:
            own(key).wait()
            _, _, to, size = parts[key]
            from_all = tail_buf.at[pl.ds(0, n - 1)] if key == (1, 'tail') else outs[key[0]].at[pl.ds(0, n - 1), pl.ds(to, size)]
            pltpu.make_async_copy(from_all, from_all, recv_sem.at[index[key]]).wait()

    launch_plain(0)
    for a in (0, 1):
        for e in (0, 1):
            over_load(a, e).wait()

        def put_first(r, c):
            slot = lax.broadcasted_iota(jnp.int32, over_a.shape[2:], 0)
            over_a[a, r] = jnp.where(slot < len_ref[r] - WINDOW, over_b[a, r], over_a[a, r])
            return c
        lax.fori_loop(0, n, put_first, 0)
        if nst:
            own_load(a).wait()
            other_load(a).wait()

            def put_mixed(i, c):
                r, j = lax.div(i, nst), lax.rem(i, nst)
                blocks = lax.div(jnp.minimum(len_ref[r], WINDOW) + group - 1, group)
                other = kv_buf[r + 1 - 2 * lax.rem(r, 2), pl.ds(pl.multiple_of((a * nst + nst - 1 - j) * group, group), group), :]
                at = pl.ds(pl.multiple_of(j * group, group), group)
                staged[a, r, at, :] = jnp.where(first + j < blocks, staged[a, r, at, :], other)
                return c
            lax.fori_loop(0, n * nst, put_mixed, 0)
    launch((0, 'mixed'))
    launch((0, 'first'))
    launch((1, 'mixed'))
    launch((1, 'first'))
    launch_plain(1)

    x = x_ref[...].astype(jnp.float32)
    inv_rms = lax.rsqrt(jnp.mean(x * x, axis=-1, keepdims=True) + EPS)
    for j in range(x.shape[1] // head_dim):
        at = pl.ds(j * head_dim, head_dim)
        normed[:, at] = (x_ref[:, at].astype(jnp.float32) * inv_rms * g_ref[pl.ds(j, 1), :].astype(jnp.float32)).astype(normed.dtype)
    proj[...] = jnp.zeros_like(proj)
    strip = 1024

    def project(step, c):
        slot = lax.rem(step, 2)

        @pl.when(step + 1 < wsteps)
        def _():
            for i in range(3):
                w_load(step + 1, 1 - slot, i).start()
        for i in range(3):
            w_load(step, slot, i).wait()
        h = normed[:, pl.ds(pl.multiple_of(step * depth, depth), depth)]

        for lo in range(0, wide, strip):
            proj[:, pl.ds(lo, strip)] += jnp.dot(h, wbuf[slot, :, pl.ds(lo, strip)], preferred_element_type=jnp.float32)
        return c
    lax.fori_loop(0, wsteps, project, 0)
    keep = pltpu.make_async_copy(wo, wo_keep, wo_sem)
    keep.start()
    for j in range(wide // head_dim):
        proj2[pl.ds(j, 1), :] = proj[:, pl.ds(j * head_dim, head_dim)]
    cos_row, sin_row = cos_ref[pl.ds(me, 1), :], sin_ref[pl.ds(me, 1), :]

    def turn(value):
        value = value.astype(jnp.bfloat16).astype(jnp.float32)
        return (value * cos_row + pltpu.roll(value, head_dim // 2, 1) * sin_row).astype(jnp.bfloat16)
    nq = heads * q_group
    turned = turn(proj2[pl.ds(0, nq), :])
    for h in range(heads):
        q_heads[h] = turned[h * q_group:(h + 1) * q_group]
    new32[0] = turn(proj2[pl.ds(nq, heads), :]).astype(jnp.float32)
    new32[1] = proj2[pl.ds(nq + heads, heads), :].astype(jnp.bfloat16).astype(jnp.float32)
    part = perm.shape[0] // heads
    row = lax.broadcasted_iota(jnp.int32, perm.shape, 0)
    col = lax.broadcasted_iota(jnp.int32, perm.shape, 1)
    perm[...] = jnp.where(col == lax.rem(row, heads) * part + lax.div(row, heads), 1.0, 0.0).astype(perm.dtype)

    def forward(a, head, j):
        return pltpu.make_async_remote_copy(
            src_ref=outs[a].at[head, pl.ds(pl.multiple_of(j * group, group), group)],
            dst_ref=outs[a].at[head, pl.ds(pl.multiple_of((2 * half - 1 - j) * group, group), group)],
            send_sem=fsend_sem.at[a], recv_sem=frecv_sem.at[a], device_id={'sh': mate}, device_id_type=MESH)

    def pass_on(a):
        arrived((a, 'mixed'))

        def go(i, c):
            forward(a, lax.div(i, nst), first + lax.rem(i, nst)).start()
            return c
        lax.fori_loop(0, n * nst, go, 0)

    def passed(a):
        return pltpu.make_async_remote_copy(
            src_ref=outs[a].at[:, pl.ds(first * group, nst * group)], dst_ref=outs[a].at[:, pl.ds(half * group, nst * group)],
            send_sem=fsend_sem.at[a], recv_sem=frecv_sem.at[a], device_id={'sh': mate}, device_id_type=MESH)

    length = len_ref[me]
    fresh = lax.rem(length, WINDOW)

    def put(a, at, parity):
        rows = piece * heads
        return pltpu.make_async_copy(obuf.at[parity], mids[a].at[pl.ds(pl.multiple_of(at * heads, rows), rows), :], o_sem.at[parity])

    npiece, start_piece = WINDOW // piece, first * group // piece
    due = {}

    def fetch(a, lo, hi):
        copy = pltpu.make_async_copy(outs[a].at[:, pl.ds(lo, hi - lo)], kv_buf.at[:, pl.ds(lo, hi - lo)], kv_sem)
        copy.start()
        copy.wait()

    def get(key):
        arrived(key)
        _, _, lo, size = parts[key]
        if key == (1, 'tail'):
            kv_buf[:, pl.ds(lo, size), :] = tail_buf[...]
        else:
            fetch(key[0], lo, lo + size)

    def get_mixed(a):
        pass_on(a)
        fetch(a, first * group, half * group)

    def get_passed(a):
        passed(a).wait_recv()
        fetch(a, half * group, WINDOW)
    for a in (0, 1):
        if nst:
            due.setdefault(a * npiece, []).append(functools.partial(get_mixed, a))
            due.setdefault(a * npiece + half * group // piece - start_piece, []).append(functools.partial(get_passed, a))
        for key in parts:
            if key[0] == a and key[1] != 'mixed':
                due.setdefault(a * npiece + npiece - start_piece + parts[key][2] // piece, []).append(functools.partial(get, key))

    def soften(h, c):
        slot = lax.broadcasted_iota(jnp.int32, (q_group, WINDOW), 1)
        s_key = new32[0, pl.ds(h, 1), :]
        s_new = jnp.sum(q_heads[h].astype(jnp.float32) * s_key, axis=-1, keepdims=True)
        s = jnp.where(slot == fresh, s_new, scores[h]) / head_dim ** 0.5
        s = jnp.where(slot <= length, s, -jnp.inf)
        e = jnp.exp(s - jnp.max(s, axis=-1, keepdims=True))
        p = e / jnp.sum(e, axis=-1, keepdims=True)
        p_new[h] = jnp.broadcast_to(jnp.sum(jnp.where(slot == fresh, p, 0.0), axis=-1, keepdims=True), (q_group, head_dim))
        probs[h] = jnp.where(slot == fresh, 0.0, p).astype(probs.dtype)
        acc[h] = jnp.zeros_like(acc[h])
        return c
    def soften_all():
        lax.fori_loop(0, heads, soften, 0)
    due.setdefault(npiece, []).insert(0, soften_all)

    def walk(t, c):
        def act(actions):
            for action in actions:
                action()
        for at_step, actions in due.items():
            pl.when(t == at_step)(functools.partial(act, actions))
        a = lax.div(t, npiece)
        base = pl.multiple_of(lax.rem(start_piece + t, npiece) * piece, piece)
        at = pl.ds(base, piece)
        parity = lax.rem(t, 2)

        @pl.when(t >= 2)
        def _():
            put(0, base, parity).wait()

        @pl.when(a == 0)
        def _():
            for h in range(heads):
                scores[h, :, at] = lax.dot_general(q_heads[h], kv_buf[h, at, :], (((1,), (1,)), ((), ())), preferred_element_type=jnp.float32)

        @pl.when(a == 1)
        def _():
            for h in range(heads):
                acc[h] += jnp.dot(probs[h, :, at], kv_buf[h, at, :], preferred_element_type=jnp.float32)
        new_rows = jnp.tile(new32[a], (part, 1))
        for g in range(0, piece // part, 2):
            pair = jnp.concatenate([kv_buf[:, pl.ds(base + (g + e) * part, part), :].reshape(heads * part, head_dim) for e in (0, 1)], axis=1)
            mixed = jnp.dot(perm[...], pair, preferred_element_type=jnp.float32)
            for e in (0, 1):
                row = lax.broadcasted_iota(jnp.int32, (heads * part, head_dim), 0) + (base + (g + e) * part) * heads
                value = mixed[:, e * head_dim:(e + 1) * head_dim]
                value = jnp.where(row < length * heads, value, 0.0)
                value = jnp.where((row >= fresh * heads) & (row < (fresh + 1) * heads), new_rows, value)
                obuf[parity, pl.ds((g + e) * part * heads, part * heads), :] = value.astype(obuf.dtype)
        for b in (0, 1):
            pl.when(a == b)(put(b, base, parity).start)
        return c
    lax.fori_loop(0, 2 * npiece, walk, 0)
    for h in range(heads):
        o = acc[h] + p_new[h].astype(jnp.bfloat16).astype(jnp.float32) * new32[1, pl.ds(h, 1), :]
        for g in range(q_group):
            flat[:, pl.ds((h * q_group + g) * head_dim, head_dim)] = o[g:g + 1].astype(flat.dtype)
    for parity in (0, 1):
        put(0, 0, parity).wait()
    keep.wait()
    def sent(d, c):
        gone = outs[0].at[pl.ds(0, 2), pl.ds(0, half * group)]
        pltpu.make_async_copy(gone, gone, send_sem.at[d]).wait()
        return c
    lax.fori_loop(1, n, sent, 0)
    if nst:
        for a in (0, 1):
            passed(a).wait_send()


def exchange(n, group, half, lengths, residual, norm_gain, cos_rows, sin_rows, k_rows, v_rows, w_query, w_key, w_value, w_out):
    rows, seq, head_dim = k_rows.shape
    over = seq - WINDOW
    kv_heads = w_key.shape[1] // head_dim
    q_group = w_query.shape[1] // w_key.shape[1]
    wide = w_query.shape[1] + w_key.shape[1] + w_value.shape[1]
    depth = 128
    nst = WINDOW // group - half
    bf16, f32 = k_rows.dtype, jnp.float32
    out = jax.ShapeDtypeStruct((n, WINDOW, head_dim), bf16)
    mid = pltpu.HBM((WINDOW * kv_heads, head_dim), bf16)
    any_spec = pl.BlockSpec(memory_space=pl.ANY)
    vmem = pl.BlockSpec(memory_space=pltpu.VMEM)
    hbm = pl.BlockSpec(memory_space=pltpu.HBM)
    dma = pltpu.SemaphoreType.DMA
    return pl.pallas_call(
        functools.partial(exchange_kernel, n, group, half),
        out_shape=(out, out, mid, mid, pltpu.VMEM((1, w_query.shape[1]), bf16), pltpu.VMEM(w_out.shape, bf16)),
        in_specs=[pl.BlockSpec(memory_space=pltpu.SMEM)] + [vmem] * 4 + [any_spec] * 6,
        out_specs=(any_spec,) * 2 + (hbm,) * 2 + (vmem, vmem),
        scratch_shapes=[
            pltpu.VMEM((2, rows, over, head_dim), bf16), pltpu.VMEM((2, rows, over, head_dim), bf16),
            pltpu.VMEM((2, rows, max(nst, 1) * group, head_dim), bf16),
            pltpu.VMEM((n, WINDOW, head_dim), bf16),
            pltpu.VMEM((2, depth, wide), bf16),
            pltpu.VMEM((1, w_query.shape[0]), bf16), pltpu.VMEM((1, wide), f32), pltpu.VMEM((wide // head_dim, head_dim), f32),
            pltpu.VMEM((kv_heads, q_group, head_dim), bf16),
            pltpu.VMEM((kv_heads, q_group, WINDOW), f32), pltpu.VMEM((kv_heads, q_group, WINDOW), bf16),
            pltpu.VMEM((kv_heads, q_group, head_dim), f32), pltpu.VMEM((kv_heads, q_group, head_dim), f32), pltpu.VMEM((2, kv_heads, head_dim), f32),
            pltpu.VMEM((256, 256), bf16), pltpu.VMEM((2, 2 * group * kv_heads, head_dim), bf16), pltpu.VMEM((n, 2 * group, head_dim), bf16),
            dma((n,)), dma((16,)), dma((16,)), dma((2,)), dma((2,)), dma((2, 2)), dma((2, 2)), dma((2, 3)), dma, dma((2,)), dma,
        ],
        compiler_params=pltpu.CompilerParams(collective_id=0, has_side_effects=True, vmem_limit_bytes=VMEM_EXCHANGE),
        cost_estimate=pl.CostEstimate(flops=10 ** 11, bytes_accessed=128 << 20, transcendentals=0),
        name=f'exchange{half}',
    )(lengths, residual, norm_gain, cos_rows, sin_rows, k_rows, v_rows, w_query, w_key, w_value, w_out)[2:]


def finish_kernel(k_in, v_in, x_ref, flat_ref, w_ref, k_out, v_out, x_out, bufs, in_sem, out_sem):
    count, size = bufs.shape[:2]
    each = count // 2

    def rows(i):
        return pl.ds(pl.multiple_of(i * size, size), size)

    def read(a, i):
        return pltpu.make_async_copy((k_in, v_in)[a].at[rows(i), :], bufs.at[a * each + i], in_sem.at[a * each + i])

    def write(a, i):
        return pltpu.make_async_copy(bufs.at[a * each + i], (k_out, v_out)[a].at[rows(i), :], out_sem.at[a * each + i])
    for i in range(each):
        for a in (0, 1):
            read(a, i).start()
    wide = w_ref.shape[1] // each

    def one(i, c):
        at = pl.ds(pl.multiple_of(i * wide, wide), wide)
        o = jnp.dot(flat_ref[...], w_ref[:, at], preferred_element_type=jnp.float32)
        x_out[:, at] = (x_ref[:, at].astype(jnp.float32) + o).astype(x_out.dtype)
        for a in (0, 1):
            read(a, i).wait()
            write(a, i).start()
        return c
    lax.fori_loop(0, each, one, 0)
    for i in range(each):
        for a in (0, 1):
            write(a, i).wait()


def finish(k_mid, v_mid, flat, residual, w_out):
    size, head_dim = k_mid.shape
    width, dim = w_out.shape
    count = 16
    cache = jax.ShapeDtypeStruct(k_mid.shape, k_mid.dtype)
    hbm = pl.BlockSpec(memory_space=pltpu.HBM)
    vmem = pl.BlockSpec(memory_space=pltpu.VMEM)
    return pl.pallas_call(
        finish_kernel,
        in_specs=[hbm, hbm, vmem, vmem, vmem],
        out_specs=[hbm, hbm, vmem],
        scratch_shapes=[pltpu.VMEM((count, 2 * size // count, head_dim), k_mid.dtype), pltpu.SemaphoreType.DMA((count,)), pltpu.SemaphoreType.DMA((count,))],
        out_shape=(cache, cache, jax.ShapeDtypeStruct(residual.shape, residual.dtype)),
        compiler_params=pltpu.CompilerParams(vmem_limit_bytes=VMEM_FINISH),
        cost_estimate=pl.CostEstimate(flops=10 ** 9, bytes_accessed=64 << 20, transcendentals=0),
        name='finish',
    )(pltpu.with_memory_space_constraint(k_mid, pltpu.HBM), pltpu.with_memory_space_constraint(v_mid, pltpu.HBM), residual, pltpu.with_memory_space_constraint(flat, pltpu.VMEM), pltpu.with_memory_space_constraint(w_out, pltpu.VMEM))


GROUP = 128
VMEM_EXCHANGE = 27 << 20
VMEM_FINISH = 20 << 20


def solution(mesh):
    head_spec = P('dp', None, 'sh', None)
    row_spec = P(('dp', 'sh'))
    full_spec = P(None, None)
    n = mesh.shape['sh']

    def per_device(k_prefill, v_prefill, lengths, residual, norm_gain, w_query, w_key, w_value, w_out):
        num_rows = residual.shape[0]
        rows, seq, _, head_dim = k_prefill.shape
        kv_heads = w_key.shape[1] // head_dim
        half_dim = head_dim // 2
        k_rows = k_prefill.reshape(rows, seq, head_dim)
        v_rows = v_prefill.reshape(rows, seq, head_dim)
        blocks = (jnp.minimum(lengths, WINDOW) + GROUP - 1) // GROUP
        need = (jnp.max(blocks.reshape(-1, 2).sum(axis=1)) + 1) // 2
        level = jnp.maximum(need - levels(GROUP)[0], 0)
        inv_freq = THETA ** (-2.0 * jnp.arange(half_dim, dtype=jnp.float32) / head_dim)
        angles = lengths.astype(jnp.float32)[:, None] * inv_freq
        cos_rows = jnp.concatenate([jnp.cos(angles), jnp.cos(angles)], axis=1)
        sin_rows = jnp.concatenate([-jnp.sin(angles), jnp.sin(angles)], axis=1)
        k_mid, v_mid, flat, w_keep = lax.switch(
            level, [functools.partial(exchange, n, GROUP, half) for half in levels(GROUP)],
            lengths, residual, norm_gain.reshape(-1, head_dim), cos_rows, sin_rows, k_rows, v_rows, w_query, w_key, w_value, w_out)
        k_cache, v_cache, resid_out = finish(k_mid, v_mid, flat, residual, w_keep)
        cache_shape = (num_rows, WINDOW, kv_heads, head_dim)
        return resid_out, k_cache.reshape(cache_shape), v_cache.reshape(cache_shape)
    return jax.shard_map(per_device, mesh=mesh, in_specs=(head_spec, head_spec, P('dp'), P(('dp', 'sh'), None), P(None), full_spec, full_spec, full_spec, full_spec), out_specs=(P(('dp', 'sh'), None), row_spec, row_spec), check_vma=False)
```
